16 devices in a mesh: dp: 2 (over z), tp: 8 (over y, x, core).
Axes of the slice: x: 2, y: 2, z: 2, core: 2. Of those that a mesh axis runs over, the one named last changes fastest.
Arguments:
- hidden: bfloat16 [512, 3072], P('dp'), parts along dimension 0
- positions: int32 [512], P('dp'), parts along dimension 0
- k_cache: bfloat16 [2, 512, 128, 8, 128], P(None, 'dp', None, 'tp'), parts along dimension 1
- v_cache: bfloat16 [2, 512, 128, 8, 128], P(None, 'dp', None, 'tp'), parts along dimension 1
- attn_norm: bfloat16 [2, 3072], replicated
- w_query: bfloat16 [2, 3072, 3072], P(None, None, 'tp')
- w_key: bfloat16 [2, 3072, 1024], P(None, None, 'tp')
- w_value: bfloat16 [2, 3072, 1024], P(None, None, 'tp')
- w_out: bfloat16 [2, 3072, 3072], P(None, 'tp')
- mlp_norm: bfloat16 [2, 3072], replicated
- w_gate: bfloat16 [2, 3072, 8192], P(None, None, 'tp')
- w_up: bfloat16 [2, 3072, 8192], P(None, None, 'tp')
- w_down: bfloat16 [2, 8192, 3072], P(None, 'tp')
Outputs:
- output 1: bfloat16 [512, 3072], P('dp'), parts along dimension 0
- output 2: bfloat16 [2, 512, 128, 8, 128], P(None, 'dp', None, 'tp'), parts along dimension 1
- output 3: bfloat16 [2, 512, 128, 8, 128], P(None, 'dp', None, 'tp'), parts along dimension 1
There are 2 independent parts. The reference program is written for one: setup_inputs(seed, part) draws one part's arguments, and reference() takes and returns one part's arrays. A program takes and returns all parts, laid end to end along the dimension named above; an argument that names none is the same for every part.
All inputs are finite; a program needn't handle non-finite values.
Results may differ from the reference program's by a relative error of at most 0.02.
Values are sent between devices in bfloat16 or wider.
A program may use at most 1 GiB of HBM per device.

```python
import math
import jax
import jax.numpy as jnp
from jax import lax

LAYERS = 2
BATCH = 256
SEQ = 128
D = 3072
HEADS = 24
KV_HEADS = 8
HEAD = 128
FF = 8192


def normal_weight(rng_key, shape, scale):
    return (jax.random.normal(rng_key, shape, jnp.float32) * scale).astype(jnp.bfloat16)


def setup_inputs(seed: int = 0, part: int = 0) -> dict:
    base_key = jax.random.key(seed)
    shared_keys = jax.random.split(base_key, 9)
    part_keys = jax.random.split(jax.random.fold_in(base_key, part), 5)
    cache_shape = (LAYERS, BATCH, SEQ, KV_HEADS, HEAD)
    drawn_pos = jax.random.randint(part_keys[1], (BATCH,), SEQ // 8, SEQ, dtype=jnp.int32)
    drawn_pos = drawn_pos.at[0].set(SEQ - 1).at[1].set(SEQ // 8)
    return dict(
        hidden=normal_weight(part_keys[0], (BATCH, D), 1.0),
        positions=jax.random.permutation(part_keys[2], drawn_pos),
        k_cache=normal_weight(part_keys[3], cache_shape, 1.0),
        v_cache=normal_weight(part_keys[4], cache_shape, 1.0),
        attn_norm=(1.0 + 0.3 * jax.random.normal(shared_keys[0], (LAYERS, D), jnp.float32)).astype(jnp.bfloat16),
        w_query=normal_weight(shared_keys[1], (LAYERS, D, HEADS * HEAD), D ** -0.5),
        w_key=normal_weight(shared_keys[2], (LAYERS, D, KV_HEADS * HEAD), 1.5 * D ** -0.5),
        w_value=normal_weight(shared_keys[3], (LAYERS, D, KV_HEADS * HEAD), 1.5 * D ** -0.5),
        w_out=normal_weight(shared_keys[4], (LAYERS, HEADS * HEAD, D), 0.5 * (SEQ / (HEADS * HEAD)) ** 0.5),
        mlp_norm=(1.0 + 0.3 * jax.random.normal(shared_keys[5], (LAYERS, D), jnp.float32)).astype(jnp.bfloat16),
        w_gate=normal_weight(shared_keys[6], (LAYERS, D, FF), D ** -0.5),
        w_up=normal_weight(shared_keys[7], (LAYERS, D, FF), D ** -0.5),
        w_down=normal_weight(shared_keys[8], (LAYERS, FF, D), 1.5 * FF ** -0.5),
    )


def rms_norm(hidden, weight):
    hidden_f32 = hidden.astype(jnp.float32)
    mean_sq = jnp.mean(hidden_f32 * hidden_f32, axis=-1, keepdims=True)
    return (hidden_f32 * lax.rsqrt(mean_sq + 1e-5) * weight.astype(jnp.float32)).astype(jnp.bfloat16)


def rope_tables(positions, head_dim):
    half_dim = head_dim // 2
    inv_freq = jnp.power(500000.0, -jnp.arange(half_dim, dtype=jnp.float32) * (2.0 / head_dim))
    wavelen = (2.0 * math.pi) / inv_freq
    smooth = (8192.0 / wavelen - 1.0) / 3.0
    blended = (1.0 - smooth) * inv_freq / 8.0 + smooth * inv_freq
    scaled = jnp.where(wavelen < 2048.0, inv_freq, jnp.where(wavelen > 8192.0, inv_freq / 8.0, blended))
    angles = positions.astype(jnp.float32)[:, None] * scaled[None, :]
    return jnp.cos(angles), jnp.sin(angles)


def apply_rope(vectors, cos_tab, sin_tab):
    half_dim = vectors.shape[-1] // 2
    vec_f32 = vectors.astype(jnp.float32)
    first = vec_f32[..., :half_dim]
    second = vec_f32[..., half_dim:]
    cos_b = cos_tab[:, None, :]
    sin_b = sin_tab[:, None, :]
    return jnp.concatenate([first * cos_b - second * sin_b, second * cos_b + first * sin_b], axis=-1).astype(jnp.bfloat16)


def attend(query, k_all, v_all, visible):
    scores = jnp.einsum('bkgd,bskd->bkgs', query.astype(jnp.float32), k_all.astype(jnp.float32)) * (query.shape[-1] ** -0.5)
    scores = jnp.where(visible, scores, -jnp.inf)
    prob_rows = jax.nn.softmax(scores, axis=-1).astype(jnp.bfloat16)
    attn_out = jnp.einsum('bkgs,bskd->bkgd', prob_rows.astype(jnp.float32), v_all.astype(jnp.float32))
    return attn_out.astype(jnp.bfloat16)


def reference(hidden, positions, k_cache, v_cache, attn_norm, w_query, w_key, w_value, w_out, mlp_norm, w_gate, w_up, w_down):
    group = HEADS // KV_HEADS
    cos_tab, sin_tab = rope_tables(positions, HEAD)
    seq_ids = jnp.arange(SEQ)
    at_pos = (seq_ids[None, :] == positions[:, None])[:, :, None, None]
    visible = (seq_ids[None, :] <= positions[:, None])[:, None, None, :]

    def layer_step(state, layer_args):
        norm_attn, wq_layer, wk_layer, wv_layer, wo_layer, norm_mlp, wg_layer, wu_layer, wd_layer, k_layer, v_layer = layer_args
        normed = rms_norm(state, norm_attn)
        query = jnp.dot(normed, wq_layer, preferred_element_type=jnp.float32).astype(jnp.bfloat16)
        key_new = jnp.dot(normed, wk_layer, preferred_element_type=jnp.float32).astype(jnp.bfloat16)
        value_new = jnp.dot(normed, wv_layer, preferred_element_type=jnp.float32).astype(jnp.bfloat16)
        query = apply_rope(query.reshape(BATCH, HEADS, HEAD), cos_tab, sin_tab)
        key_new = apply_rope(key_new.reshape(BATCH, KV_HEADS, HEAD), cos_tab, sin_tab)
        value_new = value_new.reshape(BATCH, KV_HEADS, HEAD)
        k_layer = jnp.where(at_pos, key_new[:, None], k_layer)
        v_layer = jnp.where(at_pos, value_new[:, None], v_layer)
        attended = attend(query.reshape(BATCH, KV_HEADS, group, HEAD), k_layer, v_layer, visible)
        mixed = jnp.dot(attended.reshape(BATCH, HEADS * HEAD), wo_layer, preferred_element_type=jnp.float32)
        state = state + mixed.astype(jnp.bfloat16)
        normed = rms_norm(state, norm_mlp)
        gate_proj = jnp.dot(normed, wg_layer, preferred_element_type=jnp.float32).astype(jnp.bfloat16)
        up_proj = jnp.dot(normed, wu_layer, preferred_element_type=jnp.float32).astype(jnp.bfloat16)
        activated = (jax.nn.silu(gate_proj.astype(jnp.float32)) * up_proj.astype(jnp.float32)).astype(jnp.bfloat16)
        state = state + jnp.dot(activated, wd_layer, preferred_element_type=jnp.float32).astype(jnp.bfloat16)
        return state, (k_layer, v_layer)

    stacked = (attn_norm, w_query, w_key, w_value, w_out, mlp_norm, w_gate, w_up, w_down, k_cache, v_cache)
    final, (k_out, v_out) = lax.scan(layer_step, hidden, stacked)
    return final, k_out, v_out
```

```python
import functools
import math

import jax
import jax.numpy as jnp
from jax import lax
from jax.experimental import pallas as pl
from jax.experimental.pallas import tpu as pltpu
from jax.sharding import PartitionSpec as P

F32 = jnp.float32
BF16 = jnp.bfloat16
MESH = pl.DeviceIdType.MESH
VMEM_BYTES = 64 * 1024 * 1024 - 128 * 1024
EPS = 1e-5


def rope_tables(positions, head_dim):
    half_dim = head_dim // 2
    inv_freq = jnp.power(500000.0, -jnp.arange(half_dim, dtype=jnp.float32) * (2.0 / head_dim))
    wavelen = (2.0 * math.pi) / inv_freq
    smooth = (8192.0 / wavelen - 1.0) / 3.0
    blended = (1.0 - smooth) * inv_freq / 8.0 + smooth * inv_freq
    scaled = jnp.where(wavelen < 2048.0, inv_freq, jnp.where(wavelen > 8192.0, inv_freq / 8.0, blended))
    angles = positions.astype(jnp.float32)[:, None] * scaled[None, :]
    return jnp.cos(angles), jnp.sin(angles)


def normed(x, gain):
    xf = x.astype(F32)
    mean_sq = jnp.mean(xf * xf, axis=-1, keepdims=True)
    return (xf * lax.rsqrt(mean_sq + EPS) * gain).astype(BF16)


def first_qkv_kernel(x_ref, g_ref, wq_ref, wk_ref, wv_ref, o_ref, h_ref):
    rows = x_ref.shape[0]
    qd = wq_ref.shape[2]
    kd = wk_ref.shape[2]
    gain = g_ref[0:1, :].astype(F32)

    @pl.loop(0, rows // 16)
    def _(i):
        sl = pl.ds(pl.multiple_of(i * 16, 16), 16)
        h_ref[sl, :] = normed(x_ref[sl, :], gain)

    h = h_ref[...]
    o_ref[:, 0:qd] = jnp.dot(h, wq_ref[0], preferred_element_type=F32).astype(BF16)
    o_ref[:, qd:qd + kd] = jnp.dot(h, wk_ref[0], preferred_element_type=F32).astype(BF16)
    o_ref[:, qd + kd:] = jnp.dot(h, wv_ref[0], preferred_element_type=F32).astype(BF16)


def first_qkv(hidden, attn_norm, w_query, w_key, w_value):
    rows, d = hidden.shape
    qd, kd = w_query.shape[2], w_key.shape[2]

    def first(shape):
        return pl.BlockSpec((1,) + shape, lambda i: (0, 0, 0))

    return pl.pallas_call(
        first_qkv_kernel,
        grid=(1,),
        in_specs=[
            pl.BlockSpec((rows, d), lambda i: (0, 0)),
            pl.BlockSpec(attn_norm.shape, lambda i: (0, 0)),
            first((d, qd)), first((d, kd)), first((d, kd)),
        ],
        out_specs=pl.BlockSpec((rows, qd + 2 * kd), lambda i: (0, 0)),
        out_shape=jax.ShapeDtypeStruct((rows, qd + 2 * kd), BF16),
        scratch_shapes=[pltpu.VMEM((rows, d), BF16)],
        compiler_params=pltpu.CompilerParams(vmem_limit_bytes=40 * 1024 * 1024),
        name="first_qkv",
    )(hidden, attn_norm, w_query, w_key, w_value)


BLOCK = 32


def attention_kernel(layer, pos_s, qkv_ref, cos_ref, sin_ref, posr_ref, k_ref, v_ref, *rest):
    o_ref, ko_ref, vo_ref = rest[-3:]
    step = pl.program_id(0)
    head = k_ref.shape[3]
    seq = k_ref.shape[2]
    heads = o_ref.shape[1] // head
    scale = head ** -0.5
    cos = cos_ref[...]
    sin = sin_ref[...]

    def rope(vec):
        return vec * cos + pltpu.roll(vec, head // 2, 1) * sin

    qs = [rope(qkv_ref[:, h * head:(h + 1) * head].astype(F32)) for h in range(heads)]
    kn = rope(qkv_ref[:, heads * head:(heads + 1) * head].astype(F32))
    vn = qkv_ref[:, (heads + 1) * head:(heads + 2) * head].astype(F32)

    seq_ids = lax.broadcasted_iota(jnp.int32, (seq // 16, 16, head), 0) * 16 + lax.broadcasted_iota(jnp.int32, (seq // 16, 16, head), 1)
    seq_bf = seq_ids.astype(F32).astype(BF16)
    row_of = lax.broadcasted_iota(jnp.int32, (32, head), 0) % 8
    lane = lax.broadcasted_iota(jnp.int32, (32, seq), 1)
    outs = []
    for j in range(BLOCK // 8):
        pieces = [q[8 * j:8 * j + 8] for q in qs]
        pieces += [jnp.zeros((8, head), F32)] * (4 - heads)
        qj = jnp.concatenate(pieces, axis=0).astype(BF16)
        scores = None
        for b8 in range(8):
            b = 8 * j + b8
            pos_b = pos_s[step * BLOCK + b].astype(F32)
            here = seq_bf == jnp.full((16, head), pos_b, F32).astype(BF16)[None]
            k_row = jnp.broadcast_to(kn[b:b + 1], (16, head)).astype(BF16)[None]
            v_row = jnp.broadcast_to(vn[b:b + 1], (16, head)).astype(BF16)[None]
            k_b = jnp.where(here, k_row, k_ref[0, b].reshape(seq // 16, 16, head)).reshape(seq, head)
            ko_ref[0, b] = k_b
            vo_ref[0, b] = jnp.where(here, v_row, v_ref[0, b].reshape(seq // 16, 16, head)).reshape(seq, head)
            s_b = lax.dot_general(qj, k_b, (((1,), (1,)), ((), ())), preferred_element_type=F32)
            scores = s_b if scores is None else jnp.where(row_of == b8, s_b, scores)
        scores = jnp.where(lane <= posr_ref[32 * j:32 * j + 32, :], scores * scale, -jnp.inf)
        peak = jnp.max(scores, axis=1, keepdims=True)
        weight = jnp.exp(scores - peak)
        total = jnp.sum(weight, axis=1, keepdims=True)
        prob = (weight * (1.0 / total)).astype(BF16)
        mixed = None
        for b8 in range(8):
            o_b = jnp.dot(prob, vo_ref[0, 8 * j + b8], preferred_element_type=F32)
            mixed = o_b if mixed is None else jnp.where(row_of == b8, o_b, mixed)
        outs.append(mixed)
    for h in range(heads):
        o_h = jnp.concatenate([m[8 * h:8 * h + 8] for m in outs], axis=0)
        o_ref[:, h * head:(h + 1) * head] = o_h.astype(BF16)


def attention(layer, qkv, cos2, sin2, posr, positions, k_cache, v_cache, k_prev, v_prev):
    layers, batch, seq, head = k_cache.shape
    qd = qkv.shape[1] - 2 * head
    cache_spec = pl.BlockSpec((1, BLOCK, seq, head), lambda i, p: (layer, i, 0, 0))
    row_spec = lambda width: pl.BlockSpec((BLOCK, width), lambda i, p: (i, 0))
    in_specs = [
        row_spec(qkv.shape[1]), row_spec(head), row_spec(head),
        pl.BlockSpec((BLOCK * 4, 1), lambda i, p: (i, 0)),
        cache_spec, cache_spec,
    ]
    args = [qkv, cos2, sin2, posr, k_cache, v_cache]
    aliases = {}
    if k_prev is not None:
        in_specs += [pl.BlockSpec(memory_space=pl.ANY)] * 2
        args += [k_prev, v_prev]
        aliases = {7: 1, 8: 2}
    return pl.pallas_call(
        functools.partial(attention_kernel, layer),
        grid_spec=pltpu.PrefetchScalarGridSpec(
            num_scalar_prefetch=1,
            grid=(batch // BLOCK,),
            in_specs=in_specs,
            out_specs=[row_spec(qd), cache_spec, cache_spec],
        ),
        out_shape=[
            jax.ShapeDtypeStruct((batch, qd), BF16),
            jax.ShapeDtypeStruct(k_cache.shape, BF16),
            jax.ShapeDtypeStruct(v_cache.shape, BF16),
        ],
        input_output_aliases=aliases,
        compiler_params=pltpu.CompilerParams(vmem_limit_bytes=40 * 1024 * 1024),
        name=f"attention_{layer}",
    )(positions, *args)


CHUNKS = 2


def mlp_kernel(layer, last, *refs):
    refs = list(refs)
    o_ref, x_hbm, gm_ref, ga_ref, wo_hbm, wg_hbm, wu_hbm, wd_hbm = refs[:8]
    refs = refs[8:]
    if last:
        x_out = refs[0]
        refs = refs[1:]
    else:
        wq_hbm, wk_hbm, wv_hbm, qkv_out, xres_out = refs[:5]
        refs = refs[5:]
    (wo, wg, wu, wd, xres, part, hbuf, abuf, d2d_in, rs_out, rs_in, acc, w_sem, x_sem,
     d2d_s, d2d_r, rs_s, rs_r, ag_s, ag_r, fw_s, fw_r) = refs[:22]
    refs = refs[22:]
    if last:
        (out_sem,) = refs
    else:
        wq, wk, wv = refs

    chunks, _, chips_n, own, d = part.shape
    rows = 8 * own
    ff = wg.shape[1]
    me = lax.axis_index("tp")
    group = lax.axis_index("dp")
    core = me % 2
    chip = me // 2
    chips = [chip, chip + 1 - 2 * (chip % 2), (chip + 2) % 4, 3 - chip]
    partner = (group, chip * 2 + 1 - core)
    peers = [None] + [(group, chips[k] * 2 + core) for k in (1, 2, 3)]
    order = (3, 1, 2)

    loads = [(wo_hbm, wo), (wg_hbm, wg), (wu_hbm, wu), (wd_hbm, wd)]
    nxt = layer
    if not last:
        loads += [(wq_hbm, wq), (wk_hbm, wk), (wv_hbm, wv)]
    load = []
    for i, (src, dst) in enumerate(loads):
        which = layer if i < 4 else layer + 1
        cp = pltpu.make_async_copy(src.at[which], dst, w_sem.at[i])
        cp.start()
        load.append(cp)
    x_loads = []
    for hh in range(chunks):
        src = x_hbm.at[hh, core, chip] if layer == 0 else x_hbm.at[hh]
        cp = pltpu.make_async_copy(src, xres.at[hh], x_sem.at[hh])
        cp.start()
        x_loads.append(cp)

    barrier = pltpu.get_barrier_semaphore()
    for dev in [partner] + peers[1:]:
        pl.semaphore_signal(barrier, inc=1, device_id=dev, device_id_type=MESH)
    pl.semaphore_wait(barrier, 4)

    def remote(src, dst, s, r, dev):
        return pltpu.make_async_remote_copy(
            src_ref=src, dst_ref=dst, send_sem=s, recv_sem=r, device_id=dev, device_id_type=MESH)

    def d2d(hh):
        return remote(part.at[hh, 1 - core], d2d_in.at[hh], d2d_s.at[hh], d2d_r.at[hh], partner)

    def rs(hh, k):
        return remote(rs_out.at[hh, k - 1], rs_in.at[hh, k - 1], rs_s.at[hh, k - 1], rs_r.at[hh, k - 1], peers[k])

    def ag(hh, k):
        ref = hbuf.at[hh, core, chip]
        return remote(ref, ref, ag_s.at[hh, k - 1], ag_r.at[hh, k - 1], peers[k])

    def ag_in(hh, k):
        ref = hbuf.at[hh, core, chips[k]]
        return remote(ref, ref, ag_s.at[hh, k - 1], ag_r.at[hh, k - 1], peers[k])

    def fw(hh, k):
        ref = hbuf.at[hh, core, chips[k]]
        return remote(ref, ref, fw_s.at[hh, k], fw_r.at[hh, k], partner)

    def fw_in(hh, k):
        ref = hbuf.at[hh, 1 - core, chips[k]]
        return remote(ref, ref, fw_s.at[hh, k], fw_r.at[hh, k], partner)

    def put_part(hh, cols, value):
        value = value.astype(BF16)
        for p in range(2):
            for c in range(4):
                at = (p * 4 + c) * own
                part[hh, p, c, :, cols] = value[at:at + own]

    def ph0(hh):
        d2d(hh).start()

    def ph1(hh):
        d2d(hh).wait_recv()
        for k in order:
            pair = part[hh, core, chips[k]].astype(F32) + d2d_in[hh, chips[k]].astype(F32)
            rs_out[hh, k - 1] = pair.astype(BF16)
            rs(hh, k).start()
        acc[hh] = part[hh, core, chip].astype(F32) + d2d_in[hh, chip].astype(F32)
        d2d(hh).wait_send()

    def ph2(hh, mode):
        for k in (1, 2, 3):
            rs(hh, k).wait_recv()
        total = acc[hh]
        for k in (1, 2, 3):
            total = total + rs_in[hh, k - 1].astype(F32)
        x = (xres[hh].astype(F32) + total.astype(BF16).astype(F32)).astype(BF16)
        if mode == "final":
            hbuf[hh, core, chip] = x
        else:
            xres[hh] = x
            gain = (gm_ref[layer:layer + 1, :] if mode == "mlp" else ga_ref[layer + 1:layer + 2, :]).astype(F32)
            hbuf[hh, core, chip] = normed(x, gain)
            if mode == "attn":
                xres_out[hh] = x
        for k in order:
            ag(hh, k).start()
        fw(hh, 0).start()
        for k in (1, 2, 3):
            rs(hh, k).wait_send()

    def ph3(hh):
        for k in (1, 2, 3):
            ag_in(hh, k).wait_recv()
            fw(hh, k).start()

    def ph4(hh):
        for k in range(4):
            fw_in(hh, k).wait_recv()
        for k in (1, 2, 3):
            ag(hh, k).wait_send()
        for k in range(4):
            fw(hh, k).wait_send()

    def out_product(hh):
        o = o_ref[hh * rows:(hh + 1) * rows, :]

        @pl.loop(0, d // 1024)
        def _(n):
            cols = pl.ds(pl.multiple_of(n * 1024, 1024), 1024)
            put_part(hh, cols, jnp.dot(o, wo[:, cols], preferred_element_type=F32))

    def gate_up(hh):
        h = hbuf[hh].reshape(rows, d)

        @pl.loop(0, ff // 256)
        def _(n):
            cols = pl.ds(pl.multiple_of(n * 256, 256), 256)
            g = jnp.dot(h, wg[:, cols], preferred_element_type=F32).astype(BF16).astype(F32)
            u = jnp.dot(h, wu[:, cols], preferred_element_type=F32).astype(BF16).astype(F32)
            abuf[:, cols] = (g * jax.nn.sigmoid(g) * u).astype(BF16)

    def down(hh):
        @pl.loop(0, d // 1024)
        def _(n):
            cols = pl.ds(pl.multiple_of(n * 1024, 1024), 1024)
            put_part(hh, cols, jnp.dot(abuf[...], wd[:, cols], preferred_element_type=F32))

    def next_qkv(hh):
        h = hbuf[hh].reshape(rows, d)
        qd, kd = wq.shape[1], wk.shape[1]
        at = slice(hh * rows, (hh + 1) * rows)
        qkv_out[at, 0:qd] = jnp.dot(h, wq[...], preferred_element_type=F32).astype(BF16)
        qkv_out[at, qd:qd + kd] = jnp.dot(h, wk[...], preferred_element_type=F32).astype(BF16)
        qkv_out[at, qd + kd:] = jnp.dot(h, wv[...], preferred_element_type=F32).astype(BF16)

    end = "final" if last else "attn"
    load[0].wait()
    for hh in range(chunks):
        out_product(hh)
        ph0(hh)
    for cp in x_loads:
        cp.wait()
    ph1(0)
    ph1(1)
    ph2(0, "mlp")
    ph2(1, "mlp")
    ph3(0)
    ph4(0)
    load[1].wait()
    load[2].wait()
    gate_up(0)
    ph3(1)
    load[3].wait()
    down(0)
    ph0(0)
    ph4(1)
    gate_up(1)
    ph1(0)
    down(1)
    ph0(1)
    ph1(1)
    ph2(0, end)
    ph2(1, end)
    if last:
        def put(hh):
            return pltpu.make_async_copy(hbuf.at[hh], x_out.at[hh], out_sem.at[hh])
        ph3(0)
        ph4(0)
        put(0).start()
        ph3(1)
        ph4(1)
        put(1).start()
        put(0).wait()
        put(1).wait()
    else:
        ph3(0)
        ph4(0)
        for i in (4, 5, 6):
            load[i].wait()
        next_qkv(0)
        ph3(1)
        ph4(1)
        next_qkv(1)


def sums_and_mlp(layer, last, o, x, mlp_norm, attn_norm, w_out, w_gate, w_up, w_down, w_query, w_key, w_value):
    batch, qd = o.shape
    d = w_out.shape[2]
    ff = w_gate.shape[2]
    kd = w_key.shape[2]
    own = batch // (8 * CHUNKS)
    rows = 8 * own
    vmem = pl.BlockSpec(memory_space=pltpu.VMEM)
    hbm = pl.BlockSpec(memory_space=pl.ANY)
    args = [o, x, mlp_norm, attn_norm, w_out, w_gate, w_up, w_down]
    in_specs = [vmem, hbm, vmem, vmem] + [hbm] * 4
    if last:
        out_shape = jax.ShapeDtypeStruct((CHUNKS, 2, 4, own, d), BF16)
        out_specs = hbm
    else:
        args += [w_query, w_key, w_value]
        in_specs += [hbm] * 3
        out_shape = [jax.ShapeDtypeStruct((batch, qd + 2 * kd), BF16), jax.ShapeDtypeStruct((CHUNKS, own, d), BF16)]
        out_specs = [vmem, vmem]
    dma = pltpu.SemaphoreType.DMA
    scratch = [
        pltpu.VMEM((qd, d), BF16), pltpu.VMEM((d, ff), BF16), pltpu.VMEM((d, ff), BF16), pltpu.VMEM((ff, d), BF16),
        pltpu.VMEM((CHUNKS, own, d), BF16),
        pltpu.VMEM((CHUNKS, 2, 4, own, d), BF16),
        pltpu.VMEM((CHUNKS, 2, 4, own, d), BF16),
        pltpu.VMEM((rows, ff), BF16),
        pltpu.VMEM((CHUNKS, 4, own, d), BF16),
        pltpu.VMEM((CHUNKS, 3, own, d), BF16),
        pltpu.VMEM((CHUNKS, 3, own, d), BF16),
        pltpu.VMEM((CHUNKS, own, d), F32),
        dma((7,)), dma((CHUNKS,)),
        dma((CHUNKS,)), dma((CHUNKS,)),
        dma((CHUNKS, 3)), dma((CHUNKS, 3)),
        dma((CHUNKS, 3)), dma((CHUNKS, 3)),
        dma((CHUNKS, 4)), dma((CHUNKS, 4)),
    ]
    if last:
        scratch += [dma((CHUNKS,))]
    else:
        scratch += [pltpu.VMEM((d, qd), BF16), pltpu.VMEM((d, kd), BF16), pltpu.VMEM((d, kd), BF16)]
    return pl.pallas_call(
        functools.partial(mlp_kernel, layer, last),
        in_specs=in_specs,
        out_specs=out_specs,
        out_shape=out_shape,
        scratch_shapes=scratch,
        compiler_params=pltpu.CompilerParams(
            vmem_limit_bytes=56 * 1024 * 1024, collective_id=layer, has_side_effects=True),
        name=f"sums_and_mlp_{layer}",
    )(*args)


def solution(mesh):
    row_spec = P('dp', None)
    pos_spec = P('dp')
    cache_spec = P(None, 'dp', None, 'tp', None)
    norm_spec = P(None, None)
    col_spec = P(None, None, 'tp')
    split_rows = P(None, 'tp', None)

    def local_step(hidden, positions, k_cache, v_cache, attn_norm, w_query, w_key, w_value, w_out, mlp_norm, w_gate, w_up, w_down):
        layers, batch, seq, _, head = k_cache.shape
        d = hidden.shape[1]
        own = batch // (8 * CHUNKS)
        kc = k_cache.reshape(layers, batch, seq, head)
        vc = v_cache.reshape(layers, batch, seq, head)
        cos_tab, sin_tab = rope_tables(positions, head)
        cos2 = jnp.concatenate([cos_tab, cos_tab], axis=1)
        sin2 = jnp.concatenate([-sin_tab, sin_tab], axis=1)
        posr = jnp.broadcast_to(positions.reshape(batch // 8, 1, 8), (batch // 8, 4, 8)).reshape(batch * 4, 1)
        qkv = first_qkv(hidden, attn_norm, w_query, w_key, w_value)
        x = hidden.reshape(CHUNKS, 2, 4, own, d)
        k_out = v_out = None
        for layer in range(layers):
            o, k_out, v_out = attention(layer, qkv, cos2, sin2, posr, positions, kc, vc, k_out, v_out)
            last = layer == layers - 1
            res = sums_and_mlp(layer, last, o, x, mlp_norm, attn_norm, w_out, w_gate, w_up, w_down, w_query, w_key, w_value)
            if last:
                hidden_out = res.reshape(batch, d)
            else:
                qkv, x = res
        return hidden_out, k_out.reshape(k_cache.shape), v_out.reshape(v_cache.shape)

    return jax.shard_map(local_step, mesh=mesh, in_specs=(row_spec, pos_spec, cache_spec, cache_spec, norm_spec, col_spec, col_spec, col_spec, split_rows, norm_spec, col_spec, col_spec, split_rows), out_specs=(row_spec, cache_spec, cache_spec), check_vma=False)
```

```python
import functools
import math

import jax
import jax.numpy as jnp
from jax import lax
from jax.experimental import pallas as pl
from jax.experimental.pallas import tpu as pltpu
from jax.sharding import PartitionSpec as P

F32 = jnp.float32
BF16 = jnp.bfloat16
MESH = pl.DeviceIdType.MESH
VMEM_BYTES = 64 * 1024 * 1024 - 128 * 1024
EPS = 1e-5


def rope_tables(positions, head_dim):
    half_dim = head_dim // 2
    inv_freq = jnp.power(500000.0, -jnp.arange(half_dim, dtype=jnp.float32) * (2.0 / head_dim))
    wavelen = (2.0 * math.pi) / inv_freq
    smooth = (8192.0 / wavelen - 1.0) / 3.0
    blended = (1.0 - smooth) * inv_freq / 8.0 + smooth * inv_freq
    scaled = jnp.where(wavelen < 2048.0, inv_freq, jnp.where(wavelen > 8192.0, inv_freq / 8.0, blended))
    angles = positions.astype(jnp.float32)[:, None] * scaled[None, :]
    return jnp.cos(angles), jnp.sin(angles)


def normed(x, gain):
    xf = x.astype(F32)
    mean_sq = jnp.mean(xf * xf, axis=-1, keepdims=True)
    return (xf * lax.rsqrt(mean_sq + EPS) * gain).astype(BF16)


def first_qkv_kernel(x_hbm, g_ref, wq_hbm, wk_hbm, wv_hbm, o_ref, h_ref, wq, wk, wv, sem):
    rows = h_ref.shape[0]
    qd = wq.shape[1]
    kd = wk.shape[1]
    copies = [pltpu.make_async_copy(src, dst, sem.at[i]) for i, (src, dst) in enumerate(
        [(x_hbm, h_ref), (wq_hbm.at[0], wq), (wk_hbm.at[0], wk), (wv_hbm.at[0], wv)])]
    for cp in copies:
        cp.start()
    gain = g_ref[0:1, :].astype(F32)
    copies[0].wait()

    @pl.loop(0, rows // 16)
    def _(i):
        sl = pl.ds(pl.multiple_of(i * 16, 16), 16)
        h_ref[sl, :] = normed(h_ref[sl, :], gain)

    h = h_ref[...]
    copies[1].wait()
    o_ref[:, 0:qd] = jnp.dot(h, wq[...], preferred_element_type=F32).astype(BF16)
    copies[2].wait()
    o_ref[:, qd:qd + kd] = jnp.dot(h, wk[...], preferred_element_type=F32).astype(BF16)
    copies[3].wait()
    o_ref[:, qd + kd:] = jnp.dot(h, wv[...], preferred_element_type=F32).astype(BF16)


def first_qkv(hidden, attn_norm, w_query, w_key, w_value):
    rows, d = hidden.shape
    qd, kd = w_query.shape[2], w_key.shape[2]
    vmem = pl.BlockSpec(memory_space=pltpu.VMEM)
    hbm = pl.BlockSpec(memory_space=pl.ANY)
    return pl.pallas_call(
        first_qkv_kernel,
        in_specs=[hbm, vmem, hbm, hbm, hbm],
        out_specs=vmem,
        out_shape=jax.ShapeDtypeStruct((rows, qd + 2 * kd), BF16),
        scratch_shapes=[pltpu.VMEM((rows, d), BF16), pltpu.VMEM((d, qd), BF16), pltpu.VMEM((d, kd), BF16),
                        pltpu.VMEM((d, kd), BF16), pltpu.SemaphoreType.DMA((4,))],
        compiler_params=pltpu.CompilerParams(vmem_limit_bytes=VMEM_BYTES),
        name="first_qkv",
    )(hidden, attn_norm, w_query, w_key, w_value)


BLOCK = 32


def attend_block(qkv, cos, sin, posr, pos_at, k_at, v_at, k_put, v_put):
    head = cos.shape[1]
    seq = k_at(0).shape[0]
    heads = qkv.shape[1] // head - 2
    scale = head ** -0.5

    def rope(vec):
        vec = vec.astype(F32)
        return vec * cos + pltpu.roll(vec, head // 2, 1) * sin

    qs = [rope(qkv[:, h * head:(h + 1) * head]) for h in range(heads)]
    kn = rope(qkv[:, heads * head:(heads + 1) * head])
    vn = qkv[:, (heads + 1) * head:(heads + 2) * head].astype(F32)

    tiles = (seq // 16, 16, head)
    seq_ids = lax.broadcasted_iota(jnp.int32, tiles, 0) * 16 + lax.broadcasted_iota(jnp.int32, tiles, 1)
    seq_bf = seq_ids.astype(F32).astype(BF16)
    row_of = lax.broadcasted_iota(jnp.int32, (32, head), 0) % 8
    lane = lax.broadcasted_iota(jnp.int32, (32, seq), 1)

    def updated(cache, row, b):
        here = seq_bf == jnp.full((16, head), pos_at(b).astype(F32), F32).astype(BF16)[None]
        row = jnp.broadcast_to(row, (16, head)).astype(BF16)[None]
        return jnp.where(here, row, cache.reshape(tiles)).reshape(seq, head)

    all_scores = []
    for j in range(BLOCK // 8):
        pieces = [q[8 * j:8 * j + 8] for q in qs] + [jnp.zeros((8, head), F32)] * (4 - heads)
        qj = jnp.concatenate(pieces, axis=0).astype(BF16)
        scores = None
        for b8 in range(8):
            b = 8 * j + b8
            k_b = updated(k_at(b), kn[b:b + 1], b)
            if k_put is not None:
                k_put(b, k_b)
            s_b = lax.dot_general(qj, k_b, (((1,), (1,)), ((), ())), preferred_element_type=F32)
            scores = s_b if scores is None else jnp.where(row_of == b8, s_b, scores)
        all_scores.append(scores)
    probs = []
    for j in range(BLOCK // 8):
        scores = jnp.where(lane <= posr[32 * j:32 * j + 32, :], all_scores[j] * scale, -jnp.inf)
        peak = jnp.max(scores, axis=1, keepdims=True)
        weight = jnp.exp(scores - peak)
        total = jnp.sum(weight, axis=1, keepdims=True)
        probs.append((weight * (1.0 / total)).astype(BF16))
    outs = []
    for j in range(BLOCK // 8):
        mixed = None
        for b8 in range(8):
            b = 8 * j + b8
            v_b = updated(v_at(b), vn[b:b + 1], b)
            if v_put is not None:
                v_put(b, v_b)
            o_b = jnp.dot(probs[j], v_b, preferred_element_type=F32)
            mixed = o_b if mixed is None else jnp.where(row_of == b8, o_b, mixed)
        outs.append(mixed)
    o = [jnp.concatenate([m[8 * h:8 * h + 8] for m in outs], axis=0).astype(BF16) for h in range(heads)]
    return o, kn, vn


def attention_kernel(pos_s, qkv_ref, cos_ref, sin_ref, posr_ref, k_ref, v_ref, *rest):
    o_ref, ko_ref, vo_ref = rest[-3:]
    step = pl.program_id(0)
    head = k_ref.shape[3]

    def k_put(b, value):
        ko_ref[0, b] = value

    def v_put(b, value):
        vo_ref[0, b] = value

    o, _, _ = attend_block(
        qkv_ref[...], cos_ref[...], sin_ref[...], posr_ref[...], lambda b: pos_s[step * BLOCK + b],
        lambda b: k_ref[0, b], lambda b: v_ref[0, b], k_put, v_put)
    for h, o_h in enumerate(o):
        o_ref[:, h * head:(h + 1) * head] = o_h


def attention(layer, qkv, cos2, sin2, posr, positions, k_cache, v_cache, k_prev, v_prev):
    layers, batch, seq, head = k_cache.shape
    qd = qkv.shape[1] - 2 * head
    cache_spec = pl.BlockSpec((1, BLOCK, seq, head), lambda i, p: (layer, i, 0, 0))
    row_spec = lambda width: pl.BlockSpec((BLOCK, width), lambda i, p: (i, 0))
    in_specs = [
        row_spec(qkv.shape[1]), row_spec(head), row_spec(head),
        pl.BlockSpec((BLOCK * 4, 1), lambda i, p: (i, 0)),
        cache_spec, cache_spec,
    ]
    args = [qkv, cos2, sin2, posr, k_cache, v_cache]
    aliases = {}
    if k_prev is not None:
        in_specs += [pl.BlockSpec(memory_space=pl.ANY)] * 2
        args += [k_prev, v_prev]
        aliases = {7: 1, 8: 2}
    return pl.pallas_call(
        attention_kernel,
        grid_spec=pltpu.PrefetchScalarGridSpec(
            num_scalar_prefetch=1,
            grid=(batch // BLOCK,),
            in_specs=in_specs,
            out_specs=[row_spec(qd), cache_spec, cache_spec],
        ),
        out_shape=[
            jax.ShapeDtypeStruct((batch, qd), BF16),
            jax.ShapeDtypeStruct(k_cache.shape, BF16),
            jax.ShapeDtypeStruct(v_cache.shape, BF16),
        ],
        input_output_aliases=aliases,
        compiler_params=pltpu.CompilerParams(vmem_limit_bytes=VMEM_BYTES),
        name=f"attention_{layer}",
    )(positions, *args)


CHUNKS = 2


def mlp_kernel(layer, last, *refs):
    refs = list(refs)
    o_ref, x_hbm, gm_ref, ga_ref, wo_hbm, wg_hbm, wu_hbm, wd_hbm = refs[:8]
    refs = refs[8:]
    if last:
        x_out = refs[0]
        refs = refs[1:]
    else:
        wq_hbm, wk_hbm, wv_hbm, qkv_out, xres_out = refs[:5]
        refs = refs[5:]
    (wo, wg, wu, wd, xres, part, hbuf, abuf, d2d_in, rs_out, rs_in, acc, w_sem, x_sem,
     d2d_s, d2d_r, rs_s, rs_r, ag_s, ag_r, fw_s, fw_r) = refs[:22]
    refs = refs[22:]
    if last:
        (out_sem,) = refs
    else:
        wq, wk, wv = refs

    chunks, _, chips_n, own, d = part.shape
    rows = 8 * own
    ff = wg.shape[1]
    me = lax.axis_index("tp")
    group = lax.axis_index("dp")
    core = me % 2
    chip = me // 2
    chips = [chip, chip + 1 - 2 * (chip % 2), (chip + 2) % 4, 3 - chip]
    partner = (group, chip * 2 + 1 - core)
    peers = [None] + [(group, chips[k] * 2 + core) for k in (1, 2, 3)]
    order = (3, 1, 2)

    loads = [(wo_hbm, wo), (wg_hbm, wg), (wu_hbm, wu), (wd_hbm, wd)]
    nxt = layer
    if not last:
        loads += [(wq_hbm, wq), (wk_hbm, wk), (wv_hbm, wv)]
    load = []
    for i, (src, dst) in enumerate(loads):
        which = layer if i < 4 else layer + 1
        cp = pltpu.make_async_copy(src.at[which], dst, w_sem.at[i])
        cp.start()
        load.append(cp)
    x_loads = []
    for hh in range(chunks):
        src = x_hbm.at[hh, core, chip] if layer == 0 else x_hbm.at[hh]
        cp = pltpu.make_async_copy(src, xres.at[hh], x_sem.at[hh])
        cp.start()
        x_loads.append(cp)

    barrier = pltpu.get_barrier_semaphore()
    for dev in [partner] + peers[1:]:
        pl.semaphore_signal(barrier, inc=1, device_id=dev, device_id_type=MESH)
    pl.semaphore_wait(barrier, 4)

    def remote(src, dst, s, r, dev):
        return pltpu.make_async_remote_copy(
            src_ref=src, dst_ref=dst, send_sem=s, recv_sem=r, device_id=dev, device_id_type=MESH)

    def d2d(hh):
        return remote(part.at[hh, 1 - core], d2d_in.at[hh], d2d_s.at[hh], d2d_r.at[hh], partner)

    def rs(hh, k):
        return remote(rs_out.at[hh, k - 1], rs_in.at[hh, k - 1], rs_s.at[hh, k - 1], rs_r.at[hh, k - 1], peers[k])

    def ag(hh, k):
        ref = hbuf.at[hh, core, chip]
        return remote(ref, ref, ag_s.at[hh, k - 1], ag_r.at[hh, k - 1], peers[k])

    def ag_in(hh, k):
        ref = hbuf.at[hh, core, chips[k]]
        return remote(ref, ref, ag_s.at[hh, k - 1], ag_r.at[hh, k - 1], peers[k])

    def fw(hh, k):
        ref = hbuf.at[hh, core, chips[k]]
        return remote(ref, ref, fw_s.at[hh, k], fw_r.at[hh, k], partner)

    def fw_in(hh, k):
        ref = hbuf.at[hh, 1 - core, chips[k]]
        return remote(ref, ref, fw_s.at[hh, k], fw_r.at[hh, k], partner)

    def put_part(hh, cols, value):
        value = value.astype(BF16)
        for p in range(2):
            for c in range(4):
                at = (p * 4 + c) * own
                part[hh, p, c, :, cols] = value[at:at + own]

    def ph0(hh):
        d2d(hh).start()

    def ph1(hh):
        d2d(hh).wait_recv()
        for k in order:
            pair = part[hh, core, chips[k]].astype(F32) + d2d_in[hh, chips[k]].astype(F32)
            rs_out[hh, k - 1] = pair.astype(BF16)
            rs(hh, k).start()
        acc[hh] = part[hh, core, chip].astype(F32) + d2d_in[hh, chip].astype(F32)
        d2d(hh).wait_send()

    def ph2(hh, mode):
        for k in (1, 2, 3):
            rs(hh, k).wait_recv()
        total = acc[hh]
        for k in (1, 2, 3):
            total = total + rs_in[hh, k - 1].astype(F32)
        x = (xres[hh].astype(F32) + total.astype(BF16).astype(F32)).astype(BF16)
        if mode == "final":
            hbuf[hh, core, chip] = x
        else:
            xres[hh] = x
            gain = (gm_ref[layer:layer + 1, :] if mode == "mlp" else ga_ref[layer + 1:layer + 2, :]).astype(F32)
            hbuf[hh, core, chip] = normed(x, gain)
            if mode == "attn":
                xres_out[hh] = x
        for k in order:
            ag(hh, k).start()
        fw(hh, 0).start()
        for k in (1, 2, 3):
            rs(hh, k).wait_send()

    def ph3(hh):
        for k in (1, 2, 3):
            ag_in(hh, k).wait_recv()
            fw(hh, k).start()

    def ph4(hh):
        for k in range(4):
            fw_in(hh, k).wait_recv()
        for k in (1, 2, 3):
            ag(hh, k).wait_send()
        for k in range(4):
            fw(hh, k).wait_send()

    def out_product(hh):
        o = o_ref[hh * rows:(hh + 1) * rows, :]

        @pl.loop(0, d // 1024)
        def _(n):
            cols = pl.ds(pl.multiple_of(n * 1024, 1024), 1024)
            put_part(hh, cols, jnp.dot(o, wo[:, cols], preferred_element_type=F32))

    def gate_up(hh):
        h = hbuf[hh].reshape(rows, d)

        @pl.loop(0, ff // 256)
        def _(n):
            cols = pl.ds(pl.multiple_of(n * 256, 256), 256)
            g = jnp.dot(h, wg[:, cols], preferred_element_type=F32).astype(BF16).astype(F32)
            u = jnp.dot(h, wu[:, cols], preferred_element_type=F32).astype(BF16).astype(F32)
            abuf[:, cols] = (g * jax.nn.sigmoid(g) * u).astype(BF16)

    def down(hh):
        @pl.loop(0, d // 1024)
        def _(n):
            cols = pl.ds(pl.multiple_of(n * 1024, 1024), 1024)
            put_part(hh, cols, jnp.dot(abuf[...], wd[:, cols], preferred_element_type=F32))

    def next_qkv(hh):
        h = hbuf[hh].reshape(rows, d)
        qd, kd = wq.shape[1], wk.shape[1]
        at = slice(hh * rows, (hh + 1) * rows)
        qkv_out[at, 0:qd] = jnp.dot(h, wq[...], preferred_element_type=F32).astype(BF16)
        qkv_out[at, qd:qd + kd] = jnp.dot(h, wk[...], preferred_element_type=F32).astype(BF16)
        qkv_out[at, qd + kd:] = jnp.dot(h, wv[...], preferred_element_type=F32).astype(BF16)

    end = "final" if last else "attn"
    load[0].wait()
    for hh in range(chunks):
        out_product(hh)
        ph0(hh)
    for cp in x_loads:
        cp.wait()
    ph1(0)
    ph1(1)
    ph2(0, "mlp")
    ph2(1, "mlp")
    ph3(0)
    ph4(0)
    load[1].wait()
    load[2].wait()
    gate_up(0)
    ph3(1)
    load[3].wait()
    down(0)
    ph0(0)
    ph4(1)
    gate_up(1)
    ph1(0)
    down(1)
    ph0(1)
    ph1(1)
    ph2(0, end)
    ph2(1, end)
    if last:
        def put(hh):
            return pltpu.make_async_copy(hbuf.at[hh], x_out.at[hh], out_sem.at[hh])
        ph3(0)
        ph4(0)
        put(0).start()
        ph3(1)
        ph4(1)
        put(1).start()
        put(0).wait()
        put(1).wait()
    else:
        ph3(0)
        ph4(0)
        for i in (4, 5, 6):
            load[i].wait()
        next_qkv(0)
        ph3(1)
        ph4(1)
        next_qkv(1)


def sums_and_mlp(layer, last, o, x, mlp_norm, attn_norm, w_out, w_gate, w_up, w_down, w_query, w_key, w_value):
    batch, qd = o.shape
    d = w_out.shape[2]
    ff = w_gate.shape[2]
    kd = w_key.shape[2]
    own = batch // (8 * CHUNKS)
    rows = 8 * own
    vmem = pl.BlockSpec(memory_space=pltpu.VMEM)
    hbm = pl.BlockSpec(memory_space=pl.ANY)
    args = [o, x, mlp_norm, attn_norm, w_out, w_gate, w_up, w_down]
    in_specs = [vmem, hbm, vmem, vmem] + [hbm] * 4
    if last:
        out_shape = jax.ShapeDtypeStruct((CHUNKS, 2, 4, own, d), BF16)
        out_specs = hbm
    else:
        args += [w_query, w_key, w_value]
        in_specs += [hbm] * 3
        out_shape = [jax.ShapeDtypeStruct((batch, qd + 2 * kd), BF16), jax.ShapeDtypeStruct((CHUNKS, own, d), BF16)]
        out_specs = [vmem, vmem]
    dma = pltpu.SemaphoreType.DMA
    scratch = [
        pltpu.VMEM((qd, d), BF16), pltpu.VMEM((d, ff), BF16), pltpu.VMEM((d, ff), BF16), pltpu.VMEM((ff, d), BF16),
        pltpu.VMEM((CHUNKS, own, d), BF16),
        pltpu.VMEM((CHUNKS, 2, 4, own, d), BF16),
        pltpu.VMEM((CHUNKS, 2, 4, own, d), BF16),
        pltpu.VMEM((rows, ff), BF16),
        pltpu.VMEM((CHUNKS, 4, own, d), BF16),
        pltpu.VMEM((CHUNKS, 3, own, d), BF16),
        pltpu.VMEM((CHUNKS, 3, own, d), BF16),
        pltpu.VMEM((CHUNKS, own, d), F32),
        dma((7,)), dma((CHUNKS,)),
        dma((CHUNKS,)), dma((CHUNKS,)),
        dma((CHUNKS, 3)), dma((CHUNKS, 3)),
        dma((CHUNKS, 3)), dma((CHUNKS, 3)),
        dma((CHUNKS, 4)), dma((CHUNKS, 4)),
    ]
    if last:
        scratch += [dma((CHUNKS,))]
    else:
        scratch += [pltpu.VMEM((d, qd), BF16), pltpu.VMEM((d, kd), BF16), pltpu.VMEM((d, kd), BF16)]
    return pl.pallas_call(
        functools.partial(mlp_kernel, layer, last),
        in_specs=in_specs,
        out_specs=out_specs,
        out_shape=out_shape,
        scratch_shapes=scratch,
        compiler_params=pltpu.CompilerParams(
            vmem_limit_bytes=VMEM_BYTES, collective_id=layer, has_side_effects=True),
        name=f"sums_and_mlp_{layer}",
    )(*args)


def solution(mesh):
    row_spec = P('dp', None)
    pos_spec = P('dp')
    cache_spec = P(None, 'dp', None, 'tp', None)
    norm_spec = P(None, None)
    col_spec = P(None, None, 'tp')
    split_rows = P(None, 'tp', None)

    def local_step(hidden, positions, k_cache, v_cache, attn_norm, w_query, w_key, w_value, w_out, mlp_norm, w_gate, w_up, w_down):
        layers, batch, seq, _, head = k_cache.shape
        d = hidden.shape[1]
        own = batch // (8 * CHUNKS)
        kc = k_cache.reshape(layers, batch, seq, head)
        vc = v_cache.reshape(layers, batch, seq, head)
        cos_tab, sin_tab = rope_tables(positions, head)
        cos2 = jnp.concatenate([cos_tab, cos_tab], axis=1)
        sin2 = jnp.concatenate([-sin_tab, sin_tab], axis=1)
        posr = jnp.broadcast_to(positions.reshape(batch // 8, 1, 8), (batch // 8, 4, 8)).reshape(batch * 4, 1)
        qkv = first_qkv(hidden, attn_norm, w_query, w_key, w_value)
        x = hidden.reshape(CHUNKS, 2, 4, own, d)
        k_out = v_out = None
        for layer in range(layers):
            o, k_out, v_out = attention(layer, qkv, cos2, sin2, posr, positions, kc, vc, k_out, v_out)
            last = layer == layers - 1
            res = sums_and_mlp(layer, last, o, x, mlp_norm, attn_norm, w_out, w_gate, w_up, w_down, w_query, w_key, w_value)
            if last:
                hidden_out = res.reshape(batch, d)
            else:
                qkv, x = res
        return hidden_out, k_out.reshape(k_cache.shape), v_out.reshape(v_cache.shape)

    return jax.shard_map(local_step, mesh=mesh, in_specs=(row_spec, pos_spec, cache_spec, cache_spec, norm_spec, col_spec, col_spec, col_spec, split_rows, norm_spec, col_spec, col_spec, split_rows), out_specs=(row_spec, cache_spec, cache_spec), check_vma=False)
```

```python
import functools
import math

import jax
import jax.numpy as jnp
import numpy as np
from jax import lax
from jax.experimental import pallas as pl
from jax.experimental.pallas import tpu as pltpu
from jax.sharding import PartitionSpec as P

F32 = jnp.float32
BF16 = jnp.bfloat16
MESH = pl.DeviceIdType.MESH
VMEM_BYTES = 64 * 1024 * 1024 - 128 * 1024
EPS = 1e-5


def rope_rows(head_dim):
    half_dim = head_dim // 2
    f32 = np.float32
    inv_freq = np.power(f32(500000.0), -np.arange(half_dim, dtype=f32) * f32(2.0 / head_dim))
    wavelen = f32(2.0 * math.pi) / inv_freq
    smooth = (f32(8192.0) / wavelen - f32(1.0)) / f32(3.0)
    blended = (f32(1.0) - smooth) * inv_freq / f32(8.0) + smooth * inv_freq
    scaled = np.where(wavelen < 2048.0, inv_freq, np.where(wavelen > 8192.0, inv_freq / f32(8.0), blended)).astype(f32)
    ones = np.ones(half_dim, f32)
    return np.stack([np.concatenate([scaled, scaled]), np.concatenate([-ones, ones])])


def normed(x, gain):
    xf = x.astype(F32)
    mean_sq = jnp.mean(xf * xf, axis=-1, keepdims=True)
    return (xf * lax.rsqrt(mean_sq + EPS) * gain).astype(BF16)


BLOCK = 32


def attend_block(qkv, cos, sin, posc, pos_at, k_at, v_at, k_put, v_put):
    head = cos.shape[1]
    seq = k_at(0).shape[0]
    heads = qkv.shape[1] // head - 2
    scale = head ** -0.5

    def rope(vec):
        vec = vec.astype(F32)
        return vec * cos + pltpu.roll(vec, head // 2, 1) * sin

    qs = [rope(qkv[:, h * head:(h + 1) * head]) for h in range(heads)]
    kn = rope(qkv[:, heads * head:(heads + 1) * head])
    vn = qkv[:, (heads + 1) * head:(heads + 2) * head].astype(F32)

    tiles = (seq // 16, 16, head)
    seq_ids = lax.broadcasted_iota(jnp.int32, tiles, 0) * 16 + lax.broadcasted_iota(jnp.int32, tiles, 1)
    seq_bf = seq_ids.astype(F32).astype(BF16)
    row_of = lax.broadcasted_iota(jnp.int32, (32, head), 0) % 8
    lane = lax.broadcasted_iota(jnp.int32, (32, seq), 1).astype(F32)

    def updated(cache, row, b):
        here = seq_bf == jnp.full((16, head), pos_at(b).astype(F32), F32).astype(BF16)[None]
        row = jnp.broadcast_to(row, (16, head)).astype(BF16)[None]
        return jnp.where(here, row, cache.reshape(tiles)).reshape(seq, head)

    all_scores = []
    for j in range(BLOCK // 8):
        pieces = [q[8 * j:8 * j + 8] for q in qs] + [jnp.zeros((8, head), F32)] * (4 - heads)
        qj = jnp.concatenate(pieces, axis=0).astype(BF16)
        scores = None
        for b8 in range(8):
            b = 8 * j + b8
            k_b = updated(k_at(b), kn[b:b + 1], b)
            if k_put is not None:
                k_put(b, k_b)
            s_b = lax.dot_general(qj, k_b, (((1,), (1,)), ((), ())), preferred_element_type=F32)
            scores = s_b if scores is None else jnp.where(row_of == b8, s_b, scores)
        all_scores.append(scores)
    probs = []
    for j in range(BLOCK // 8):
        limit = jnp.concatenate([posc[8 * j:8 * j + 8]] * 4, axis=0)
        scores = jnp.where(lane <= limit, all_scores[j] * scale, -jnp.inf)
        peak = jnp.max(scores, axis=1, keepdims=True)
        weight = jnp.exp(scores - peak)
        total = jnp.sum(weight, axis=1, keepdims=True)
        probs.append((weight * (1.0 / total)).astype(BF16))
    outs = []
    for j in range(BLOCK // 8):
        mixed = None
        for b8 in range(8):
            b = 8 * j + b8
            v_b = updated(v_at(b), vn[b:b + 1], b)
            if v_put is not None:
                v_put(b, v_b)
            o_b = jnp.dot(probs[j], v_b, preferred_element_type=F32)
            mixed = o_b if mixed is None else jnp.where(row_of == b8, o_b, mixed)
        outs.append(mixed)
    o = [jnp.concatenate([m[8 * h:8 * h + 8] for m in outs], axis=0).astype(BF16) for h in range(heads)]
    return o, kn, vn


def first_kernel(
    pos_s, x_hbm, g_hbm, wq_hbm, wk_hbm, wv_hbm, pos_ref, rope_ref, k_hbm, v_hbm,
    o_ref, cos_ref, sin_ref, posc_ref, ko_hbm, vo_hbm,
    h_ref, g_ref, wq, wk, wv, qkv_ref, kbuf, vbuf, sem, in_sem, out_sem,
):
    rows = h_ref.shape[0]
    qd = wq.shape[1]
    kd = wk.shape[1]
    blocks = rows // BLOCK
    copies = [pltpu.make_async_copy(src, dst, sem.at[i]) for i, (src, dst) in enumerate(
        [(x_hbm, h_ref), (g_hbm, g_ref), (wq_hbm.at[0], wq), (wk_hbm.at[0], wk), (wv_hbm.at[0], wv)])]
    for cp in copies:
        cp.start()

    def reads(i):
        at = pl.ds(i * BLOCK, BLOCK)
        return (pltpu.make_async_copy(k_hbm.at[0, at], kbuf.at[at], in_sem.at[0, i]),
                pltpu.make_async_copy(v_hbm.at[0, at], vbuf.at[at], in_sem.at[1, i]))

    def writes(i):
        at = pl.ds(i * BLOCK, BLOCK)
        return (pltpu.make_async_copy(kbuf.at[at], ko_hbm.at[0, at], out_sem.at[0, i]),
                pltpu.make_async_copy(vbuf.at[at], vo_hbm.at[0, at], out_sem.at[1, i]))

    for i in range(blocks):
        for cp in reads(i):
            cp.start()

    width = pos_ref.shape[1]
    diagonal = (lax.broadcasted_iota(jnp.int32, (width, width), 0) == lax.broadcasted_iota(jnp.int32, (width, width), 1))
    for i in range(rows // width):
        across = jnp.broadcast_to(pos_ref[i:i + 1, :].astype(F32), (width, width))
        down = jnp.sum(jnp.where(diagonal, across, 0.0), axis=1, keepdims=True)
        at = slice(i * width, (i + 1) * width)
        angles = down * rope_ref[0:1, :]
        posc_ref[at, :] = jnp.broadcast_to(down, (width, width))
        cos_ref[at, :] = jnp.cos(angles)
        sin_ref[at, :] = jnp.sin(angles) * rope_ref[1:2, :]

    copies[0].wait()
    copies[1].wait()
    gain = g_ref[0:1, :].astype(F32)

    @pl.loop(0, rows // 16)
    def _(i):
        sl = pl.ds(pl.multiple_of(i * 16, 16), 16)
        h_ref[sl, :] = normed(h_ref[sl, :], gain)

    h = h_ref[...]
    copies[2].wait()
    qkv_ref[:, 0:qd] = jnp.dot(h, wq[...], preferred_element_type=F32).astype(BF16)
    copies[3].wait()
    copies[4].wait()
    qkv_ref[:, qd:qd + kd] = jnp.dot(h, wk[...], preferred_element_type=F32).astype(BF16)
    qkv_ref[:, qd + kd:] = jnp.dot(h, wv[...], preferred_element_type=F32).astype(BF16)

    @pl.loop(0, blocks)
    def _(i):
        base = pl.multiple_of(i * BLOCK, BLOCK)
        at = pl.ds(base, BLOCK)
        for cp in reads(i):
            cp.wait()

        def k_put(b, value):
            kbuf[base + b] = value

        def v_put(b, value):
            vbuf[base + b] = value

        o, _, _ = attend_block(
            qkv_ref[at, :], cos_ref[at, :], sin_ref[at, :], posc_ref[at, :], lambda b: pos_s[base + b],
            lambda b: kbuf[base + b], lambda b: vbuf[base + b], k_put, v_put)
        for n, o_n in enumerate(o):
            o_ref[at, n * kd:(n + 1) * kd] = o_n
        for cp in writes(i):
            cp.start()

    for i in range(blocks):
        for cp in writes(i):
            cp.wait()


def first(hidden, attn_norm, w_query, w_key, w_value, positions, k_cache, v_cache):
    rows, d = hidden.shape
    qd, kd = w_query.shape[2], w_key.shape[2]
    seq = k_cache.shape[2]
    blocks = rows // BLOCK
    vmem = pl.BlockSpec(memory_space=pltpu.VMEM)
    hbm = pl.BlockSpec(memory_space=pl.ANY)
    dma = pltpu.SemaphoreType.DMA
    table = jax.ShapeDtypeStruct((rows, kd), F32)
    cache = jax.ShapeDtypeStruct(k_cache.shape, BF16)
    return pl.pallas_call(
        first_kernel,
        in_specs=[pl.BlockSpec(memory_space=pltpu.SMEM)] + [hbm] * 5 + [vmem, vmem, hbm, hbm],
        out_specs=[vmem] * 4 + [hbm, hbm],
        out_shape=[jax.ShapeDtypeStruct((rows, qd), BF16), table, table, table, cache, cache],
        scratch_shapes=[
            pltpu.VMEM((rows, d), BF16), pltpu.VMEM(attn_norm.shape, BF16), pltpu.VMEM((d, qd), BF16),
            pltpu.VMEM((d, kd), BF16), pltpu.VMEM((d, kd), BF16), pltpu.VMEM((rows, qd + 2 * kd), BF16),
            pltpu.VMEM((rows, seq, kd), BF16), pltpu.VMEM((rows, seq, kd), BF16),
            dma((5,)), dma((2, blocks)), dma((2, blocks)),
        ],
        compiler_params=pltpu.CompilerParams(vmem_limit_bytes=VMEM_BYTES),
        name="first",
    )(positions, hidden, attn_norm, w_query, w_key, w_value, positions.reshape(rows // kd, kd),
      jnp.asarray(rope_rows(kd)), k_cache, v_cache)


def cache_kernel(layer, pos_s, kn_ref, vn_ref, k_hbm, v_hbm, k_prev, v_prev, ko_hbm, vo_hbm, kbuf, vbuf, in_sem, out_sem):
    batch, seq, head = kbuf.shape
    blocks = batch // BLOCK

    def reads(i):
        at = pl.ds(i * BLOCK, BLOCK)
        return (pltpu.make_async_copy(k_hbm.at[layer, at], kbuf.at[at], in_sem.at[0, i]),
                pltpu.make_async_copy(v_hbm.at[layer, at], vbuf.at[at], in_sem.at[1, i]))

    def writes(i):
        at = pl.ds(i * BLOCK, BLOCK)
        return (pltpu.make_async_copy(kbuf.at[at], ko_hbm.at[layer, at], out_sem.at[0, i]),
                pltpu.make_async_copy(vbuf.at[at], vo_hbm.at[layer, at], out_sem.at[1, i]))

    for i in range(blocks):
        for cp in reads(i):
            cp.start()
    row_of = lax.broadcasted_iota(jnp.int32, (16, head), 0)

    @pl.loop(0, blocks)
    def _(i):
        base = pl.multiple_of(i * BLOCK, BLOCK)
        at = pl.ds(base, BLOCK)
        new_rows = [(ref[at, :].astype(F32), buf) for ref, buf in ((kn_ref, kbuf), (vn_ref, vbuf))]
        for cp in reads(i):
            cp.wait()
        for b in range(BLOCK):
            pos = pos_s[base + b]
            tile = pl.ds(pl.multiple_of(pos // 16 * 16, 16), 16)
            here = row_of == pos % 16
            for rows, buf in new_rows:
                old = buf[base + b, tile, :].astype(F32)
                buf[base + b, tile, :] = jnp.where(here, rows[b:b + 1], old).astype(BF16)
        for cp in writes(i):
            cp.start()

    for i in range(blocks):
        for cp in writes(i):
            cp.wait()


def write_cache(layer, positions, k_rows, v_rows, k_cache, v_cache, k_prev, v_prev):
    layers, batch, seq, head = k_cache.shape
    blocks = batch // BLOCK
    vmem = pl.BlockSpec(memory_space=pltpu.VMEM)
    hbm = pl.BlockSpec(memory_space=pl.ANY)
    dma = pltpu.SemaphoreType.DMA
    return pl.pallas_call(
        functools.partial(cache_kernel, layer),
        in_specs=[pl.BlockSpec(memory_space=pltpu.SMEM), vmem, vmem] + [hbm] * 4,
        out_specs=[hbm, hbm],
        out_shape=[jax.ShapeDtypeStruct(k_cache.shape, BF16), jax.ShapeDtypeStruct(v_cache.shape, BF16)],
        input_output_aliases={5: 0, 6: 1},
        scratch_shapes=[pltpu.VMEM((batch, seq, head), BF16), pltpu.VMEM((batch, seq, head), BF16),
                        dma((2, blocks)), dma((2, blocks))],
        compiler_params=pltpu.CompilerParams(vmem_limit_bytes=VMEM_BYTES),
        name="write_cache",
    )(positions, k_rows, v_rows, k_cache, v_cache, k_prev, v_prev)


CHUNKS = 4

ORDER = (
    "O00O01O02O03P00P01P02S00P03S01S02F00",
    "G00D00F01S03P10G01F02D01G02P11F03D02",
    "S10G03P12D03S11P13F10Q20A20S12B20F11",
    "O20S13Q21P20A21F12B21O21Q22F13A22P21",
    "S20B22O22Q23A23P22B23S21O23F20P23G20",
    "D20S22F21P30G21D21S23F22P31G22S30D22",
    "F23P32G23S31D23F30P33S32E30F31E31S33",
    "F32E32F33E33",
)


def body_kernel(
    pos_s, o_hbm, x_hbm, gm_hbm, ga_hbm, wo_hbm, wg_hbm, wu_hbm, wd_hbm, wq_hbm, wk_hbm, wv_hbm, k_hbm, v_hbm,
    cos_hbm, sin_hbm, posc_hbm,
    x_out, kn_out, vn_out,
    wo, wg, wu, wd, wq, wk, wv, kbuf, vbuf, o_s, xres, part, hbuf, hst, abuf, qkv_s, d2d_in, rs_out, rs_in, acc,
    gm, ga, cos, sin, posc,
    w_sem, x_sem, kv_sem, t_sem, out_sem, d2d_s, d2d_r, rs_s, rs_r, ag_s, ag_r, fw_s, fw_r,
):
    chunks, _, _, own, d = part.shape
    rows = 8 * own
    ff = wg.shape[1]
    head = kbuf.shape[2]
    me = lax.axis_index("tp")
    group = lax.axis_index("dp")
    core = me % 2
    chip = me // 2
    chips = [chip, chip + 1 - 2 * (chip % 2), (chip + 2) % 4, 3 - chip]
    partner = (group, chip * 2 + 1 - core)
    peers = [None] + [(group, chips[k] * 2 + core) for k in (1, 2, 3)]
    order = (3, 1, 2)

    loads = {}

    def load(name, src, dst, sem):
        loads[name] = pltpu.make_async_copy(src, dst, sem)
        loads[name].start()

    def need(*names):
        for name in names:
            if name in loads:
                loads.pop(name).wait()

    load("o", o_hbm, o_s, t_sem.at[0])
    load("wo", wo_hbm.at[0], wo, w_sem.at[0])
    load("gm", gm_hbm, gm, t_sem.at[1])
    for q in range(chunks):
        load(("x", q), x_hbm.at[q, core, chip], xres.at[q], x_sem.at[q])
    load("wg", wg_hbm.at[0], wg, w_sem.at[1])
    load("wu", wu_hbm.at[0], wu, w_sem.at[2])
    load("wd", wd_hbm.at[0], wd, w_sem.at[3])
    load("ga", ga_hbm, ga, t_sem.at[2])
    load("wq", wq_hbm.at[1], wq, w_sem.at[4])
    load("wk", wk_hbm.at[1], wk, w_sem.at[5])
    load("wv", wv_hbm.at[1], wv, w_sem.at[6])
    load("cos", cos_hbm, cos, t_sem.at[3])
    load("sin", sin_hbm, sin, t_sem.at[4])
    load("posc", posc_hbm, posc, t_sem.at[5])

    def load_kv(i):
        at = pl.ds(i * BLOCK, BLOCK)
        load(("k", i), k_hbm.at[1, at], kbuf.at[at], kv_sem.at[0, i])
        load(("v", i), v_hbm.at[1, at], vbuf.at[at], kv_sem.at[1, i])

    barrier = pltpu.get_barrier_semaphore()
    for dev in [partner] + peers[1:]:
        pl.semaphore_signal(barrier, inc=1, device_id=dev, device_id_type=MESH)
    pl.semaphore_wait(barrier, 4)

    def remote(src, dst, s, r, dev):
        return pltpu.make_async_remote_copy(
            src_ref=src, dst_ref=dst, send_sem=s, recv_sem=r, device_id=dev, device_id_type=MESH)

    def d2d(q):
        return remote(part.at[q, 1 - core], d2d_in.at[q], d2d_s.at[q], d2d_r.at[q], partner)

    def rs(q, k):
        return remote(rs_out.at[q, k - 1], rs_in.at[q, k - 1], rs_s.at[q, k - 1], rs_r.at[q, k - 1], peers[k])

    def ag(q, k):
        ref = hbuf.at[q, core, chip]
        return remote(ref, ref, ag_s.at[q, k - 1], ag_r.at[q, k - 1], peers[k])

    def ag_in(q, k):
        ref = hbuf.at[q, core, chips[k]]
        return remote(ref, ref, ag_s.at[q, k - 1], ag_r.at[q, k - 1], peers[k])

    def fw(q, k):
        ref = hbuf.at[q, core, chips[k]]
        return remote(ref, ref, fw_s.at[q, k], fw_r.at[q, k], partner)

    def fw_in(q, k):
        ref = hbuf.at[q, 1 - core, chips[k]]
        return remote(ref, ref, fw_s.at[q, k], fw_r.at[q, k], partner)

    def put_part(q, cols, value):
        for p in range(2):
            for c in range(4):
                at = (p * 4 + c) * own
                part[q, p, c, :, cols] = value[at:at + own].astype(BF16)

    def pair_sums(q):
        d2d(q).wait_recv()
        for k in order:
            pair = part[q, core, chips[k]].astype(F32) + d2d_in[q, chips[k]].astype(F32)
            rs_out[q, k - 1] = pair.astype(BF16)
            rs(q, k).start()
        acc[q] = part[q, core, chip].astype(F32) + d2d_in[q, chip].astype(F32)
        d2d(q).wait_send()

    def totals(a, q):
        for k in (1, 2, 3):
            rs(q, k).wait_recv()
        need(("x", q))
        total = acc[q]
        for k in (1, 2, 3):
            total = total + rs_in[q, k - 1].astype(F32)
        x = (xres[q].astype(F32) + total.astype(BF16).astype(F32)).astype(BF16)
        if a == 3:
            hbuf[q, core, chip] = x
        else:
            xres[q] = x
            if a == 1:
                need("ga")
                gain = ga[1:2, :]
            else:
                need("gm")
                gain = gm[a // 2:a // 2 + 1, :]
            hbuf[q, core, chip] = normed(x, gain.astype(F32))
        for k in order:
            ag(q, k).start()
        fw(q, 0).start()
        for k in (1, 2, 3):
            rs(q, k).wait_send()

    def forward(q):
        for k in (1, 2, 3):
            ag_in(q, k).wait_recv()
            fw(q, k).start()

    def gathered(q):
        for k in range(4):
            fw_in(q, k).wait_recv()
        for k in (1, 2, 3):
            ag(q, k).wait_send()
        for k in range(4):
            fw(q, k).wait_send()

    def stage(q):
        gathered(q)
        hst[...] = hbuf[q].reshape(rows, d)

    def out_product(a, q):
        need("o", "wo")

        @pl.loop(0, d // 1024)
        def _(n):
            cols = pl.ds(pl.multiple_of(n * 1024, 1024), 1024)
            put_part(q, cols, jnp.dot(o_s[q * rows:(q + 1) * rows, :], wo[:, cols], preferred_element_type=F32))

        d2d(q).start()

    def gate_up(q):
        stage(q)
        need("wg", "wu")

        @pl.loop(0, ff // 256)
        def _(n):
            cols = pl.ds(pl.multiple_of(n * 256, 256), 256)
            h = hst[...]
            g = jnp.dot(h, wg[:, cols], preferred_element_type=F32).astype(BF16).astype(F32)
            u = jnp.dot(h, wu[:, cols], preferred_element_type=F32).astype(BF16).astype(F32)
            abuf[q, :, cols] = (g * jax.nn.sigmoid(g) * u).astype(BF16)

    def down(q):
        need("wd")

        @pl.loop(0, d // 1024)
        def _(n):
            cols = pl.ds(pl.multiple_of(n * 1024, 1024), 1024)
            put_part(q, cols, jnp.dot(abuf[q], wd[:, cols], preferred_element_type=F32))

        d2d(q).start()

    def qkv(q):
        stage(q)
        need("wq", "wk", "wv")
        qd, kd = wq.shape[1], wk.shape[1]
        h = hst[...]
        qkv_s[q, :, 0:qd] = jnp.dot(h, wq[...], preferred_element_type=F32).astype(BF16)
        qkv_s[q, :, qd:qd + kd] = jnp.dot(h, wk[...], preferred_element_type=F32).astype(BF16)
        qkv_s[q, :, qd + kd:] = jnp.dot(h, wv[...], preferred_element_type=F32).astype(BF16)

    def attend(q, i):
        need("cos", "sin", "posc")
        for j in range(rows // BLOCK // 2):
            first = i * (rows // 2) + j * BLOCK
            block = (q * rows + first) // BLOCK
            need(("k", block), ("v", block))
            base = block * BLOCK
            at = slice(base, base + BLOCK)
            o, kn, vn = attend_block(
                qkv_s[q, first:first + BLOCK, :], cos[at, :], sin[at, :], posc[at, :], lambda b: pos_s[base + b],
                lambda b: kbuf[base + b], lambda b: vbuf[base + b], None, None)
            for h, o_h in enumerate(o):
                o_s[at, h * head:(h + 1) * head] = o_h
            kn_out[at, :] = kn.astype(BF16)
            vn_out[at, :] = vn.astype(BF16)

    def result(q):
        gathered(q)
        load(("out", q), hbuf.at[q], x_out.at[q], out_sem.at[q])

    steps = [line[i:i + 3] for line in ORDER for i in range(0, len(line), 3)]
    last = {name: max(i for i, s in enumerate(steps) if s[0] == name and s[1] == "0") for name in "OGD"}
    for i, code in enumerate(steps):
        name, a, q = code[0], int(code[1]), int(code[2])
        if name == "O":
            out_product(a, q)
        elif name == "P":
            pair_sums(q)
        elif name == "S":
            totals(a, q)
        elif name == "F":
            forward(q)
        elif name == "G":
            gate_up(q)
        elif name == "D":
            down(q)
        elif name == "Q":
            qkv(q)
        elif name in "AB":
            attend(q, "AB".index(name))
        else:
            result(q)
        if i == last["O"]:
            load("wo", wo_hbm.at[1], wo, w_sem.at[0])
            for j in range(kbuf.shape[0] // BLOCK):
                load_kv(j)
        if i == last["G"]:
            load("wg", wg_hbm.at[1], wg, w_sem.at[1])
            load("wu", wu_hbm.at[1], wu, w_sem.at[2])
        if i == last["D"]:
            load("wd", wd_hbm.at[1], wd, w_sem.at[3])
    need(*[("out", q) for q in range(chunks)])


def body(positions, o, x, mlp_norm, attn_norm, w_out, w_gate, w_up, w_down, w_query, w_key, w_value, k_cache, v_cache, cos2, sin2, posc):
    batch, qd = o.shape
    d = w_out.shape[2]
    ff = w_gate.shape[2]
    kd = w_key.shape[2]
    seq = k_cache.shape[2]
    own = batch // (8 * CHUNKS)
    rows = 8 * own
    vmem = pl.BlockSpec(memory_space=pltpu.VMEM)
    hbm = pl.BlockSpec(memory_space=pl.ANY)
    dma = pltpu.SemaphoreType.DMA
    row = jax.ShapeDtypeStruct((batch, kd), BF16)
    return pl.pallas_call(
        body_kernel,
        in_specs=[pl.BlockSpec(memory_space=pltpu.SMEM)] + [hbm] * 16,
        out_specs=[hbm, vmem, vmem],
        out_shape=[jax.ShapeDtypeStruct((CHUNKS, 2, 4, own, d), BF16), row, row],
        scratch_shapes=[
            pltpu.VMEM((qd, d), BF16), pltpu.VMEM((d, ff), BF16), pltpu.VMEM((d, ff), BF16), pltpu.VMEM((ff, d), BF16),
            pltpu.VMEM((d, qd), BF16), pltpu.VMEM((d, kd), BF16), pltpu.VMEM((d, kd), BF16),
            pltpu.VMEM((batch, seq, kd), BF16), pltpu.VMEM((batch, seq, kd), BF16),
            pltpu.VMEM((batch, qd), BF16),
            pltpu.VMEM((CHUNKS, own, d), BF16),
            pltpu.VMEM((CHUNKS, 2, 4, own, d), BF16),
            pltpu.VMEM((CHUNKS, 2, 4, own, d), BF16),
            pltpu.VMEM((rows, d), BF16),
            pltpu.VMEM((CHUNKS, rows, ff), BF16),
            pltpu.VMEM((CHUNKS, rows, qd + 2 * kd), BF16),
            pltpu.VMEM((CHUNKS, 4, own, d), BF16),
            pltpu.VMEM((CHUNKS, 3, own, d), BF16),
            pltpu.VMEM((CHUNKS, 3, own, d), BF16),
            pltpu.VMEM((CHUNKS, own, d), F32),
            pltpu.VMEM(mlp_norm.shape, BF16), pltpu.VMEM(attn_norm.shape, BF16),
            pltpu.VMEM((batch, kd), F32), pltpu.VMEM((batch, kd), F32), pltpu.VMEM((batch, kd), F32),
            dma((7,)), dma((CHUNKS,)), dma((2, batch // BLOCK)), dma((6,)), dma((CHUNKS,)),
            dma((CHUNKS,)), dma((CHUNKS,)),
            dma((CHUNKS, 3)), dma((CHUNKS, 3)),
            dma((CHUNKS, 3)), dma((CHUNKS, 3)),
            dma((CHUNKS, 4)), dma((CHUNKS, 4)),
        ],
        compiler_params=pltpu.CompilerParams(vmem_limit_bytes=VMEM_BYTES, collective_id=0, has_side_effects=True),
        name="body",
    )(positions, o, x, mlp_norm, attn_norm, w_out, w_gate, w_up, w_down, w_query, w_key, w_value, k_cache, v_cache, cos2, sin2, posc)


def solution(mesh):
    row_spec = P('dp', None)
    pos_spec = P('dp')
    cache_spec = P(None, 'dp', None, 'tp', None)
    norm_spec = P(None, None)
    col_spec = P(None, None, 'tp')
    split_rows = P(None, 'tp', None)

    def local_step(hidden, positions, k_cache, v_cache, attn_norm, w_query, w_key, w_value, w_out, mlp_norm, w_gate, w_up, w_down):
        layers, batch, seq, _, head = k_cache.shape
        d = hidden.shape[1]
        own = batch // (8 * CHUNKS)
        kc = k_cache.reshape(layers, batch, seq, head)
        vc = v_cache.reshape(layers, batch, seq, head)
        o, cos2, sin2, posc, k_out, v_out = first(hidden, attn_norm, w_query, w_key, w_value, positions, kc, vc)
        x = hidden.reshape(CHUNKS, 2, 4, own, d)
        x_out, k_rows, v_rows = body(positions, o, x, mlp_norm, attn_norm, w_out, w_gate, w_up, w_down,
                                     w_query, w_key, w_value, kc, vc, cos2, sin2, posc)
        k_out, v_out = write_cache(1, positions, k_rows, v_rows, kc, vc, k_out, v_out)
        return x_out.reshape(batch, d), k_out.reshape(k_cache.shape), v_out.reshape(v_cache.shape)

    return jax.shard_map(local_step, mesh=mesh, in_specs=(row_spec, pos_spec, cache_spec, cache_spec, norm_spec, col_spec, col_spec, col_spec, split_rows, norm_spec, col_spec, col_spec, split_rows), out_specs=(row_spec, cache_spec, cache_spec), check_vma=False)
```

```python
import functools
import math

import jax
import jax.numpy as jnp
import numpy as np
from jax import lax
from jax.experimental import pallas as pl
from jax.experimental.pallas import tpu as pltpu
from jax.sharding import PartitionSpec as P

F32 = jnp.float32
BF16 = jnp.bfloat16
MESH = pl.DeviceIdType.MESH
VMEM_BYTES = 64 * 1024 * 1024 - 128 * 1024
EPS = 1e-5


def rope_rows(head_dim):
    half_dim = head_dim // 2
    f32 = np.float32
    inv_freq = np.power(f32(500000.0), -np.arange(half_dim, dtype=f32) * f32(2.0 / head_dim))
    wavelen = f32(2.0 * math.pi) / inv_freq
    smooth = (f32(8192.0) / wavelen - f32(1.0)) / f32(3.0)
    blended = (f32(1.0) - smooth) * inv_freq / f32(8.0) + smooth * inv_freq
    scaled = np.where(wavelen < 2048.0, inv_freq, np.where(wavelen > 8192.0, inv_freq / f32(8.0), blended)).astype(f32)
    ones = np.ones(half_dim, f32)
    return np.stack([np.concatenate([scaled, scaled]), np.concatenate([-ones, ones])])


def normed(x, gain):
    xf = x.astype(F32)
    mean_sq = jnp.mean(xf * xf, axis=-1, keepdims=True)
    return (xf * lax.rsqrt(mean_sq + EPS) * gain).astype(BF16)


BLOCK = 32


def attend_block(qkv, cos, sin, posc, pos_at, k_at, v_at, k_put, v_put):
    head = cos.shape[1]
    seq = k_at(0).shape[0]
    heads = qkv.shape[1] // head - 2
    scale = head ** -0.5

    def rope(vec):
        vec = vec.astype(F32)
        return vec * cos + pltpu.roll(vec, head // 2, 1) * sin

    qs = [rope(qkv[:, h * head:(h + 1) * head]) for h in range(heads)]
    kn = rope(qkv[:, heads * head:(heads + 1) * head])
    vn = qkv[:, (heads + 1) * head:(heads + 2) * head].astype(F32)

    tiles = (seq // 16, 16, head)
    seq_ids = lax.broadcasted_iota(jnp.int32, tiles, 0) * 16 + lax.broadcasted_iota(jnp.int32, tiles, 1)
    seq_bf = seq_ids.astype(F32).astype(BF16)
    row_of = lax.broadcasted_iota(jnp.int32, (32, head), 0) % 8
    lane = lax.broadcasted_iota(jnp.int32, (32, seq), 1).astype(F32)

    def updated(cache, row, b):
        here = seq_bf == jnp.full((16, head), pos_at(b).astype(F32), F32).astype(BF16)[None]
        row = jnp.broadcast_to(row, (16, head)).astype(BF16)[None]
        return jnp.where(here, row, cache.reshape(tiles)).reshape(seq, head)

    all_scores = []
    for j in range(BLOCK // 8):
        pieces = [q[8 * j:8 * j + 8] for q in qs] + [jnp.zeros((8, head), F32)] * (4 - heads)
        qj = jnp.concatenate(pieces, axis=0).astype(BF16)
        scores = None
        for b8 in range(8):
            b = 8 * j + b8
            k_b = updated(k_at(b), kn[b:b + 1], b)
            if k_put is not None:
                k_put(b, k_b)
            s_b = lax.dot_general(qj, k_b, (((1,), (1,)), ((), ())), preferred_element_type=F32)
            scores = s_b if scores is None else jnp.where(row_of == b8, s_b, scores)
        all_scores.append(scores)
    probs = []
    for j in range(BLOCK // 8):
        limit = jnp.concatenate([posc[8 * j:8 * j + 8]] * 4, axis=0)
        scores = jnp.where(lane <= limit, all_scores[j] * scale, -jnp.inf)
        peak = jnp.max(scores, axis=1, keepdims=True)
        weight = jnp.exp(scores - peak)
        total = jnp.sum(weight, axis=1, keepdims=True)
        probs.append((weight * (1.0 / total)).astype(BF16))
    outs = []
    for j in range(BLOCK // 8):
        mixed = None
        for b8 in range(8):
            b = 8 * j + b8
            v_b = updated(v_at(b), vn[b:b + 1], b)
            if v_put is not None:
                v_put(b, v_b)
            o_b = jnp.dot(probs[j], v_b, preferred_element_type=F32)
            mixed = o_b if mixed is None else jnp.where(row_of == b8, o_b, mixed)
        outs.append(mixed)
    o = [jnp.concatenate([m[8 * h:8 * h + 8] for m in outs], axis=0).astype(BF16) for h in range(heads)]
    return o, kn, vn


def first_kernel(
    pos_s, x_hbm, g_hbm, wq_hbm, wk_hbm, wv_hbm, pos_ref, rope_ref, k_hbm, v_hbm,
    o_ref, cos_ref, sin_ref, posc_ref, ko_hbm, vo_hbm,
    h_ref, g_ref, wq, wk, wv, qkv_ref, kbuf, vbuf, sem, in_sem, out_sem,
):
    rows = h_ref.shape[0]
    qd = wq.shape[1]
    kd = wk.shape[1]
    blocks = rows // BLOCK
    copies = [pltpu.make_async_copy(src, dst, sem.at[i]) for i, (src, dst) in enumerate(
        [(x_hbm, h_ref), (g_hbm, g_ref), (wq_hbm.at[0], wq), (wk_hbm.at[0], wk), (wv_hbm.at[0], wv)])]
    for cp in copies:
        cp.start()

    def reads(i):
        at = pl.ds(i * BLOCK, BLOCK)
        return (pltpu.make_async_copy(k_hbm.at[0, at], kbuf.at[at], in_sem.at[0, i]),
                pltpu.make_async_copy(v_hbm.at[0, at], vbuf.at[at], in_sem.at[1, i]))

    def writes(i):
        at = pl.ds(i * BLOCK, BLOCK)
        return (pltpu.make_async_copy(kbuf.at[at], ko_hbm.at[0, at], out_sem.at[0, i]),
                pltpu.make_async_copy(vbuf.at[at], vo_hbm.at[0, at], out_sem.at[1, i]))

    width = pos_ref.shape[1]
    diagonal = (lax.broadcasted_iota(jnp.int32, (width, width), 0) == lax.broadcasted_iota(jnp.int32, (width, width), 1))
    for i in range(rows // width):
        across = jnp.broadcast_to(pos_ref[i:i + 1, :].astype(F32), (width, width))
        down = jnp.sum(jnp.where(diagonal, across, 0.0), axis=1, keepdims=True)
        at = slice(i * width, (i + 1) * width)
        angles = down * rope_ref[0:1, :]
        posc_ref[at, :] = jnp.broadcast_to(down, (width, width))
        cos_ref[at, :] = jnp.cos(angles)
        sin_ref[at, :] = jnp.sin(angles) * rope_ref[1:2, :]

    copies[0].wait()
    copies[1].wait()
    for i in range(blocks):
        for cp in reads(i):
            cp.start()
    gain = g_ref[0:1, :].astype(F32)

    @pl.loop(0, rows // 16)
    def _(i):
        sl = pl.ds(pl.multiple_of(i * 16, 16), 16)
        h_ref[sl, :] = normed(h_ref[sl, :], gain)

    h = h_ref[...]
    copies[2].wait()
    qkv_ref[:, 0:qd] = jnp.dot(h, wq[...], preferred_element_type=F32).astype(BF16)
    copies[3].wait()
    copies[4].wait()
    qkv_ref[:, qd:qd + kd] = jnp.dot(h, wk[...], preferred_element_type=F32).astype(BF16)
    qkv_ref[:, qd + kd:] = jnp.dot(h, wv[...], preferred_element_type=F32).astype(BF16)

    @pl.loop(0, blocks)
    def _(i):
        base = pl.multiple_of(i * BLOCK, BLOCK)
        at = pl.ds(base, BLOCK)
        for cp in reads(i):
            cp.wait()

        def k_put(b, value):
            kbuf[base + b] = value

        def v_put(b, value):
            vbuf[base + b] = value

        o, _, _ = attend_block(
            qkv_ref[at, :], cos_ref[at, :], sin_ref[at, :], posc_ref[at, :], lambda b: pos_s[base + b],
            lambda b: kbuf[base + b], lambda b: vbuf[base + b], k_put, v_put)
        for n, o_n in enumerate(o):
            o_ref[at, n * kd:(n + 1) * kd] = o_n
        for cp in writes(i):
            cp.start()

    for i in range(blocks):
        for cp in writes(i):
            cp.wait()


def first(hidden, attn_norm, w_query, w_key, w_value, positions, k_cache, v_cache):
    rows, d = hidden.shape
    qd, kd = w_query.shape[2], w_key.shape[2]
    seq = k_cache.shape[2]
    blocks = rows // BLOCK
    vmem = pl.BlockSpec(memory_space=pltpu.VMEM)
    hbm = pl.BlockSpec(memory_space=pl.ANY)
    dma = pltpu.SemaphoreType.DMA
    table = jax.ShapeDtypeStruct((rows, kd), F32)
    cache = jax.ShapeDtypeStruct(k_cache.shape, BF16)
    return pl.pallas_call(
        first_kernel,
        in_specs=[pl.BlockSpec(memory_space=pltpu.SMEM)] + [hbm] * 5 + [vmem, vmem, hbm, hbm],
        out_specs=[vmem] * 4 + [hbm, hbm],
        out_shape=[jax.ShapeDtypeStruct((rows, qd), BF16), table, table, table, cache, cache],
        scratch_shapes=[
            pltpu.VMEM((rows, d), BF16), pltpu.VMEM(attn_norm.shape, BF16), pltpu.VMEM((d, qd), BF16),
            pltpu.VMEM((d, kd), BF16), pltpu.VMEM((d, kd), BF16), pltpu.VMEM((rows, qd + 2 * kd), BF16),
            pltpu.VMEM((rows, seq, kd), BF16), pltpu.VMEM((rows, seq, kd), BF16),
            dma((5,)), dma((2, blocks)), dma((2, blocks)),
        ],
        compiler_params=pltpu.CompilerParams(vmem_limit_bytes=VMEM_BYTES),
        name="first",
    )(positions, hidden, attn_norm, w_query, w_key, w_value, positions.reshape(rows // kd, kd),
      jnp.asarray(rope_rows(kd)), k_cache, v_cache)


def cache_kernel(
    layer, pos_s, kn_ref, vn_ref, x_hbm, k_hbm, v_hbm, k_prev, v_prev,
    x_out, ko_hbm, vo_hbm,
    kbuf, vbuf, xbuf, in_sem, out_sem, x_sem,
):
    batch, seq, head = kbuf.shape
    blocks = batch // BLOCK
    x_in = pltpu.make_async_copy(x_hbm, xbuf, x_sem.at[0])
    x_in.start()
    x_put = pltpu.make_async_copy(xbuf, x_out, x_sem.at[1])

    def reads(i):
        at = pl.ds(i * BLOCK, BLOCK)
        return (pltpu.make_async_copy(k_hbm.at[layer, at], kbuf.at[at], in_sem.at[0, i]),
                pltpu.make_async_copy(v_hbm.at[layer, at], vbuf.at[at], in_sem.at[1, i]))

    def writes(i):
        at = pl.ds(i * BLOCK, BLOCK)
        return (pltpu.make_async_copy(kbuf.at[at], ko_hbm.at[layer, at], out_sem.at[0, i]),
                pltpu.make_async_copy(vbuf.at[at], vo_hbm.at[layer, at], out_sem.at[1, i]))

    for i in range(blocks):
        for cp in reads(i):
            cp.start()
    row_of = lax.broadcasted_iota(jnp.int32, (16, head), 0)

    @pl.loop(0, blocks)
    def _(i):
        base = pl.multiple_of(i * BLOCK, BLOCK)
        at = pl.ds(base, BLOCK)
        new_rows = [(ref[at, :].astype(F32), buf) for ref, buf in ((kn_ref, kbuf), (vn_ref, vbuf))]
        for cp in reads(i):
            cp.wait()
        for b in range(BLOCK):
            pos = pos_s[base + b]
            tile = pl.ds(pl.multiple_of(pos // 16 * 16, 16), 16)
            here = row_of == pos % 16
            for rows, buf in new_rows:
                old = buf[base + b, tile, :].astype(F32)
                buf[base + b, tile, :] = jnp.where(here, rows[b:b + 1], old).astype(BF16)
        for cp in writes(i):
            cp.start()

    x_in.wait()
    x_put.start()
    for i in range(blocks):
        for cp in writes(i):
            cp.wait()
    x_put.wait()


def write_cache(layer, positions, k_rows, v_rows, x, k_cache, v_cache, k_prev, v_prev):
    layers, batch, seq, head = k_cache.shape
    blocks = batch // BLOCK
    vmem = pl.BlockSpec(memory_space=pltpu.VMEM)
    hbm = pl.BlockSpec(memory_space=pl.ANY)
    dma = pltpu.SemaphoreType.DMA
    return pl.pallas_call(
        functools.partial(cache_kernel, layer),
        in_specs=[pl.BlockSpec(memory_space=pltpu.SMEM), vmem, vmem] + [hbm] * 5,
        out_specs=[hbm] * 3,
        out_shape=[jax.ShapeDtypeStruct(a.shape, BF16) for a in (x, k_cache, v_cache)],
        input_output_aliases={6: 1, 7: 2},
        scratch_shapes=[pltpu.VMEM((batch, seq, head), BF16), pltpu.VMEM((batch, seq, head), BF16), pltpu.VMEM(x.shape, BF16),
                        dma((2, blocks)), dma((2, blocks)), dma((2,))],
        compiler_params=pltpu.CompilerParams(vmem_limit_bytes=VMEM_BYTES),
        name="write_cache",
    )(positions, k_rows, v_rows, x, k_cache, v_cache, k_prev, v_prev)


CHUNKS = 4

ORDER = (
    "O03O00P03O01P00P01S03O02P02S00S01F03G03g03S02F00",
    "D03G00P13F01g00D00G01F02P10g01D01S13G02P11g02D02",
    "S10F13P12Q23S11A23B23O23F10P23S12Q20A20F11B20O20",
    "Q21A21P20B21O21S23F12P21Q22A22B22S20O22F23P22G23",
    "S21g23F20D23G20S22g20F21D20P33G21P30g21F22D21G22",
    "P31g22S33D22P32S30S31S32F30F31F33E30F32E33E31E32",
)


def body_kernel(
    pos_s, o_hbm, x_hbm, gm_hbm, ga_hbm, wo_hbm, wg_hbm, wu_hbm, wd_hbm, wq_hbm, wk_hbm, wv_hbm, k_hbm, v_hbm,
    cos_hbm, sin_hbm, posc_hbm,
    x_out, kn_out, vn_out,
    wo, wg, wu, wd, wq, wk, wv, kbuf, vbuf, o_s, xres, part, hbuf, hst, abuf, qkv_s, d2d_in, rs_out, rs_in, acc,
    gm, ga, cos, sin, posc,
    w_sem, x_sem, kv_sem, t_sem, out_sem, d2d_s, d2d_r, rs_s, rs_r, ag_s, ag_r, fw_s, fw_r,
):
    chunks, _, _, own, d = part.shape
    rows = 8 * own
    ff = wg.shape[1]
    head = kbuf.shape[2]
    me = lax.axis_index("tp")
    group = lax.axis_index("dp")
    core = me % 2
    chip = me // 2
    chips = [chip, chip + 1 - 2 * (chip % 2), (chip + 2) % 4, 3 - chip]
    partner = (group, chip * 2 + 1 - core)
    peers = [None] + [(group, chips[k] * 2 + core) for k in (1, 2, 3)]
    order = (3, 1, 2)

    loads = {}

    def load(name, src, dst, sem):
        loads[name] = pltpu.make_async_copy(src, dst, sem)
        loads[name].start()

    def need(*names):
        for name in names:
            if name in loads:
                loads.pop(name).wait()

    load("o", o_hbm, o_s, t_sem.at[0])
    load("wo", wo_hbm.at[0], wo, w_sem.at[0])
    load("gm", gm_hbm, gm, t_sem.at[1])
    for q in range(chunks):
        load(("x", q), x_hbm.at[q, core, chip], xres.at[q], x_sem.at[q])
    load("wg", wg_hbm.at[0], wg, w_sem.at[1])
    load("wu", wu_hbm.at[0], wu, w_sem.at[2])
    load("wd", wd_hbm.at[0], wd, w_sem.at[3])
    load("ga", ga_hbm, ga, t_sem.at[2])
    load("wq", wq_hbm.at[1], wq, w_sem.at[4])
    load("wk", wk_hbm.at[1], wk, w_sem.at[5])
    load("wv", wv_hbm.at[1], wv, w_sem.at[6])
    load("cos", cos_hbm, cos, t_sem.at[3])
    load("sin", sin_hbm, sin, t_sem.at[4])
    load("posc", posc_hbm, posc, t_sem.at[5])

    def load_kv(i):
        at = pl.ds(i * BLOCK, BLOCK)
        load(("k", i), k_hbm.at[1, at], kbuf.at[at], kv_sem.at[0, i])
        load(("v", i), v_hbm.at[1, at], vbuf.at[at], kv_sem.at[1, i])

    barrier = pltpu.get_barrier_semaphore()
    for dev in [partner] + peers[1:]:
        pl.semaphore_signal(barrier, inc=1, device_id=dev, device_id_type=MESH)
    pl.semaphore_wait(barrier, 4)

    def remote(src, dst, s, r, dev):
        return pltpu.make_async_remote_copy(
            src_ref=src, dst_ref=dst, send_sem=s, recv_sem=r, device_id=dev, device_id_type=MESH)

    def d2d(q):
        return remote(part.at[q, 1 - core], d2d_in.at[q], d2d_s.at[q], d2d_r.at[q], partner)

    def rs(q, k):
        return remote(rs_out.at[q, k - 1], rs_in.at[q, k - 1], rs_s.at[q, k - 1], rs_r.at[q, k - 1], peers[k])

    def ag(q, k):
        ref = hbuf.at[q, core, chip]
        return remote(ref, ref, ag_s.at[q, k - 1], ag_r.at[q, k - 1], peers[k])

    def ag_in(q, k):
        ref = hbuf.at[q, core, chips[k]]
        return remote(ref, ref, ag_s.at[q, k - 1], ag_r.at[q, k - 1], peers[k])

    def fw(q, k):
        ref = hbuf.at[q, core, chips[k]]
        return remote(ref, ref, fw_s.at[q, k], fw_r.at[q, k], partner)

    def fw_in(q, k):
        ref = hbuf.at[q, 1 - core, chips[k]]
        return remote(ref, ref, fw_s.at[q, k], fw_r.at[q, k], partner)

    def put_part(q, cols, value):
        for p in range(2):
            for c in range(4):
                at = (p * 4 + c) * own
                part[q, p, c, :, cols] = value[at:at + own].astype(BF16)

    def pair_sums(q):
        d2d(q).wait_recv()
        for k in order:
            pair = part[q, core, chips[k]].astype(F32) + d2d_in[q, chips[k]].astype(F32)
            rs_out[q, k - 1] = pair.astype(BF16)
            rs(q, k).start()
        acc[q] = part[q, core, chip].astype(F32) + d2d_in[q, chip].astype(F32)
        d2d(q).wait_send()

    def totals(a, q):
        for k in (1, 2, 3):
            rs(q, k).wait_recv()
        need(("x", q))
        total = acc[q]
        for k in (1, 2, 3):
            total = total + rs_in[q, k - 1].astype(F32)
        x = (xres[q].astype(F32) + total.astype(BF16).astype(F32)).astype(BF16)
        if a == 3:
            hbuf[q, core, chip] = x
        else:
            xres[q] = x
            if a == 1:
                need("ga")
                gain = ga[1:2, :]
            else:
                need("gm")
                gain = gm[a // 2:a // 2 + 1, :]
            hbuf[q, core, chip] = normed(x, gain.astype(F32))
        for k in order:
            ag(q, k).start()
        fw(q, 0).start()
        for k in (1, 2, 3):
            rs(q, k).wait_send()

    def forward(q):
        for k in (1, 2, 3):
            ag_in(q, k).wait_recv()
            fw(q, k).start()

    def gathered(q):
        for k in range(4):
            fw_in(q, k).wait_recv()
        for k in (1, 2, 3):
            ag(q, k).wait_send()
        for k in range(4):
            fw(q, k).wait_send()

    def stage(q):
        gathered(q)
        hst[q] = hbuf[q].reshape(rows, d)

    def out_product(a, q):
        need("o", "wo")

        @pl.loop(0, d // 1024)
        def _(n):
            cols = pl.ds(pl.multiple_of(n * 1024, 1024), 1024)
            put_part(q, cols, jnp.dot(o_s[q * rows:(q + 1) * rows, :], wo[:, cols], preferred_element_type=F32))

        d2d(q).start()

    def gate_up(q, half):
        if half == 0:
            stage(q)
            need("wg", "wu")
        steps_n = ff // 512

        @pl.loop(half * steps_n, (half + 1) * steps_n)
        def _(n):
            cols = pl.ds(pl.multiple_of(n * 256, 256), 256)
            h = hst[q]
            g = jnp.dot(h, wg[:, cols], preferred_element_type=F32).astype(BF16).astype(F32)
            u = jnp.dot(h, wu[:, cols], preferred_element_type=F32).astype(BF16).astype(F32)
            abuf[q, :, cols] = (g * jax.nn.sigmoid(g) * u).astype(BF16)

    def down(q):
        need("wd")

        @pl.loop(0, d // 1024)
        def _(n):
            cols = pl.ds(pl.multiple_of(n * 1024, 1024), 1024)
            put_part(q, cols, jnp.dot(abuf[q], wd[:, cols], preferred_element_type=F32))

        d2d(q).start()

    def qkv(q):
        stage(q)
        need("wq", "wk", "wv")
        qd, kd = wq.shape[1], wk.shape[1]
        h = hst[q]
        qkv_s[q, :, 0:qd] = jnp.dot(h, wq[...], preferred_element_type=F32).astype(BF16)
        qkv_s[q, :, qd:qd + kd] = jnp.dot(h, wk[...], preferred_element_type=F32).astype(BF16)
        qkv_s[q, :, qd + kd:] = jnp.dot(h, wv[...], preferred_element_type=F32).astype(BF16)

    def attend(q, i):
        need("cos", "sin", "posc")
        for j in range(rows // BLOCK // 2):
            first = i * (rows // 2) + j * BLOCK
            block = (q * rows + first) // BLOCK
            need(("k", block), ("v", block))
            base = block * BLOCK
            at = slice(base, base + BLOCK)
            o, kn, vn = attend_block(
                qkv_s[q, first:first + BLOCK, :], cos[at, :], sin[at, :], posc[at, :], lambda b: pos_s[base + b],
                lambda b: kbuf[base + b], lambda b: vbuf[base + b], None, None)
            for h, o_h in enumerate(o):
                o_s[at, h * head:(h + 1) * head] = o_h
            kn_out[at, :] = kn.astype(BF16)
            vn_out[at, :] = vn.astype(BF16)

    def result(q):
        gathered(q)
        load(("out", q), hbuf.at[q], x_out.at[q], out_sem.at[q])

    steps = [line[i:i + 3] for line in ORDER for i in range(0, len(line), 3)]
    last = {name: max(i for i, s in enumerate(steps) if s[0] == name and s[1] == "0") for name in "OgD"}
    for i, code in enumerate(steps):
        name, a, q = code[0], int(code[1]), int(code[2])
        if name == "O":
            out_product(a, q)
        elif name == "P":
            pair_sums(q)
        elif name == "S":
            totals(a, q)
        elif name == "F":
            forward(q)
        elif name in "Gg":
            gate_up(q, "Gg".index(name))
        elif name == "D":
            down(q)
        elif name == "Q":
            qkv(q)
        elif name in "AB":
            attend(q, "AB".index(name))
        else:
            result(q)
        if i == last["O"]:
            load("wo", wo_hbm.at[1], wo, w_sem.at[0])
            for j in range(kbuf.shape[0] // BLOCK):
                load_kv(j)
        if i == last["g"]:
            load("wg", wg_hbm.at[1], wg, w_sem.at[1])
            load("wu", wu_hbm.at[1], wu, w_sem.at[2])
        if i == last["D"]:
            load("wd", wd_hbm.at[1], wd, w_sem.at[3])
    need(*[("out", q) for q in range(chunks)])


def body(positions, o, x, mlp_norm, attn_norm, w_out, w_gate, w_up, w_down, w_query, w_key, w_value, k_cache, v_cache, cos2, sin2, posc):
    batch, qd = o.shape
    d = w_out.shape[2]
    ff = w_gate.shape[2]
    kd = w_key.shape[2]
    seq = k_cache.shape[2]
    own = batch // (8 * CHUNKS)
    rows = 8 * own
    vmem = pl.BlockSpec(memory_space=pltpu.VMEM)
    hbm = pl.BlockSpec(memory_space=pl.ANY)
    dma = pltpu.SemaphoreType.DMA
    row = jax.ShapeDtypeStruct((batch, kd), BF16)
    return pl.pallas_call(
        body_kernel,
        in_specs=[pl.BlockSpec(memory_space=pltpu.SMEM)] + [hbm] * 16,
        out_specs=[hbm, vmem, vmem],
        out_shape=[jax.ShapeDtypeStruct((CHUNKS, 2, 4, own, d), BF16), row, row],
        scratch_shapes=[
            pltpu.VMEM((qd, d), BF16), pltpu.VMEM((d, ff), BF16), pltpu.VMEM((d, ff), BF16), pltpu.VMEM((ff, d), BF16),
            pltpu.VMEM((d, qd), BF16), pltpu.VMEM((d, kd), BF16), pltpu.VMEM((d, kd), BF16),
            pltpu.VMEM((batch, seq, kd), BF16), pltpu.VMEM((batch, seq, kd), BF16),
            pltpu.VMEM((batch, qd), BF16),
            pltpu.VMEM((CHUNKS, own, d), BF16),
            pltpu.VMEM((CHUNKS, 2, 4, own, d), BF16),
            pltpu.VMEM((CHUNKS, 2, 4, own, d), BF16),
            pltpu.VMEM((CHUNKS, rows, d), BF16),
            pltpu.VMEM((CHUNKS, rows, ff), BF16),
            pltpu.VMEM((CHUNKS, rows, qd + 2 * kd), BF16),
            pltpu.VMEM((CHUNKS, 4, own, d), BF16),
            pltpu.VMEM((CHUNKS, 3, own, d), BF16),
            pltpu.VMEM((CHUNKS, 3, own, d), BF16),
            pltpu.VMEM((CHUNKS, own, d), F32),
            pltpu.VMEM(mlp_norm.shape, BF16), pltpu.VMEM(attn_norm.shape, BF16),
            pltpu.VMEM((batch, kd), F32), pltpu.VMEM((batch, kd), F32), pltpu.VMEM((batch, kd), F32),
            dma((7,)), dma((CHUNKS,)), dma((2, batch // BLOCK)), dma((6,)), dma((CHUNKS,)),
            dma((CHUNKS,)), dma((CHUNKS,)),
            dma((CHUNKS, 3)), dma((CHUNKS, 3)),
            dma((CHUNKS, 3)), dma((CHUNKS, 3)),
            dma((CHUNKS, 4)), dma((CHUNKS, 4)),
        ],
        compiler_params=pltpu.CompilerParams(vmem_limit_bytes=VMEM_BYTES, collective_id=0, has_side_effects=True),
        name="body",
    )(positions, o, x, mlp_norm, attn_norm, w_out, w_gate, w_up, w_down, w_query, w_key, w_value, k_cache, v_cache, cos2, sin2, posc)


def solution(mesh):
    row_spec = P('dp', None)
    pos_spec = P('dp')
    cache_spec = P(None, 'dp', None, 'tp', None)
    norm_spec = P(None, None)
    col_spec = P(None, None, 'tp')
    split_rows = P(None, 'tp', None)

    def local_step(hidden, positions, k_cache, v_cache, attn_norm, w_query, w_key, w_value, w_out, mlp_norm, w_gate, w_up, w_down):
        layers, batch, seq, _, head = k_cache.shape
        d = hidden.shape[1]
        own = batch // (8 * CHUNKS)
        kc = k_cache.reshape(layers, batch, seq, head)
        vc = v_cache.reshape(layers, batch, seq, head)
        o, cos2, sin2, posc, k_out, v_out = first(hidden, attn_norm, w_query, w_key, w_value, positions, kc, vc)
        x = hidden.reshape(CHUNKS, 2, 4, own, d)
        x_out, k_rows, v_rows = body(positions, o, x, mlp_norm, attn_norm, w_out, w_gate, w_up, w_down,
                                     w_query, w_key, w_value, kc, vc, cos2, sin2, posc)
        x_out, k_out, v_out = write_cache(1, positions, k_rows, v_rows, x_out.reshape(batch, d), kc, vc, k_out, v_out)
        return x_out, k_out.reshape(k_cache.shape), v_out.reshape(v_cache.shape)

    return jax.shard_map(local_step, mesh=mesh, in_specs=(row_spec, pos_spec, cache_spec, cache_spec, norm_spec, col_spec, col_spec, col_spec, split_rows, norm_spec, col_spec, col_spec, split_rows), out_specs=(row_spec, cache_spec, cache_spec), check_vma=False)
```

```python
import functools
import math

import jax
import jax.numpy as jnp
import numpy as np
from jax import lax
from jax.experimental import pallas as pl
from jax.experimental.pallas import tpu as pltpu
from jax.sharding import PartitionSpec as P

F32 = jnp.float32
BF16 = jnp.bfloat16
MESH = pl.DeviceIdType.MESH
VMEM_BYTES = 64 * 1024 * 1024 - 128 * 1024
BODY_BYTES = 36 * 1024 * 1024
FIRST_BYTES = 48 * 1024 * 1024
EPS = 1e-5


def in_hbm(*arrays):
    return [pltpu.with_memory_space_constraint(a, pltpu.HBM) for a in arrays]


def on_chip(*arrays):
    return [pltpu.with_memory_space_constraint(a, pltpu.VMEM) for a in arrays]


def rope_rows(head_dim):
    half_dim = head_dim // 2
    f32 = np.float32
    inv_freq = np.power(f32(500000.0), -np.arange(half_dim, dtype=f32) * f32(2.0 / head_dim))
    wavelen = f32(2.0 * math.pi) / inv_freq
    smooth = (f32(8192.0) / wavelen - f32(1.0)) / f32(3.0)
    blended = (f32(1.0) - smooth) * inv_freq / f32(8.0) + smooth * inv_freq
    scaled = np.where(wavelen < 2048.0, inv_freq, np.where(wavelen > 8192.0, inv_freq / f32(8.0), blended)).astype(f32)
    ones = np.ones(half_dim, f32)
    return np.stack([np.concatenate([scaled, scaled]), np.concatenate([-ones, ones])])


def normed(x, gain):
    xf = x.astype(F32)
    mean_sq = jnp.mean(xf * xf, axis=-1, keepdims=True)
    return (xf * lax.rsqrt(mean_sq + EPS) * gain).astype(BF16)


BLOCK = 32


def attend_block(qkv, cos, sin, posc, pos_at, k_at, v_at, k_put, v_put):
    head = cos.shape[1]
    seq = k_at(0).shape[0]
    heads = qkv.shape[1] // head - 2
    scale = head ** -0.5

    def rope(vec):
        vec = vec.astype(F32)
        return vec * cos + pltpu.roll(vec, head // 2, 1) * sin

    qs = [rope(qkv[:, h * head:(h + 1) * head]) for h in range(heads)]
    kn = rope(qkv[:, heads * head:(heads + 1) * head])
    vn = qkv[:, (heads + 1) * head:(heads + 2) * head].astype(F32)

    tiles = (seq // 16, 16, head)
    seq_ids = lax.broadcasted_iota(jnp.int32, tiles, 0) * 16 + lax.broadcasted_iota(jnp.int32, tiles, 1)
    seq_bf = seq_ids.astype(F32).astype(BF16)
    row_of = lax.broadcasted_iota(jnp.int32, (32, head), 0) % 8
    lane = lax.broadcasted_iota(jnp.int32, (32, seq), 1).astype(F32)

    def updated(cache, row, b):
        here = seq_bf == jnp.full((16, head), pos_at(b).astype(F32), F32).astype(BF16)[None]
        row = jnp.broadcast_to(row, (16, head)).astype(BF16)[None]
        return jnp.where(here, row, cache.reshape(tiles)).reshape(seq, head)

    all_scores = []
    for j in range(BLOCK // 8):
        pieces = [q[8 * j:8 * j + 8] for q in qs] + [jnp.zeros((8, head), F32)] * (4 - heads)
        qj = jnp.concatenate(pieces, axis=0).astype(BF16)
        scores = None
        for b8 in range(8):
            b = 8 * j + b8
            k_b = updated(k_at(b), kn[b:b + 1], b)
            k_put(b, k_b)
            s_b = lax.dot_general(qj, k_b, (((1,), (1,)), ((), ())), preferred_element_type=F32)
            scores = s_b if scores is None else jnp.where(row_of == b8, s_b, scores)
        all_scores.append(scores)
    probs = []
    for j in range(BLOCK // 8):
        limit = jnp.concatenate([posc[8 * j:8 * j + 8]] * 4, axis=0)
        scores = jnp.where(lane <= limit, all_scores[j] * scale, -jnp.inf)
        peak = jnp.max(scores, axis=1, keepdims=True)
        weight = jnp.exp(scores - peak)
        total = jnp.sum(weight, axis=1, keepdims=True)
        probs.append((weight * (1.0 / total)).astype(BF16))
    outs = []
    for j in range(BLOCK // 8):
        mixed = None
        for b8 in range(8):
            b = 8 * j + b8
            v_b = updated(v_at(b), vn[b:b + 1], b)
            v_put(b, v_b)
            o_b = jnp.dot(probs[j], v_b, preferred_element_type=F32)
            mixed = o_b if mixed is None else jnp.where(row_of == b8, o_b, mixed)
        outs.append(mixed)
    o = [jnp.concatenate([m[8 * h:8 * h + 8] for m in outs], axis=0).astype(BF16) for h in range(heads)]
    return o


def first_kernel(
    pos_hbm, x_hbm, g_hbm, wq_hbm, wk_hbm, wv_hbm, wo_hbm, pos2_hbm, rope_hbm, k_hbm, v_hbm,
    o_ref, wo_ref, cos_ref, sin_ref, posc_ref, ko_hbm, vo_hbm,
    h_ref, g_ref, wq, wk, wv, pos_s, pos_ref, rope_ref, qkv_ref, kbuf, vbuf, sem, in_sem, out_sem,
):
    rows = h_ref.shape[0]
    qd = wq.shape[1]
    kd = wk.shape[1]
    blocks = rows // BLOCK
    copies = [pltpu.make_async_copy(src, dst, sem.at[i]) for i, (src, dst) in enumerate(
        [(x_hbm, h_ref), (g_hbm, g_ref), (wq_hbm.at[0], wq), (wk_hbm.at[0], wk), (wv_hbm.at[0], wv)])]
    small = [pltpu.make_async_copy(src, dst, sem.at[i]) for i, (src, dst) in enumerate(
        [(pos_hbm, pos_s), (pos2_hbm, pos_ref), (rope_hbm, rope_ref)], 6)]
    for cp in copies[:2] + small + copies[2:]:
        cp.start()

    def reads(i):
        at = pl.ds(i * BLOCK, BLOCK)
        return (pltpu.make_async_copy(k_hbm.at[0, at], kbuf.at[at], in_sem.at[0, i]),
                pltpu.make_async_copy(v_hbm.at[0, at], vbuf.at[at], in_sem.at[1, i]))

    def writes(i):
        at = pl.ds(i * BLOCK, BLOCK)
        return (pltpu.make_async_copy(kbuf.at[at], ko_hbm.at[0, at], out_sem.at[0, i]),
                pltpu.make_async_copy(vbuf.at[at], vo_hbm.at[0, at], out_sem.at[1, i]))

    for cp in small:
        cp.wait()
    width = pos_ref.shape[1]
    diagonal = (lax.broadcasted_iota(jnp.int32, (width, width), 0) == lax.broadcasted_iota(jnp.int32, (width, width), 1))
    for i in range(rows // width):
        across = jnp.broadcast_to(pos_ref[i:i + 1, :].astype(F32), (width, width))
        down = jnp.sum(jnp.where(diagonal, across, 0.0), axis=1, keepdims=True)
        at = slice(i * width, (i + 1) * width)
        angles = down * rope_ref[0:1, :]
        posc_ref[at, :] = jnp.broadcast_to(down, (width, width))
        cos_ref[at, :] = jnp.cos(angles)
        sin_ref[at, :] = jnp.sin(angles) * rope_ref[1:2, :]

    copies[0].wait()
    copies[1].wait()
    for i in range(blocks):
        for cp in reads(i):
            cp.start()
    wo_copy = pltpu.make_async_copy(wo_hbm.at[0], wo_ref, sem.at[5])
    wo_copy.start()
    gain = g_ref[0:1, :].astype(F32)

    @pl.loop(0, rows // 16)
    def _(i):
        sl = pl.ds(pl.multiple_of(i * 16, 16), 16)
        h_ref[sl, :] = normed(h_ref[sl, :], gain)

    h = h_ref[...]
    copies[2].wait()
    qkv_ref[:, 0:qd] = jnp.dot(h, wq[...], preferred_element_type=F32).astype(BF16)
    copies[3].wait()
    copies[4].wait()
    qkv_ref[:, qd:qd + kd] = jnp.dot(h, wk[...], preferred_element_type=F32).astype(BF16)
    qkv_ref[:, qd + kd:] = jnp.dot(h, wv[...], preferred_element_type=F32).astype(BF16)

    @pl.loop(0, blocks)
    def _(i):
        base = pl.multiple_of(i * BLOCK, BLOCK)
        at = pl.ds(base, BLOCK)
        for cp in reads(i):
            cp.wait()

        def k_put(b, value):
            kbuf[base + b] = value

        def v_put(b, value):
            vbuf[base + b] = value

        o = attend_block(
            qkv_ref[at, :], cos_ref[at, :], sin_ref[at, :], posc_ref[at, :], lambda b: pos_s[base + b],
            lambda b: kbuf[base + b], lambda b: vbuf[base + b], k_put, v_put)
        for n, o_n in enumerate(o):
            o_ref[at, n * kd:(n + 1) * kd] = o_n
        for cp in writes(i):
            cp.start()

    for i in range(blocks):
        for cp in writes(i):
            cp.wait()
    wo_copy.wait()


def first(hidden, attn_norm, w_query, w_key, w_value, w_out, positions, k_cache, v_cache):
    rows, d = hidden.shape
    qd, kd = w_query.shape[2], w_key.shape[2]
    seq = k_cache.shape[2]
    blocks = rows // BLOCK
    vmem = pl.BlockSpec(memory_space=pltpu.VMEM)
    hbm = pl.BlockSpec(memory_space=pl.ANY)
    dma = pltpu.SemaphoreType.DMA
    table = pltpu.VMEM((rows, kd), F32)
    cache = jax.ShapeDtypeStruct(k_cache.shape, BF16)
    return pl.pallas_call(
        first_kernel,
        in_specs=[hbm] * 11,
        out_specs=[vmem] * 5 + [hbm, hbm],
        out_shape=[pltpu.VMEM((rows, qd), BF16), pltpu.VMEM(w_out.shape[1:], BF16), table, table, table, cache, cache],
        scratch_shapes=[
            pltpu.VMEM((rows, d), BF16), pltpu.VMEM(attn_norm.shape, BF16), pltpu.VMEM((d, qd), BF16),
            pltpu.VMEM((d, kd), BF16), pltpu.VMEM((d, kd), BF16),
            pltpu.SMEM((rows,), jnp.int32), pltpu.VMEM((rows // kd, kd), jnp.int32), pltpu.VMEM((2, kd), F32),
            pltpu.VMEM((rows, qd + 2 * kd), BF16),
            pltpu.VMEM((rows, seq, kd), BF16), pltpu.VMEM((rows, seq, kd), BF16),
            dma((9,)), dma((2, blocks)), dma((2, blocks)),
        ],
        compiler_params=pltpu.CompilerParams(vmem_limit_bytes=FIRST_BYTES),
        name="first",
    )(*in_hbm(positions, hidden, attn_norm, w_query, w_key, w_value, w_out, positions.reshape(rows // kd, kd),
              jnp.asarray(rope_rows(kd)), k_cache, v_cache))


def cache_kernel(layer, x_ref, k_ref, v_ref, k_prev, v_prev, x_hbm, ko_hbm, vo_hbm, out_sem, x_sem):
    batch = k_ref.shape[0]
    blocks = batch // BLOCK
    writes = []
    for i in range(blocks):
        at = pl.ds(i * BLOCK, BLOCK)
        writes.append(pltpu.make_async_copy(k_ref.at[at], ko_hbm.at[layer, at], out_sem.at[0, i]))
        writes.append(pltpu.make_async_copy(v_ref.at[at], vo_hbm.at[layer, at], out_sem.at[1, i]))
    writes.append(pltpu.make_async_copy(x_ref, x_hbm, x_sem.at[0]))
    for cp in writes:
        cp.start()
    for cp in writes:
        cp.wait()


def write_cache(layer, x, k_layer, v_layer, k_prev, v_prev):
    blocks = k_layer.shape[0] // BLOCK
    vmem = pl.BlockSpec(memory_space=pltpu.VMEM)
    hbm = pl.BlockSpec(memory_space=pl.ANY)
    dma = pltpu.SemaphoreType.DMA
    return pl.pallas_call(
        functools.partial(cache_kernel, layer),
        in_specs=[vmem, vmem, vmem, hbm, hbm],
        out_specs=[hbm] * 3,
        out_shape=[jax.ShapeDtypeStruct(a.shape, BF16) for a in (x, k_prev, v_prev)],
        input_output_aliases={3: 1, 4: 2},
        scratch_shapes=[dma((2, blocks)), dma((1,))],
        compiler_params=pltpu.CompilerParams(vmem_limit_bytes=2 * 1024 * 1024),
        name="write_cache",
    )(x, k_layer, v_layer, k_prev, v_prev)


CHUNKS = 4

ORDER = (
    "O03O00P03O01P00P01S03O02P02S00S01F03G03g03S02F00",
    "D03G00P13F01g00D00G01F02P10g01D01S13G02P11g02D02",
    "S10F13P12Q23S11A23B23O23F10P23S12Q20A20F11B20O20",
    "Q21A21P20B21O21S23F12P21Q22A22B22S20O22F23P22G23",
    "S21g23F20D23G20S22g20F21D20P33G21P30g21F22D21G22",
    "P31g22S33D22P32S30S31S32F30F31F33E30F32E33E31E32",
)


def body_kernel(
    o_first, wo_first, cos, sin, posc, pos_hbm, x_hbm, gm_hbm, ga_hbm, wo_hbm, wg_hbm, wu_hbm, wd_hbm, wq_hbm, wk_hbm, wv_hbm, k_hbm, v_hbm,
    x_out, kbuf, vbuf,
    wo, wg, wu, wd, wq, wk, wv, o_s, xres, part, hbuf, hst, abuf, qkv_s, d2d_in, rs_out, rs_in, acc,
    gm, ga, pos_s,
    w_sem, x_sem, kv_sem, t_sem, d2d_s, d2d_r, rs_s, rs_r, ag_s, ag_r, fw_s, fw_r,
):
    chunks, _, _, own, d = part.shape
    rows = 8 * own
    ff = wg.shape[1]
    head = kbuf.shape[2]
    me = lax.axis_index("tp")
    group = lax.axis_index("dp")
    core = me % 2
    chip = me // 2
    chips = [chip, chip + 1 - 2 * (chip % 2), (chip + 2) % 4, 3 - chip]
    partner = (group, chip * 2 + 1 - core)
    peers = [None] + [(group, chips[k] * 2 + core) for k in (1, 2, 3)]
    order = (3, 1, 2)

    loads = {}

    def load(name, src, dst, sem):
        loads[name] = pltpu.make_async_copy(src, dst, sem)
        loads[name].start()

    def need(*names):
        for name in names:
            if name in loads:
                loads.pop(name).wait()

    load("gm", gm_hbm, gm, t_sem.at[0])
    for q in range(chunks):
        load(("x", q), x_hbm.at[q, core, chip], xres.at[q], x_sem.at[q])
    load("wg", wg_hbm.at[0], wg, w_sem.at[1])
    load("wu", wu_hbm.at[0], wu, w_sem.at[2])
    load("wd", wd_hbm.at[0], wd, w_sem.at[3])
    load("ga", ga_hbm, ga, t_sem.at[1])
    load("pos", pos_hbm, pos_s, t_sem.at[2])
    load("wq", wq_hbm.at[1], wq, w_sem.at[4])
    load("wk", wk_hbm.at[1], wk, w_sem.at[5])
    load("wv", wv_hbm.at[1], wv, w_sem.at[6])
    load("wo", wo_hbm.at[1], wo, w_sem.at[0])

    def load_kv(i):
        at = pl.ds(i * BLOCK, BLOCK)
        load(("k", i), k_hbm.at[1, at], kbuf.at[at], kv_sem.at[0, i])
        load(("v", i), v_hbm.at[1, at], vbuf.at[at], kv_sem.at[1, i])

    barrier = pltpu.get_barrier_semaphore()
    for dev in [partner] + peers[1:]:
        pl.semaphore_signal(barrier, inc=1, device_id=dev, device_id_type=MESH)
    pl.semaphore_wait(barrier, 4)

    def remote(src, dst, s, r, dev):
        return pltpu.make_async_remote_copy(
            src_ref=src, dst_ref=dst, send_sem=s, recv_sem=r, device_id=dev, device_id_type=MESH)

    def d2d(q):
        return remote(part.at[q, 1 - core], d2d_in.at[q], d2d_s.at[q], d2d_r.at[q], partner)

    def rs(q, k):
        return remote(rs_out.at[q, k - 1], rs_in.at[q, k - 1], rs_s.at[q, k - 1], rs_r.at[q, k - 1], peers[k])

    def ag(q, k):
        ref = hbuf.at[q, core, chip]
        return remote(ref, ref, ag_s.at[q, k - 1], ag_r.at[q, k - 1], peers[k])

    def ag_in(q, k):
        ref = hbuf.at[q, core, chips[k]]
        return remote(ref, ref, ag_s.at[q, k - 1], ag_r.at[q, k - 1], peers[k])

    def fw(q, k):
        ref = hbuf.at[q, core, chips[k]]
        return remote(ref, ref, fw_s.at[q, k], fw_r.at[q, k], partner)

    def fw_in(q, k):
        ref = hbuf.at[q, 1 - core, chips[k]]
        return remote(ref, ref, fw_s.at[q, k], fw_r.at[q, k], partner)

    def put_part(q, cols, value):
        for p in range(2):
            for c in range(4):
                at = (p * 4 + c) * own
                part[q, p, c, :, cols] = value[at:at + own].astype(BF16)

    def pair_sums(q):
        d2d(q).wait_recv()
        for k in order:
            pair = part[q, core, chips[k]].astype(F32) + d2d_in[q, chips[k]].astype(F32)
            rs_out[q, k - 1] = pair.astype(BF16)
            rs(q, k).start()
        acc[q] = part[q, core, chip].astype(F32) + d2d_in[q, chip].astype(F32)
        d2d(q).wait_send()

    def totals(a, q):
        for k in (1, 2, 3):
            rs(q, k).wait_recv()
        need(("x", q))
        total = acc[q]
        for k in (1, 2, 3):
            total = total + rs_in[q, k - 1].astype(F32)
        x = (xres[q].astype(F32) + total.astype(BF16).astype(F32)).astype(BF16)
        if a == 3:
            hbuf[q, core, chip] = x
        else:
            xres[q] = x
            if a == 1:
                need("ga")
                gain = ga[1:2, :]
            else:
                need("gm")
                gain = gm[a // 2:a // 2 + 1, :]
            hbuf[q, core, chip] = normed(x, gain.astype(F32))
        for k in order:
            ag(q, k).start()
        fw(q, 0).start()
        for k in (1, 2, 3):
            rs(q, k).wait_send()

    def forward(q):
        for k in (1, 2, 3):
            ag_in(q, k).wait_recv()
            fw(q, k).start()

    def gathered(q):
        for k in range(4):
            fw_in(q, k).wait_recv()
        for k in (1, 2, 3):
            ag(q, k).wait_send()
        for k in range(4):
            fw(q, k).wait_send()

    def stage(q):
        gathered(q)
        hst[q] = hbuf[q].reshape(rows, d)

    def out_product(a, q):
        if a:
            need("wo")
        o, w = (o_s, wo) if a else (o_first, wo_first)

        @pl.loop(0, d // 1024)
        def _(n):
            cols = pl.ds(pl.multiple_of(n * 1024, 1024), 1024)
            put_part(q, cols, jnp.dot(o[q * rows:(q + 1) * rows, :], w[:, cols], preferred_element_type=F32))

        d2d(q).start()

    def gate_up(q, half):
        if half == 0:
            stage(q)
            need("wg", "wu")
        steps_n = ff // 512

        @pl.loop(half * steps_n, (half + 1) * steps_n)
        def _(n):
            cols = pl.ds(pl.multiple_of(n * 256, 256), 256)
            h = hst[q]
            g = jnp.dot(h, wg[:, cols], preferred_element_type=F32).astype(BF16).astype(F32)
            u = jnp.dot(h, wu[:, cols], preferred_element_type=F32).astype(BF16).astype(F32)
            abuf[q, :, cols] = (g * jax.nn.sigmoid(g) * u).astype(BF16)

    def down(q):
        need("wd")

        @pl.loop(0, d // 1024)
        def _(n):
            cols = pl.ds(pl.multiple_of(n * 1024, 1024), 1024)
            put_part(q, cols, jnp.dot(abuf[q], wd[:, cols], preferred_element_type=F32))

        d2d(q).start()

    def qkv(q):
        stage(q)
        need("wq", "wk", "wv")
        qd, kd = wq.shape[1], wk.shape[1]
        h = hst[q]
        qkv_s[q, :, 0:qd] = jnp.dot(h, wq[...], preferred_element_type=F32).astype(BF16)
        qkv_s[q, :, qd:qd + kd] = jnp.dot(h, wk[...], preferred_element_type=F32).astype(BF16)
        qkv_s[q, :, qd + kd:] = jnp.dot(h, wv[...], preferred_element_type=F32).astype(BF16)

    def attend(q, i):
        for j in range(rows // BLOCK // 2):
            need("pos")
            first = i * (rows // 2) + j * BLOCK
            block = (q * rows + first) // BLOCK
            need(("k", block), ("v", block))
            base = block * BLOCK
            at = slice(base, base + BLOCK)

            def k_put(b, value):
                kbuf[base + b] = value

            def v_put(b, value):
                vbuf[base + b] = value

            o = attend_block(
                qkv_s[q, first:first + BLOCK, :], cos[at, :], sin[at, :], posc[at, :], lambda b: pos_s[base + b],
                lambda b: kbuf[base + b], lambda b: vbuf[base + b], k_put, v_put)
            for h, o_h in enumerate(o):
                o_s[at, h * head:(h + 1) * head] = o_h

    def result(q):
        gathered(q)
        x_out[q] = hbuf[q]

    steps = [line[i:i + 3] for line in ORDER for i in range(0, len(line), 3)]
    last = {name: max(i for i, s in enumerate(steps) if s[0] == name and s[1] == "0") for name in "OgD"}
    for i, code in enumerate(steps):
        name, a, q = code[0], int(code[1]), int(code[2])
        if name == "O":
            out_product(a, q)
        elif name == "P":
            pair_sums(q)
        elif name == "S":
            totals(a, q)
        elif name == "F":
            forward(q)
        elif name in "Gg":
            gate_up(q, "Gg".index(name))
        elif name == "D":
            down(q)
        elif name == "Q":
            qkv(q)
        elif name in "AB":
            attend(q, "AB".index(name))
        else:
            result(q)
        if i == last["O"]:
            for j in range(kbuf.shape[0] // BLOCK):
                load_kv(j)
        if i == last["g"]:
            load("wg", wg_hbm.at[1], wg, w_sem.at[1])
            load("wu", wu_hbm.at[1], wu, w_sem.at[2])
        if i == last["D"]:
            load("wd", wd_hbm.at[1], wd, w_sem.at[3])


def body(positions, o, wo_first, x, mlp_norm, attn_norm, w_out, w_gate, w_up, w_down, w_query, w_key, w_value, k_cache, v_cache, cos2, sin2, posc):
    batch, qd = o.shape
    d = w_out.shape[2]
    ff = w_gate.shape[2]
    kd = w_key.shape[2]
    seq = k_cache.shape[2]
    own = batch // (8 * CHUNKS)
    rows = 8 * own
    vmem = pl.BlockSpec(memory_space=pltpu.VMEM)
    hbm = pl.BlockSpec(memory_space=pl.ANY)
    dma = pltpu.SemaphoreType.DMA
    cache = pltpu.VMEM((batch, seq, kd), BF16)
    return pl.pallas_call(
        body_kernel,
        in_specs=[vmem] * 5 + [hbm] * 13,
        out_specs=[vmem] * 3,
        out_shape=[pltpu.VMEM((CHUNKS, 2, 4, own, d), BF16), cache, cache],
        scratch_shapes=[
            pltpu.VMEM((qd, d), BF16), pltpu.VMEM((d, ff), BF16), pltpu.VMEM((d, ff), BF16), pltpu.VMEM((ff, d), BF16),
            pltpu.VMEM((d, qd), BF16), pltpu.VMEM((d, kd), BF16), pltpu.VMEM((d, kd), BF16),
            pltpu.VMEM((batch, qd), BF16),
            pltpu.VMEM((CHUNKS, own, d), BF16),
            pltpu.VMEM((CHUNKS, 2, 4, own, d), BF16),
            pltpu.VMEM((CHUNKS, 2, 4, own, d), BF16),
            pltpu.VMEM((CHUNKS, rows, d), BF16),
            pltpu.VMEM((CHUNKS, rows, ff), BF16),
            pltpu.VMEM((CHUNKS, rows, qd + 2 * kd), BF16),
            pltpu.VMEM((CHUNKS, 4, own, d), BF16),
            pltpu.VMEM((CHUNKS, 3, own, d), BF16),
            pltpu.VMEM((CHUNKS, 3, own, d), BF16),
            pltpu.VMEM((CHUNKS, own, d), F32),
            pltpu.VMEM(mlp_norm.shape, BF16), pltpu.VMEM(attn_norm.shape, BF16), pltpu.SMEM((batch,), jnp.int32),
            dma((7,)), dma((CHUNKS,)), dma((2, batch // BLOCK)), dma((3,)),
            dma((CHUNKS,)), dma((CHUNKS,)),
            dma((CHUNKS, 3)), dma((CHUNKS, 3)),
            dma((CHUNKS, 3)), dma((CHUNKS, 3)),
            dma((CHUNKS, 4)), dma((CHUNKS, 4)),
        ],
        compiler_params=pltpu.CompilerParams(vmem_limit_bytes=BODY_BYTES, collective_id=0, has_side_effects=True),
        name="body",
    )(*on_chip(o, wo_first, cos2, sin2, posc),
      *in_hbm(positions, x, mlp_norm, attn_norm, w_out, w_gate, w_up, w_down, w_query, w_key, w_value, k_cache, v_cache))


def solution(mesh):
    row_spec = P('dp', None)
    pos_spec = P('dp')
    cache_spec = P(None, 'dp', None, 'tp', None)
    norm_spec = P(None, None)
    col_spec = P(None, None, 'tp')
    split_rows = P(None, 'tp', None)

    def local_step(hidden, positions, k_cache, v_cache, attn_norm, w_query, w_key, w_value, w_out, mlp_norm, w_gate, w_up, w_down):
        layers, batch, seq, _, head = k_cache.shape
        d = hidden.shape[1]
        own = batch // (8 * CHUNKS)
        kc = k_cache.reshape(layers, batch, seq, head)
        vc = v_cache.reshape(layers, batch, seq, head)
        o, wo_first, cos2, sin2, posc, k_out, v_out = first(hidden, attn_norm, w_query, w_key, w_value, w_out, positions, kc, vc)
        x = hidden.reshape(CHUNKS, 2, 4, own, d)
        x_out, k_layer, v_layer = body(positions, o, wo_first, x, mlp_norm, attn_norm, w_out, w_gate, w_up, w_down,
                                     w_query, w_key, w_value, kc, vc, cos2, sin2, posc)
        x_out, k_out, v_out = write_cache(1, x_out.reshape(batch, d), k_layer, v_layer, k_out, v_out)
        return x_out, k_out.reshape(k_cache.shape), v_out.reshape(v_cache.shape)

    return jax.shard_map(local_step, mesh=mesh, in_specs=(row_spec, pos_spec, cache_spec, cache_spec, norm_spec, col_spec, col_spec, col_spec, split_rows, norm_spec, col_spec, col_spec, split_rows), out_specs=(row_spec, cache_spec, cache_spec), check_vma=False)
```

```python
import functools
import math

import jax
import jax.numpy as jnp
import numpy as np
from jax import lax
from jax.experimental import pallas as pl
from jax.experimental.pallas import tpu as pltpu
from jax.sharding import PartitionSpec as P

F32 = jnp.float32
BF16 = jnp.bfloat16
MESH = pl.DeviceIdType.MESH
VMEM_BYTES = 64 * 1024 * 1024 - 128 * 1024
BODY_BYTES = 34 * 1024 * 1024
FIRST_BYTES = 24 * 1024 * 1024
EPS = 1e-5
CHUNKS = 4
EARLY = 2
COLS = 1024


def in_hbm(*arrays):
    return [pltpu.with_memory_space_constraint(a, pltpu.HBM) for a in arrays]


def on_chip(*arrays):
    return [pltpu.with_memory_space_constraint(a, pltpu.VMEM) for a in arrays]


def rope_rows(head_dim):
    half_dim = head_dim // 2
    f32 = np.float32
    inv_freq = np.power(f32(500000.0), -np.arange(half_dim, dtype=f32) * f32(2.0 / head_dim))
    wavelen = f32(2.0 * math.pi) / inv_freq
    smooth = (f32(8192.0) / wavelen - f32(1.0)) / f32(3.0)
    blended = (f32(1.0) - smooth) * inv_freq / f32(8.0) + smooth * inv_freq
    scaled = np.where(wavelen < 2048.0, inv_freq, np.where(wavelen > 8192.0, inv_freq / f32(8.0), blended)).astype(f32)
    ones = np.ones(half_dim, f32)
    return np.stack([np.concatenate([scaled, scaled]), np.concatenate([-ones, ones])])


def normed(x, gain):
    xf = x.astype(F32)
    mean_sq = jnp.mean(xf * xf, axis=-1, keepdims=True)
    return (xf * lax.rsqrt(mean_sq + EPS) * gain).astype(BF16)


BLOCK = 32


def attend_block(qkv, cos, sin, posc, pos_at, k_at, v_at, k_put, v_put):
    head = cos.shape[1]
    seq = k_at(0).shape[0]
    heads = qkv.shape[1] // head - 2
    scale = head ** -0.5

    def rope(vec):
        vec = vec.astype(F32)
        return vec * cos + pltpu.roll(vec, head // 2, 1) * sin

    qs = [rope(qkv[:, h * head:(h + 1) * head]) for h in range(heads)]
    kn = rope(qkv[:, heads * head:(heads + 1) * head])
    vn = qkv[:, (heads + 1) * head:(heads + 2) * head].astype(F32)

    tiles = (seq // 16, 16, head)
    seq_ids = lax.broadcasted_iota(jnp.int32, tiles, 0) * 16 + lax.broadcasted_iota(jnp.int32, tiles, 1)
    seq_bf = seq_ids.astype(F32).astype(BF16)
    row_of = lax.broadcasted_iota(jnp.int32, (32, head), 0) % 8
    lane = lax.broadcasted_iota(jnp.int32, (32, seq), 1).astype(F32)

    def updated(cache, row, b):
        here = seq_bf == jnp.full((16, head), pos_at(b).astype(F32), F32).astype(BF16)[None]
        row = jnp.broadcast_to(row, (16, head)).astype(BF16)[None]
        return jnp.where(here, row, cache.reshape(tiles)).reshape(seq, head)

    all_scores = []
    for j in range(BLOCK // 8):
        pieces = [q[8 * j:8 * j + 8] for q in qs] + [jnp.zeros((8, head), F32)] * (4 - heads)
        qj = jnp.concatenate(pieces, axis=0).astype(BF16)
        scores = None
        for b8 in range(8):
            b = 8 * j + b8
            k_b = updated(k_at(b), kn[b:b + 1], b)
            k_put(b, k_b)
            s_b = lax.dot_general(qj, k_b, (((1,), (1,)), ((), ())), preferred_element_type=F32)
            scores = s_b if scores is None else jnp.where(row_of == b8, s_b, scores)
        all_scores.append(scores)
    probs = []
    for j in range(BLOCK // 8):
        limit = jnp.concatenate([posc[8 * j:8 * j + 8]] * 4, axis=0)
        scores = jnp.where(lane <= limit, all_scores[j] * scale, -jnp.inf)
        peak = jnp.max(scores, axis=1, keepdims=True)
        weight = jnp.exp(scores - peak)
        total = jnp.sum(weight, axis=1, keepdims=True)
        probs.append((weight * (1.0 / total)).astype(BF16))
    outs = []
    for j in range(BLOCK // 8):
        mixed = None
        for b8 in range(8):
            b = 8 * j + b8
            v_b = updated(v_at(b), vn[b:b + 1], b)
            v_put(b, v_b)
            o_b = jnp.dot(probs[j], v_b, preferred_element_type=F32)
            mixed = o_b if mixed is None else jnp.where(row_of == b8, o_b, mixed)
        outs.append(mixed)
    o = [jnp.concatenate([m[8 * h:8 * h + 8] for m in outs], axis=0).astype(BF16) for h in range(heads)]
    return o


def first_kernel(
    pos_hbm, x_hbm, g_hbm, wq_hbm, wk_hbm, wv_hbm, wo_hbm, pos2_hbm, rope_hbm, k_hbm, v_hbm,
    o_ref, wo_ref, cos_ref, sin_ref, posc_ref, qkv_ref, ko_hbm, vo_hbm,
    h_ref, g_ref, wq, wk, wv, pos_s, pos_ref, rope_ref, kbuf, vbuf, sem, in_sem, out_sem,
):
    rows = h_ref.shape[0]
    qd = wq.shape[1]
    kd = wk.shape[1]
    blocks = kbuf.shape[0] // BLOCK
    copies = [pltpu.make_async_copy(src, dst, sem.at[i]) for i, (src, dst) in enumerate(
        [(x_hbm, h_ref), (g_hbm, g_ref), (wq_hbm.at[0], wq), (wk_hbm.at[0], wk), (wv_hbm.at[0], wv)])]
    small = [pltpu.make_async_copy(src, dst, sem.at[i]) for i, (src, dst) in enumerate(
        [(pos_hbm, pos_s), (pos2_hbm, pos_ref), (rope_hbm, rope_ref)], 6)]
    for cp in copies[:2] + small + copies[2:]:
        cp.start()

    def reads(i):
        at = pl.ds(i * BLOCK, BLOCK)
        return (pltpu.make_async_copy(k_hbm.at[0, at], kbuf.at[at], in_sem.at[0, i]),
                pltpu.make_async_copy(v_hbm.at[0, at], vbuf.at[at], in_sem.at[1, i]))

    def writes(i):
        at = pl.ds(i * BLOCK, BLOCK)
        return (pltpu.make_async_copy(kbuf.at[at], ko_hbm.at[0, at], out_sem.at[0, i]),
                pltpu.make_async_copy(vbuf.at[at], vo_hbm.at[0, at], out_sem.at[1, i]))

    for cp in small:
        cp.wait()
    width = pos_ref.shape[1]
    diagonal = (lax.broadcasted_iota(jnp.int32, (width, width), 0) == lax.broadcasted_iota(jnp.int32, (width, width), 1))
    for i in range(rows // width):
        across = jnp.broadcast_to(pos_ref[i:i + 1, :].astype(F32), (width, width))
        down = jnp.sum(jnp.where(diagonal, across, 0.0), axis=1, keepdims=True)
        at = slice(i * width, (i + 1) * width)
        angles = down * rope_ref[0:1, :]
        posc_ref[at, :] = jnp.broadcast_to(down, (width, width))
        cos_ref[at, :] = jnp.cos(angles)
        sin_ref[at, :] = jnp.sin(angles) * rope_ref[1:2, :]

    copies[0].wait()
    copies[1].wait()
    for i in range(blocks):
        for cp in reads(i):
            cp.start()
    wo_copy = pltpu.make_async_copy(wo_hbm.at[0], wo_ref, sem.at[5])
    wo_copy.start()
    gain = g_ref[0:1, :].astype(F32)

    @pl.loop(0, rows // 16)
    def _(i):
        sl = pl.ds(pl.multiple_of(i * 16, 16), 16)
        h_ref[sl, :] = normed(h_ref[sl, :], gain)

    h = h_ref[...]
    copies[2].wait()
    qkv_ref[:, 0:qd] = jnp.dot(h, wq[...], preferred_element_type=F32).astype(BF16)
    copies[3].wait()
    copies[4].wait()
    qkv_ref[:, qd:qd + kd] = jnp.dot(h, wk[...], preferred_element_type=F32).astype(BF16)
    qkv_ref[:, qd + kd:] = jnp.dot(h, wv[...], preferred_element_type=F32).astype(BF16)

    @pl.loop(0, blocks)
    def _(i):
        base = pl.multiple_of(i * BLOCK, BLOCK)
        at = pl.ds(base, BLOCK)
        for cp in reads(i):
            cp.wait()

        def k_put(b, value):
            kbuf[base + b] = value

        def v_put(b, value):
            vbuf[base + b] = value

        o = attend_block(
            qkv_ref[at, :], cos_ref[at, :], sin_ref[at, :], posc_ref[at, :], lambda b: pos_s[base + b],
            lambda b: kbuf[base + b], lambda b: vbuf[base + b], k_put, v_put)
        for n, o_n in enumerate(o):
            o_ref[at, n * kd:(n + 1) * kd] = o_n
        for cp in writes(i):
            cp.start()

    for i in range(blocks):
        for cp in writes(i):
            cp.wait()
    wo_copy.wait()


def first(hidden, attn_norm, w_query, w_key, w_value, w_out, positions, k_cache, v_cache):
    rows, d = hidden.shape
    qd, kd = w_query.shape[2], w_key.shape[2]
    seq = k_cache.shape[2]
    head_rows = EARLY * (rows // CHUNKS)
    blocks = head_rows // BLOCK
    vmem = pl.BlockSpec(memory_space=pltpu.VMEM)
    hbm = pl.BlockSpec(memory_space=pl.ANY)
    dma = pltpu.SemaphoreType.DMA
    table = pltpu.VMEM((rows, kd), F32)
    cache = jax.ShapeDtypeStruct(k_cache.shape, BF16)
    return pl.pallas_call(
        first_kernel,
        in_specs=[hbm] * 11,
        out_specs=[vmem] * 6 + [hbm, hbm],
        out_shape=[pltpu.VMEM((head_rows, qd), BF16), pltpu.VMEM(w_out.shape[1:], BF16), table, table, table,
                   pltpu.VMEM((rows, qd + 2 * kd), BF16), cache, cache],
        scratch_shapes=[
            pltpu.VMEM((rows, d), BF16), pltpu.VMEM(attn_norm.shape, BF16), pltpu.VMEM((d, qd), BF16),
            pltpu.VMEM((d, kd), BF16), pltpu.VMEM((d, kd), BF16),
            pltpu.SMEM((rows,), jnp.int32), pltpu.VMEM((rows // kd, kd), jnp.int32), pltpu.VMEM((2, kd), F32),
            pltpu.VMEM((head_rows, seq, kd), BF16), pltpu.VMEM((head_rows, seq, kd), BF16),
            dma((9,)), dma((2, blocks)), dma((2, blocks)),
        ],
        compiler_params=pltpu.CompilerParams(vmem_limit_bytes=FIRST_BYTES),
        name="first",
    )(*in_hbm(positions, hidden, attn_norm, w_query, w_key, w_value, w_out, positions.reshape(rows // kd, kd),
              jnp.asarray(rope_rows(kd)), k_cache, v_cache))


def cache_kernel(x_ref, k_ref, v_ref, k0_ref, v0_ref, k_prev, v_prev, x_hbm, ko_hbm, vo_hbm, out_sem, x_sem):
    batch = k_ref.shape[0]
    late = k0_ref.shape[0]
    jobs = [(src, dst, 1, i, i) for i in range(0, batch, BLOCK) for src, dst in ((k_ref, ko_hbm), (v_ref, vo_hbm))]
    jobs += [(src, dst, 0, i, batch - late + i) for i in range(0, late, BLOCK)
             for src, dst in ((k0_ref, ko_hbm), (v0_ref, vo_hbm))]
    writes = [pltpu.make_async_copy(x_ref, x_hbm, x_sem.at[0])]
    for n, (src, dst, layer, i, o) in enumerate(jobs):
        writes.append(pltpu.make_async_copy(src.at[pl.ds(i, BLOCK)], dst.at[layer, pl.ds(o, BLOCK)], out_sem.at[n]))
    for cp in writes:
        cp.start()
    for cp in writes:
        cp.wait()


def write_cache(x, k_layer, v_layer, k_late, v_late, k_prev, v_prev):
    blocks = (k_layer.shape[0] + k_late.shape[0]) // BLOCK
    vmem = pl.BlockSpec(memory_space=pltpu.VMEM)
    hbm = pl.BlockSpec(memory_space=pl.ANY)
    dma = pltpu.SemaphoreType.DMA
    return pl.pallas_call(
        cache_kernel,
        in_specs=[vmem] * 5 + [hbm, hbm],
        out_specs=[hbm] * 3,
        out_shape=[jax.ShapeDtypeStruct(a.shape, BF16) for a in (x, k_prev, v_prev)],
        input_output_aliases={5: 1, 6: 2},
        scratch_shapes=[dma((2 * blocks,)), dma((1,))],
        compiler_params=pltpu.CompilerParams(vmem_limit_bytes=2 * 1024 * 1024),
        name="write_cache",
    )(x, k_layer, v_layer, k_late, v_late, k_prev, v_prev)


ORDER = (
    "O00O01P00A03P01B03O03A02P03B02O02S00P02S03S01F00",
    "G00g00S02D00F03P10G03F01g03D03G01P13g01F02S10D01",
    "G02P11g02S13D02F10P12Q20A20S11B20O20F13P20Q23A23",
    "S12B23O23F11P23Q21A21B21S20O21F12P21Q22A22S23B22",
    "O22F20P22G20S21g20F23D20G23S22g23P30F21D23G21P33",
    "g21F22D21G22P31S30g22D22P32S31S33F30S32F31E30F33",
    "E33F32E31E32",
)


def body_kernel(
    o_first, wo_first, cos, sin, posc, qkv_first, pos_hbm, x_hbm, gm_hbm, ga_hbm, wo_hbm, wg_hbm, wu_hbm, wd_hbm, wq_hbm, wk_hbm, wv_hbm, k_hbm, v_hbm,
    x_out, kbuf, vbuf, kbuf0, vbuf0,
    wo, wg, wu, wd, wq, wk, wv, o_s, xres, part, hbuf, hst, abuf, qkv_s, d2d_in, rs_out, rs_in, acc,
    gm, ga, pos_s,
    w_sem, x_sem, kv_sem, t_sem, d2d_s, d2d_r, rs_s, rs_r, ag_s, ag_r, fw_s, fw_r,
):
    chunks, _, _, own, d = part.shape
    rows = 8 * own
    ff = wg.shape[1]
    head = kbuf.shape[2]
    me = lax.axis_index("tp")
    group = lax.axis_index("dp")
    core = me % 2
    chip = me // 2
    chips = [chip, chip + 1 - 2 * (chip % 2), (chip + 2) % 4, 3 - chip]
    partner = (group, chip * 2 + 1 - core)
    peers = [None] + [(group, chips[k] * 2 + core) for k in (1, 2, 3)]
    order = (3, 1, 2)

    loads = {}

    def load(name, src, dst, sem):
        loads[name] = pltpu.make_async_copy(src, dst, sem)
        loads[name].start()

    def need(*names):
        for name in names:
            if name in loads:
                loads.pop(name).wait()

    load("pos", pos_hbm, pos_s, t_sem.at[2])
    load("gm", gm_hbm, gm, t_sem.at[0])
    early = kbuf.shape[0] - kbuf0.shape[0]

    def load_kv(layer, i):
        at = pl.ds(i * BLOCK, BLOCK)
        if layer:
            k_to, v_to = kbuf.at[at], vbuf.at[at]
        else:
            at0 = pl.ds(i * BLOCK - early, BLOCK)
            k_to, v_to = kbuf0.at[at0], vbuf0.at[at0]
        load(("k", layer, i), k_hbm.at[layer, at], k_to, kv_sem.at[2 * layer, i])
        load(("v", layer, i), v_hbm.at[layer, at], v_to, kv_sem.at[2 * layer + 1, i])

    for i in range(early // BLOCK, kbuf.shape[0] // BLOCK):
        load_kv(0, i)
    for q in range(chunks):
        load(("x", q), x_hbm.at[q, core, chip], xres.at[q], x_sem.at[q])
    load("wg", wg_hbm.at[0], wg, w_sem.at[1])
    load("wu", wu_hbm.at[0], wu, w_sem.at[2])
    load("wd", wd_hbm.at[0], wd, w_sem.at[3])
    load("ga", ga_hbm, ga, t_sem.at[1])
    load("wq", wq_hbm.at[1], wq, w_sem.at[4])
    load("wk", wk_hbm.at[1], wk, w_sem.at[5])
    load("wv", wv_hbm.at[1], wv, w_sem.at[6])
    load("wo", wo_hbm.at[1], wo, w_sem.at[0])

    barrier = pltpu.get_barrier_semaphore()
    for dev in [partner] + peers[1:]:
        pl.semaphore_signal(barrier, inc=1, device_id=dev, device_id_type=MESH)
    pl.semaphore_wait(barrier, 4)

    def remote(src, dst, s, r, dev):
        return pltpu.make_async_remote_copy(
            src_ref=src, dst_ref=dst, send_sem=s, recv_sem=r, device_id=dev, device_id_type=MESH)

    def d2d(q, n):
        cols = pl.ds(pl.multiple_of(n * COLS, COLS), COLS)
        return remote(part.at[q, 1 - core, :, :, cols], d2d_in.at[q, :, :, cols], d2d_s.at[q, n], d2d_r.at[q, n], partner)

    def rs(q, k):
        return remote(rs_out.at[q, k - 1], rs_in.at[q, k - 1], rs_s.at[q, k - 1], rs_r.at[q, k - 1], peers[k])

    def ag(q, k):
        ref = hbuf.at[q, core, chip]
        return remote(ref, ref, ag_s.at[q, k - 1], ag_r.at[q, k - 1], peers[k])

    def ag_in(q, k):
        ref = hbuf.at[q, core, chips[k]]
        return remote(ref, ref, ag_s.at[q, k - 1], ag_r.at[q, k - 1], peers[k])

    def fw(q, k):
        ref = hbuf.at[q, core, chips[k]]
        return remote(ref, ref, fw_s.at[q, k], fw_r.at[q, k], partner)

    def fw_in(q, k):
        ref = hbuf.at[q, 1 - core, chips[k]]
        return remote(ref, ref, fw_s.at[q, k], fw_r.at[q, k], partner)

    def put_part(q, cols, value):
        for p in range(2):
            for c in range(4):
                at = (p * 4 + c) * own
                part[q, p, c, :, cols] = value[at:at + own].astype(BF16)

    def pair_sums(q):
        for n in range(d // COLS):
            d2d(q, n).wait_recv()
        for k in order:
            pair = part[q, core, chips[k]].astype(F32) + d2d_in[q, chips[k]].astype(F32)
            rs_out[q, k - 1] = pair.astype(BF16)
            rs(q, k).start()
        acc[q] = part[q, core, chip].astype(F32) + d2d_in[q, chip].astype(F32)
        for n in range(d // COLS):
            d2d(q, n).wait_send()

    def totals(a, q):
        for k in (1, 2, 3):
            rs(q, k).wait_recv()
        need(("x", q))
        total = acc[q]
        for k in (1, 2, 3):
            total = total + rs_in[q, k - 1].astype(F32)
        x = (xres[q].astype(F32) + total.astype(BF16).astype(F32)).astype(BF16)
        if a == 3:
            hbuf[q, core, chip] = x
        else:
            xres[q] = x
            if a == 1:
                need("ga")
                gain = ga[1:2, :]
            else:
                need("gm")
                gain = gm[a // 2:a // 2 + 1, :]
            hbuf[q, core, chip] = normed(x, gain.astype(F32))
        for k in order:
            ag(q, k).start()
        fw(q, 0).start()
        for k in (1, 2, 3):
            rs(q, k).wait_send()

    def forward(q):
        for k in (1, 2, 3):
            ag_in(q, k).wait_recv()
            fw(q, k).start()

    def gathered(q):
        for k in range(4):
            fw_in(q, k).wait_recv()
        for k in (1, 2, 3):
            ag(q, k).wait_send()
        for k in range(4):
            fw(q, k).wait_send()

    def stage(q):
        gathered(q)
        hst[q] = hbuf[q].reshape(rows, d)

    def out_product(a, q):
        if a:
            need("wo")
        o = o_first if a == 0 and q < EARLY else o_s
        w = wo if a else wo_first

        @pl.loop(0, d // COLS)
        def _(n):
            cols = pl.ds(pl.multiple_of(n * COLS, COLS), COLS)
            put_part(q, cols, jnp.dot(o[q * rows:(q + 1) * rows, :], w[:, cols], preferred_element_type=F32))
            d2d(q, n).start()

    def gate_up(q, half):
        if half == 0:
            stage(q)
            need("wg", "wu")
        steps_n = ff // 512

        @pl.loop(half * steps_n, (half + 1) * steps_n)
        def _(n):
            cols = pl.ds(pl.multiple_of(n * 256, 256), 256)
            h = hst[q]
            g = jnp.dot(h, wg[:, cols], preferred_element_type=F32).astype(BF16).astype(F32)
            u = jnp.dot(h, wu[:, cols], preferred_element_type=F32).astype(BF16).astype(F32)
            abuf[q, :, cols] = (g * jax.nn.sigmoid(g) * u).astype(BF16)

    def down(q):
        need("wd")

        @pl.loop(0, d // COLS)
        def _(n):
            cols = pl.ds(pl.multiple_of(n * COLS, COLS), COLS)
            put_part(q, cols, jnp.dot(abuf[q], wd[:, cols], preferred_element_type=F32))
            d2d(q, n).start()

    def qkv(q):
        stage(q)
        need("wq", "wk", "wv")
        qd, kd = wq.shape[1], wk.shape[1]
        h = hst[q]
        qkv_s[q, :, 0:qd] = jnp.dot(h, wq[...], preferred_element_type=F32).astype(BF16)
        qkv_s[q, :, qd:qd + kd] = jnp.dot(h, wk[...], preferred_element_type=F32).astype(BF16)
        qkv_s[q, :, qd + kd:] = jnp.dot(h, wv[...], preferred_element_type=F32).astype(BF16)

    def attend(a, q, i):
        need("pos")
        source, k_ref, v_ref, offset = (qkv_s.at[q], kbuf, vbuf, 0) if a else (qkv_first, kbuf0, vbuf0, early)
        half = rows // 2
        for j in range(half // BLOCK):
            base = q * rows + i * half + j * BLOCK
            block = base // BLOCK
            need(("k", a // 2, block), ("v", a // 2, block))
            at = slice(base, base + BLOCK)
            first_row = base - q * rows if a else base

            def k_put(b, value):
                k_ref[base - offset + b] = value

            def v_put(b, value):
                v_ref[base - offset + b] = value

            o = attend_block(
                source[first_row:first_row + BLOCK, :], cos[at, :], sin[at, :], posc[at, :], lambda b: pos_s[base + b],
                lambda b: k_ref[base - offset + b], lambda b: v_ref[base - offset + b], k_put, v_put)
            for h, o_h in enumerate(o):
                o_s[at, h * head:(h + 1) * head] = o_h

    def result(q):
        gathered(q)
        x_out[q] = hbuf[q]

    steps = [line[i:i + 3] for line in ORDER for i in range(0, len(line), 3)]
    last = {name: max(i for i, s in enumerate(steps) if s[0] == name and s[1] == "0") for name in "OgD"}
    for i, code in enumerate(steps):
        name, a, q = code[0], int(code[1]), int(code[2])
        if name == "O":
            out_product(a, q)
        elif name == "P":
            pair_sums(q)
        elif name == "S":
            totals(a, q)
        elif name == "F":
            forward(q)
        elif name in "Gg":
            gate_up(q, "Gg".index(name))
        elif name == "D":
            down(q)
        elif name == "Q":
            qkv(q)
        elif name in "AB":
            attend(a, q, "AB".index(name))
        else:
            result(q)
        if i == last["O"]:
            for j in range(kbuf.shape[0] // BLOCK):
                load_kv(1, j)
        if i == last["g"]:
            load("wg", wg_hbm.at[1], wg, w_sem.at[1])
            load("wu", wu_hbm.at[1], wu, w_sem.at[2])
        if i == last["D"]:
            load("wd", wd_hbm.at[1], wd, w_sem.at[3])


def body(positions, o, wo_first, x, mlp_norm, attn_norm, w_out, w_gate, w_up, w_down, w_query, w_key, w_value, k_cache, v_cache, tables, qkv):
    batch, seq, kd = k_cache.shape[1:]
    qd = o.shape[1]
    d = w_out.shape[2]
    ff = w_gate.shape[2]
    own = batch // (8 * CHUNKS)
    rows = 8 * own
    vmem = pl.BlockSpec(memory_space=pltpu.VMEM)
    hbm = pl.BlockSpec(memory_space=pl.ANY)
    dma = pltpu.SemaphoreType.DMA
    cache = pltpu.VMEM((batch, seq, kd), BF16)
    late = pltpu.VMEM((batch - o.shape[0], seq, kd), BF16)
    return pl.pallas_call(
        body_kernel,
        in_specs=[vmem] * 6 + [hbm] * 13,
        out_specs=[vmem] * 5,
        out_shape=[pltpu.VMEM((CHUNKS, 2, 4, own, d), BF16), cache, cache, late, late],
        scratch_shapes=[
            pltpu.VMEM((qd, d), BF16), pltpu.VMEM((d, ff), BF16), pltpu.VMEM((d, ff), BF16), pltpu.VMEM((ff, d), BF16),
            pltpu.VMEM((d, qd), BF16), pltpu.VMEM((d, kd), BF16), pltpu.VMEM((d, kd), BF16),
            pltpu.VMEM((batch, qd), BF16),
            pltpu.VMEM((CHUNKS, own, d), BF16),
            pltpu.VMEM((CHUNKS, 2, 4, own, d), BF16),
            pltpu.VMEM((CHUNKS, 2, 4, own, d), BF16),
            pltpu.VMEM((CHUNKS, rows, d), BF16),
            pltpu.VMEM((CHUNKS, rows, ff), BF16),
            pltpu.VMEM((CHUNKS, rows, qd + 2 * kd), BF16),
            pltpu.VMEM((CHUNKS, 4, own, d), BF16),
            pltpu.VMEM((CHUNKS, 3, own, d), BF16),
            pltpu.VMEM((CHUNKS, 3, own, d), BF16),
            pltpu.VMEM((CHUNKS, own, d), F32),
            pltpu.VMEM(mlp_norm.shape, BF16), pltpu.VMEM(attn_norm.shape, BF16), pltpu.SMEM((batch,), jnp.int32),
            dma((7,)), dma((CHUNKS,)), dma((4, batch // BLOCK)), dma((3,)),
            dma((CHUNKS, d // COLS)), dma((CHUNKS, d // COLS)),
            dma((CHUNKS, 3)), dma((CHUNKS, 3)),
            dma((CHUNKS, 3)), dma((CHUNKS, 3)),
            dma((CHUNKS, 4)), dma((CHUNKS, 4)),
        ],
        compiler_params=pltpu.CompilerParams(vmem_limit_bytes=BODY_BYTES, collective_id=0, has_side_effects=True),
        name="body",
    )(*on_chip(o, wo_first, *tables, qkv),
      *in_hbm(positions, x, mlp_norm, attn_norm, w_out, w_gate, w_up, w_down, w_query, w_key, w_value, k_cache, v_cache))


def solution(mesh):
    row_spec = P('dp', None)
    pos_spec = P('dp')
    cache_spec = P(None, 'dp', None, 'tp', None)
    norm_spec = P(None, None)
    col_spec = P(None, None, 'tp')
    split_rows = P(None, 'tp', None)

    def local_step(hidden, positions, k_cache, v_cache, attn_norm, w_query, w_key, w_value, w_out, mlp_norm, w_gate, w_up, w_down):
        layers, batch, seq, _, head = k_cache.shape
        d = hidden.shape[1]
        own = batch // (8 * CHUNKS)
        kc = k_cache.reshape(layers, batch, seq, head)
        vc = v_cache.reshape(layers, batch, seq, head)
        o, wo_first, *tables, qkv, k_out, v_out = first(hidden, attn_norm, w_query, w_key, w_value, w_out, positions, kc, vc)
        x = hidden.reshape(CHUNKS, 2, 4, own, d)
        x_out, *caches = body(positions, o, wo_first, x, mlp_norm, attn_norm, w_out, w_gate, w_up, w_down,
                              w_query, w_key, w_value, kc, vc, tables, qkv)
        x_out, k_out, v_out = write_cache(x_out.reshape(batch, d), *caches, k_out, v_out)
        return x_out, k_out.reshape(k_cache.shape), v_out.reshape(v_cache.shape)

    return jax.shard_map(local_step, mesh=mesh, in_specs=(row_spec, pos_spec, cache_spec, cache_spec, norm_spec, col_spec, col_spec, col_spec, split_rows, norm_spec, col_spec, col_spec, split_rows), out_specs=(row_spec, cache_spec, cache_spec), check_vma=False)
```

```python
import functools
import math

import jax
import jax.numpy as jnp
import numpy as np
from jax import lax
from jax.experimental import pallas as pl
from jax.experimental.pallas import tpu as pltpu
from jax.sharding import PartitionSpec as P

F32 = jnp.float32
BF16 = jnp.bfloat16
MESH = pl.DeviceIdType.MESH
VMEM_BYTES = 64 * 1024 * 1024 - 128 * 1024
BODY_BYTES = 34 * 1024 * 1024
FIRST_BYTES = 24 * 1024 * 1024
EPS = 1e-5
CHUNKS = 4
EARLY = 2
COLS = 1024


def in_hbm(*arrays):
    return [pltpu.with_memory_space_constraint(a, pltpu.HBM) for a in arrays]


def on_chip(*arrays):
    return [pltpu.with_memory_space_constraint(a, pltpu.VMEM) for a in arrays]


def rope_rows(head_dim):
    half_dim = head_dim // 2
    f32 = np.float32
    inv_freq = np.power(f32(500000.0), -np.arange(half_dim, dtype=f32) * f32(2.0 / head_dim))
    wavelen = f32(2.0 * math.pi) / inv_freq
    smooth = (f32(8192.0) / wavelen - f32(1.0)) / f32(3.0)
    blended = (f32(1.0) - smooth) * inv_freq / f32(8.0) + smooth * inv_freq
    scaled = np.where(wavelen < 2048.0, inv_freq, np.where(wavelen > 8192.0, inv_freq / f32(8.0), blended)).astype(f32)
    ones = np.ones(half_dim, f32)
    return np.stack([np.concatenate([scaled, scaled]), np.concatenate([-ones, ones])])


def normed(x, gain):
    xf = x.astype(F32)
    mean_sq = jnp.mean(xf * xf, axis=-1, keepdims=True)
    return (xf * lax.rsqrt(mean_sq + EPS) * gain).astype(BF16)


BLOCK = 32


def attend_block(qkv, cos, sin, posc, pos_at, k_at, v_at, k_put, v_put):
    head = cos.shape[1]
    seq = k_at(0).shape[0]
    heads = qkv.shape[1] // head - 2
    scale = head ** -0.5

    def rope(vec):
        vec = vec.astype(F32)
        return vec * cos + pltpu.roll(vec, head // 2, 1) * sin

    qs = [rope(qkv[:, h * head:(h + 1) * head]) for h in range(heads)]
    kn = rope(qkv[:, heads * head:(heads + 1) * head])
    vn = qkv[:, (heads + 1) * head:(heads + 2) * head].astype(F32)

    tiles = (seq // 16, 16, head)
    seq_ids = lax.broadcasted_iota(jnp.int32, tiles, 0) * 16 + lax.broadcasted_iota(jnp.int32, tiles, 1)
    seq_bf = seq_ids.astype(F32).astype(BF16)
    row_of = lax.broadcasted_iota(jnp.int32, (32, head), 0) % 8
    lane = lax.broadcasted_iota(jnp.int32, (32, seq), 1).astype(F32)

    def updated(cache, row, b):
        here = seq_bf == jnp.full((16, head), pos_at(b).astype(F32), F32).astype(BF16)[None]
        row = jnp.broadcast_to(row, (16, head)).astype(BF16)[None]
        return jnp.where(here, row, cache.reshape(tiles)).reshape(seq, head)

    all_scores = []
    for j in range(BLOCK // 8):
        pieces = [q[8 * j:8 * j + 8] for q in qs] + [jnp.zeros((8, head), F32)] * (4 - heads)
        qj = jnp.concatenate(pieces, axis=0).astype(BF16)
        scores = None
        for b8 in range(8):
            b = 8 * j + b8
            k_b = updated(k_at(b), kn[b:b + 1], b)
            k_put(b, k_b)
            s_b = lax.dot_general(qj, k_b, (((1,), (1,)), ((), ())), preferred_element_type=F32)
            scores = s_b if scores is None else jnp.where(row_of == b8, s_b, scores)
        all_scores.append(scores)
    probs = []
    for j in range(BLOCK // 8):
        limit = jnp.concatenate([posc[8 * j:8 * j + 8]] * 4, axis=0)
        scores = jnp.where(lane <= limit, all_scores[j] * scale, -jnp.inf)
        peak = jnp.max(scores, axis=1, keepdims=True)
        weight = jnp.exp(scores - peak)
        total = jnp.sum(weight, axis=1, keepdims=True)
        probs.append((weight * (1.0 / total)).astype(BF16))
    outs = []
    for j in range(BLOCK // 8):
        mixed = None
        for b8 in range(8):
            b = 8 * j + b8
            v_b = updated(v_at(b), vn[b:b + 1], b)
            v_put(b, v_b)
            o_b = jnp.dot(probs[j], v_b, preferred_element_type=F32)
            mixed = o_b if mixed is None else jnp.where(row_of == b8, o_b, mixed)
        outs.append(mixed)
    o = [jnp.concatenate([m[8 * h:8 * h + 8] for m in outs], axis=0).astype(BF16) for h in range(heads)]
    return o


def first_kernel(
    pos_hbm, x_hbm, g_hbm, wq_hbm, wk_hbm, wv_hbm, wo_hbm, pos2_hbm, rope_hbm, k_hbm, v_hbm,
    o_ref, wo_ref, cos_ref, sin_ref, posc_ref, qkv_ref, ko_hbm, vo_hbm,
    h_ref, g_ref, wq, wk, wv, pos_s, pos_ref, rope_ref, kbuf, vbuf, sem, in_sem, out_sem,
):
    rows = h_ref.shape[0]
    qd = wq.shape[1]
    kd = wk.shape[1]
    blocks = kbuf.shape[0] // BLOCK
    copies = [pltpu.make_async_copy(src, dst, sem.at[i]) for i, (src, dst) in enumerate(
        [(x_hbm, h_ref), (g_hbm, g_ref), (wq_hbm.at[0], wq), (wk_hbm.at[0], wk), (wv_hbm.at[0], wv)])]
    small = [pltpu.make_async_copy(src, dst, sem.at[i]) for i, (src, dst) in enumerate(
        [(pos_hbm, pos_s), (pos2_hbm, pos_ref), (rope_hbm, rope_ref)], 6)]
    for cp in copies[:2] + small + copies[2:]:
        cp.start()

    def reads(i):
        at = pl.ds(i * BLOCK, BLOCK)
        return (pltpu.make_async_copy(k_hbm.at[0, at], kbuf.at[at], in_sem.at[0, i]),
                pltpu.make_async_copy(v_hbm.at[0, at], vbuf.at[at], in_sem.at[1, i]))

    def writes(i):
        at = pl.ds(i * BLOCK, BLOCK)
        return (pltpu.make_async_copy(kbuf.at[at], ko_hbm.at[0, at], out_sem.at[0, i]),
                pltpu.make_async_copy(vbuf.at[at], vo_hbm.at[0, at], out_sem.at[1, i]))

    for cp in small:
        cp.wait()
    width = pos_ref.shape[1]
    diagonal = (lax.broadcasted_iota(jnp.int32, (width, width), 0) == lax.broadcasted_iota(jnp.int32, (width, width), 1))
    for i in range(rows // width):
        across = jnp.broadcast_to(pos_ref[i:i + 1, :].astype(F32), (width, width))
        down = jnp.sum(jnp.where(diagonal, across, 0.0), axis=1, keepdims=True)
        at = slice(i * width, (i + 1) * width)
        angles = down * rope_ref[0:1, :]
        posc_ref[at, :] = jnp.broadcast_to(down, (width, width))
        cos_ref[at, :] = jnp.cos(angles)
        sin_ref[at, :] = jnp.sin(angles) * rope_ref[1:2, :]

    copies[0].wait()
    copies[1].wait()
    for i in range(blocks):
        for cp in reads(i):
            cp.start()
    wo_copy = pltpu.make_async_copy(wo_hbm.at[0], wo_ref, sem.at[5])
    wo_copy.start()
    gain = g_ref[0:1, :].astype(F32)

    @pl.loop(0, rows // 16)
    def _(i):
        sl = pl.ds(pl.multiple_of(i * 16, 16), 16)
        h_ref[sl, :] = normed(h_ref[sl, :], gain)

    h = h_ref[...]
    copies[2].wait()
    qkv_ref[:, 0:qd] = jnp.dot(h, wq[...], preferred_element_type=F32).astype(BF16)
    copies[3].wait()
    copies[4].wait()
    qkv_ref[:, qd:qd + kd] = jnp.dot(h, wk[...], preferred_element_type=F32).astype(BF16)
    qkv_ref[:, qd + kd:] = jnp.dot(h, wv[...], preferred_element_type=F32).astype(BF16)

    @pl.loop(0, blocks)
    def _(i):
        base = pl.multiple_of(i * BLOCK, BLOCK)
        at = pl.ds(base, BLOCK)
        for cp in reads(i):
            cp.wait()

        def k_put(b, value):
            kbuf[base + b] = value

        def v_put(b, value):
            vbuf[base + b] = value

        o = attend_block(
            qkv_ref[at, :], cos_ref[at, :], sin_ref[at, :], posc_ref[at, :], lambda b: pos_s[base + b],
            lambda b: kbuf[base + b], lambda b: vbuf[base + b], k_put, v_put)
        for n, o_n in enumerate(o):
            o_ref[at, n * kd:(n + 1) * kd] = o_n
        for cp in writes(i):
            cp.start()

    for i in range(blocks):
        for cp in writes(i):
            cp.wait()
    wo_copy.wait()


def first(hidden, attn_norm, w_query, w_key, w_value, w_out, positions, k_cache, v_cache):
    rows, d = hidden.shape
    qd, kd = w_query.shape[2], w_key.shape[2]
    seq = k_cache.shape[2]
    head_rows = EARLY * (rows // CHUNKS)
    blocks = head_rows // BLOCK
    vmem = pl.BlockSpec(memory_space=pltpu.VMEM)
    hbm = pl.BlockSpec(memory_space=pl.ANY)
    dma = pltpu.SemaphoreType.DMA
    table = pltpu.VMEM((rows, kd), F32)
    cache = jax.ShapeDtypeStruct(k_cache.shape, BF16)
    return pl.pallas_call(
        first_kernel,
        in_specs=[hbm] * 11,
        out_specs=[vmem] * 6 + [hbm, hbm],
        out_shape=[pltpu.VMEM((head_rows, qd), BF16), pltpu.VMEM(w_out.shape[1:], BF16), table, table, table,
                   pltpu.VMEM((rows, qd + 2 * kd), BF16), cache, cache],
        scratch_shapes=[
            pltpu.VMEM((rows, d), BF16), pltpu.VMEM(attn_norm.shape, BF16), pltpu.VMEM((d, qd), BF16),
            pltpu.VMEM((d, kd), BF16), pltpu.VMEM((d, kd), BF16),
            pltpu.SMEM((rows,), jnp.int32), pltpu.VMEM((rows // kd, kd), jnp.int32), pltpu.VMEM((2, kd), F32),
            pltpu.VMEM((head_rows, seq, kd), BF16), pltpu.VMEM((head_rows, seq, kd), BF16),
            dma((9,)), dma((2, blocks)), dma((2, blocks)),
        ],
        compiler_params=pltpu.CompilerParams(vmem_limit_bytes=FIRST_BYTES),
        name="first",
    )(*in_hbm(positions, hidden, attn_norm, w_query, w_key, w_value, w_out, positions.reshape(rows // kd, kd),
              jnp.asarray(rope_rows(kd)), k_cache, v_cache))


def cache_kernel(x_ref, k_ref, v_ref, k0_ref, v0_ref, k_prev, v_prev, x_hbm, ko_hbm, vo_hbm, out_sem, x_sem):
    batch = k_ref.shape[0]
    late = k0_ref.shape[0]
    jobs = [(src, dst, 1, i, i) for i in range(0, batch, BLOCK) for src, dst in ((k_ref, ko_hbm), (v_ref, vo_hbm))]
    jobs += [(src, dst, 0, i, batch - late + i) for i in range(0, late, BLOCK)
             for src, dst in ((k0_ref, ko_hbm), (v0_ref, vo_hbm))]
    writes = [pltpu.make_async_copy(x_ref, x_hbm, x_sem.at[0])]
    for n, (src, dst, layer, i, o) in enumerate(jobs):
        writes.append(pltpu.make_async_copy(src.at[pl.ds(i, BLOCK)], dst.at[layer, pl.ds(o, BLOCK)], out_sem.at[n]))
    for cp in writes:
        cp.start()
    for cp in writes:
        cp.wait()


def write_cache(x, k_layer, v_layer, k_late, v_late, k_prev, v_prev):
    blocks = (k_layer.shape[0] + k_late.shape[0]) // BLOCK
    vmem = pl.BlockSpec(memory_space=pltpu.VMEM)
    hbm = pl.BlockSpec(memory_space=pl.ANY)
    dma = pltpu.SemaphoreType.DMA
    return pl.pallas_call(
        cache_kernel,
        in_specs=[vmem] * 5 + [hbm, hbm],
        out_specs=[hbm] * 3,
        out_shape=[jax.ShapeDtypeStruct(a.shape, BF16) for a in (x, k_prev, v_prev)],
        input_output_aliases={5: 1, 6: 2},
        scratch_shapes=[dma((2 * blocks,)), dma((1,))],
        compiler_params=pltpu.CompilerParams(vmem_limit_bytes=2 * 1024 * 1024),
        name="write_cache",
    )(x, k_layer, v_layer, k_late, v_late, k_prev, v_prev)


ORDER = (
    "O00O01P00A03P01B03O03A02P03B02O02S00P02S03S01F00",
    "G00g00S02D00F03P10G03F01g03D03G01P13g01F02S10D01",
    "G02P11g02S13D02F10P12Q20A20S11B20O20F13P20Q23A23",
    "S12B23O23F11P23Q21A21B21S20O21F12P21Q22A22S23B22",
    "O22F20P22G20S21g20F23D20G23S22g23P30F21D23G21P33",
    "g21F22D21G22P31S30g22D22P32S31S33F30S32F31E30F33",
    "E33F32E31E32",
)


def body_kernel(
    o_first, wo_first, cos, sin, posc, qkv_first, pos_hbm, x_hbm, gm_hbm, ga_hbm, wo_hbm, wg_hbm, wu_hbm, wd_hbm, wq_hbm, wk_hbm, wv_hbm, k_hbm, v_hbm,
    x_out, kbuf, vbuf, kbuf0, vbuf0,
    wo, wg, wu, wd, wq, wk, wv, o_s, xres, part, hbuf, hst, abuf, qkv_s, d2d_in, rs_out, rs_in, acc,
    gm, ga, pos_s,
    w_sem, x_sem, kv_sem, t_sem, d2d_s, d2d_r, rs_s, rs_r, ag_s, ag_r, fw_s, fw_r,
):
    chunks, _, _, own, d = part.shape
    rows = 8 * own
    ff = wg.shape[1]
    head = kbuf.shape[2]
    me = lax.axis_index("tp")
    group = lax.axis_index("dp")
    core = me % 2
    chip = me // 2
    chips = [chip, chip + 1 - 2 * (chip % 2), (chip + 2) % 4, 3 - chip]
    partner = (group, chip * 2 + 1 - core)
    peers = [None] + [(group, chips[k] * 2 + core) for k in (1, 2, 3)]
    order = (3, 1, 2)

    loads = {}

    def load(name, src, dst, sem):
        loads[name] = pltpu.make_async_copy(src, dst, sem)
        loads[name].start()

    def need(*names):
        for name in names:
            if name in loads:
                loads.pop(name).wait()

    load("pos", pos_hbm, pos_s, t_sem.at[2])
    load("gm", gm_hbm, gm, t_sem.at[0])
    early = kbuf.shape[0] - kbuf0.shape[0]

    def load_kv(layer, i):
        at = pl.ds(i * BLOCK, BLOCK)
        if layer:
            k_to, v_to = kbuf.at[at], vbuf.at[at]
        else:
            at0 = pl.ds(i * BLOCK - early, BLOCK)
            k_to, v_to = kbuf0.at[at0], vbuf0.at[at0]
        load(("k", layer, i), k_hbm.at[layer, at], k_to, kv_sem.at[2 * layer, i])
        load(("v", layer, i), v_hbm.at[layer, at], v_to, kv_sem.at[2 * layer + 1, i])

    steps = [line[i:i + 3] for line in ORDER for i in range(0, len(line), 3)]
    for code in steps:
        if code[0] in "AB" and code[1] == "0":
            load_kv(0, (int(code[2]) * rows + "AB".index(code[0]) * rows // 2) // BLOCK)
    for q in range(chunks):
        load(("x", q), x_hbm.at[q, core, chip], xres.at[q], x_sem.at[q])
    load("ga", ga_hbm, ga, t_sem.at[1])

    barrier = pltpu.get_barrier_semaphore()
    for dev in [partner] + peers[1:]:
        pl.semaphore_signal(barrier, inc=1, device_id=dev, device_id_type=MESH)
    pl.semaphore_wait(barrier, 4)

    def remote(src, dst, s, r, dev):
        return pltpu.make_async_remote_copy(
            src_ref=src, dst_ref=dst, send_sem=s, recv_sem=r, device_id=dev, device_id_type=MESH)

    def d2d(q, n):
        cols = pl.ds(pl.multiple_of(n * COLS, COLS), COLS)
        return remote(part.at[q, 1 - core, :, :, cols], d2d_in.at[q, :, :, cols], d2d_s.at[q, n], d2d_r.at[q, n], partner)

    def rs(q, k):
        return remote(rs_out.at[q, k - 1], rs_in.at[q, k - 1], rs_s.at[q, k - 1], rs_r.at[q, k - 1], peers[k])

    def ag(q, k):
        ref = hbuf.at[q, core, chip]
        return remote(ref, ref, ag_s.at[q, k - 1], ag_r.at[q, k - 1], peers[k])

    def ag_in(q, k):
        ref = hbuf.at[q, core, chips[k]]
        return remote(ref, ref, ag_s.at[q, k - 1], ag_r.at[q, k - 1], peers[k])

    def fw(q, k):
        ref = hbuf.at[q, core, chips[k]]
        return remote(ref, ref, fw_s.at[q, k], fw_r.at[q, k], partner)

    def fw_in(q, k):
        ref = hbuf.at[q, 1 - core, chips[k]]
        return remote(ref, ref, fw_s.at[q, k], fw_r.at[q, k], partner)

    def put_part(q, cols, value):
        for p in range(2):
            for c in range(4):
                at = (p * 4 + c) * own
                part[q, p, c, :, cols] = value[at:at + own].astype(BF16)

    def pair_sums(q):
        for n in range(d // COLS):
            d2d(q, n).wait_recv()
        for k in order:
            pair = part[q, core, chips[k]].astype(F32) + d2d_in[q, chips[k]].astype(F32)
            rs_out[q, k - 1] = pair.astype(BF16)
            rs(q, k).start()
        acc[q] = part[q, core, chip].astype(F32) + d2d_in[q, chip].astype(F32)
        for n in range(d // COLS):
            d2d(q, n).wait_send()

    def totals(a, q):
        for k in (1, 2, 3):
            rs(q, k).wait_recv()
        need(("x", q))
        total = acc[q]
        for k in (1, 2, 3):
            total = total + rs_in[q, k - 1].astype(F32)
        x = (xres[q].astype(F32) + total.astype(BF16).astype(F32)).astype(BF16)
        if a == 3:
            hbuf[q, core, chip] = x
        else:
            xres[q] = x
            if a == 1:
                need("ga")
                gain = ga[1:2, :]
            else:
                need("gm")
                gain = gm[a // 2:a // 2 + 1, :]
            hbuf[q, core, chip] = normed(x, gain.astype(F32))
        for k in order:
            ag(q, k).start()
        fw(q, 0).start()
        for k in (1, 2, 3):
            rs(q, k).wait_send()

    def forward(q):
        for k in (1, 2, 3):
            ag_in(q, k).wait_recv()
            fw(q, k).start()

    def gathered(q):
        for k in range(4):
            fw_in(q, k).wait_recv()
        for k in (1, 2, 3):
            ag(q, k).wait_send()
        for k in range(4):
            fw(q, k).wait_send()

    def stage(q):
        gathered(q)
        hst[q] = hbuf[q].reshape(rows, d)

    def out_product(a, q):
        if a:
            need("wo")
        o = o_first if a == 0 and q < EARLY else o_s
        w = wo if a else wo_first

        @pl.loop(0, d // COLS)
        def _(n):
            cols = pl.ds(pl.multiple_of(n * COLS, COLS), COLS)
            put_part(q, cols, jnp.dot(o[q * rows:(q + 1) * rows, :], w[:, cols], preferred_element_type=F32))
            d2d(q, n).start()

    def gate_up(q, half):
        if half == 0:
            stage(q)
            need("wg", "wu")
        steps_n = ff // 512

        @pl.loop(half * steps_n, (half + 1) * steps_n)
        def _(n):
            cols = pl.ds(pl.multiple_of(n * 256, 256), 256)
            h = hst[q]
            g = jnp.dot(h, wg[:, cols], preferred_element_type=F32).astype(BF16).astype(F32)
            u = jnp.dot(h, wu[:, cols], preferred_element_type=F32).astype(BF16).astype(F32)
            abuf[q, :, cols] = (g * jax.nn.sigmoid(g) * u).astype(BF16)

    def down(q):
        need("wd")

        @pl.loop(0, d // COLS)
        def _(n):
            cols = pl.ds(pl.multiple_of(n * COLS, COLS), COLS)
            put_part(q, cols, jnp.dot(abuf[q], wd[:, cols], preferred_element_type=F32))
            d2d(q, n).start()

    def qkv(q):
        stage(q)
        need("wq", "wk", "wv")
        qd, kd = wq.shape[1], wk.shape[1]
        h = hst[q]
        qkv_s[q, :, 0:qd] = jnp.dot(h, wq[...], preferred_element_type=F32).astype(BF16)
        qkv_s[q, :, qd:qd + kd] = jnp.dot(h, wk[...], preferred_element_type=F32).astype(BF16)
        qkv_s[q, :, qd + kd:] = jnp.dot(h, wv[...], preferred_element_type=F32).astype(BF16)

    def attend(a, q, i):
        need("pos")
        source, k_ref, v_ref, offset = (qkv_s.at[q], kbuf, vbuf, 0) if a else (qkv_first, kbuf0, vbuf0, early)
        half = rows // 2
        for j in range(half // BLOCK):
            base = q * rows + i * half + j * BLOCK
            block = base // BLOCK
            need(("k", a // 2, block), ("v", a // 2, block))
            at = slice(base, base + BLOCK)
            first_row = base - q * rows if a else base

            def k_put(b, value):
                k_ref[base - offset + b] = value

            def v_put(b, value):
                v_ref[base - offset + b] = value

            o = attend_block(
                source[first_row:first_row + BLOCK, :], cos[at, :], sin[at, :], posc[at, :], lambda b: pos_s[base + b],
                lambda b: k_ref[base - offset + b], lambda b: v_ref[base - offset + b], k_put, v_put)
            for h, o_h in enumerate(o):
                o_s[at, h * head:(h + 1) * head] = o_h

    def result(q):
        gathered(q)
        x_out[q] = hbuf[q]

    last = {name: max(i for i, s in enumerate(steps) if s[0] == name and s[1] == "0") for name in "OgD"}
    first_at = {name: min(i for i, s in enumerate(steps) if s[0] == name) for name in "AGD"}
    for i, code in enumerate(steps):
        name, a, q = code[0], int(code[1]), int(code[2])
        if name == "O":
            out_product(a, q)
        elif name == "P":
            pair_sums(q)
        elif name == "S":
            totals(a, q)
        elif name == "F":
            forward(q)
        elif name in "Gg":
            gate_up(q, "Gg".index(name))
        elif name == "D":
            down(q)
        elif name == "Q":
            qkv(q)
        elif name in "AB":
            attend(a, q, "AB".index(name))
        else:
            result(q)
        if i == first_at["A"]:
            load("wg", wg_hbm.at[0], wg, w_sem.at[1])
            load("wu", wu_hbm.at[0], wu, w_sem.at[2])
        if i == last["O"]:
            load("wd", wd_hbm.at[0], wd, w_sem.at[3])
        if i == first_at["G"]:
            load("wq", wq_hbm.at[1], wq, w_sem.at[4])
            load("wk", wk_hbm.at[1], wk, w_sem.at[5])
            load("wv", wv_hbm.at[1], wv, w_sem.at[6])
            load("wo", wo_hbm.at[1], wo, w_sem.at[0])
        if i == first_at["D"]:
            for j in range(kbuf.shape[0] // BLOCK):
                load_kv(1, j)
        if i == last["g"]:
            load("wg", wg_hbm.at[1], wg, w_sem.at[1])
            load("wu", wu_hbm.at[1], wu, w_sem.at[2])
        if i == last["D"]:
            load("wd", wd_hbm.at[1], wd, w_sem.at[3])


def body(positions, o, wo_first, x, mlp_norm, attn_norm, w_out, w_gate, w_up, w_down, w_query, w_key, w_value, k_cache, v_cache, tables, qkv):
    batch, seq, kd = k_cache.shape[1:]
    qd = o.shape[1]
    d = w_out.shape[2]
    ff = w_gate.shape[2]
    own = batch // (8 * CHUNKS)
    rows = 8 * own
    vmem = pl.BlockSpec(memory_space=pltpu.VMEM)
    hbm = pl.BlockSpec(memory_space=pl.ANY)
    dma = pltpu.SemaphoreType.DMA
    cache = pltpu.VMEM((batch, seq, kd), BF16)
    late = pltpu.VMEM((batch - o.shape[0], seq, kd), BF16)
    return pl.pallas_call(
        body_kernel,
        in_specs=[vmem] * 6 + [hbm] * 13,
        out_specs=[vmem] * 5,
        out_shape=[pltpu.VMEM((CHUNKS, 2, 4, own, d), BF16), cache, cache, late, late],
        scratch_shapes=[
            pltpu.VMEM((qd, d), BF16), pltpu.VMEM((d, ff), BF16), pltpu.VMEM((d, ff), BF16), pltpu.VMEM((ff, d), BF16),
            pltpu.VMEM((d, qd), BF16), pltpu.VMEM((d, kd), BF16), pltpu.VMEM((d, kd), BF16),
            pltpu.VMEM((batch, qd), BF16),
            pltpu.VMEM((CHUNKS, own, d), BF16),
            pltpu.VMEM((CHUNKS, 2, 4, own, d), BF16),
            pltpu.VMEM((CHUNKS, 2, 4, own, d), BF16),
            pltpu.VMEM((CHUNKS, rows, d), BF16),
            pltpu.VMEM((CHUNKS, rows, ff), BF16),
            pltpu.VMEM((CHUNKS, rows, qd + 2 * kd), BF16),
            pltpu.VMEM((CHUNKS, 4, own, d), BF16),
            pltpu.VMEM((CHUNKS, 3, own, d), BF16),
            pltpu.VMEM((CHUNKS, 3, own, d), BF16),
            pltpu.VMEM((CHUNKS, own, d), F32),
            pltpu.VMEM(mlp_norm.shape, BF16), pltpu.VMEM(attn_norm.shape, BF16), pltpu.SMEM((batch,), jnp.int32),
            dma((7,)), dma((CHUNKS,)), dma((4, batch // BLOCK)), dma((3,)),
            dma((CHUNKS, d // COLS)), dma((CHUNKS, d // COLS)),
            dma((CHUNKS, 3)), dma((CHUNKS, 3)),
            dma((CHUNKS, 3)), dma((CHUNKS, 3)),
            dma((CHUNKS, 4)), dma((CHUNKS, 4)),
        ],
        compiler_params=pltpu.CompilerParams(vmem_limit_bytes=BODY_BYTES, collective_id=0, has_side_effects=True),
        name="body",
    )(*on_chip(o, wo_first, *tables, qkv),
      *in_hbm(positions, x, mlp_norm, attn_norm, w_out, w_gate, w_up, w_down, w_query, w_key, w_value, k_cache, v_cache))


def solution(mesh):
    row_spec = P('dp', None)
    pos_spec = P('dp')
    cache_spec = P(None, 'dp', None, 'tp', None)
    norm_spec = P(None, None)
    col_spec = P(None, None, 'tp')
    split_rows = P(None, 'tp', None)

    def local_step(hidden, positions, k_cache, v_cache, attn_norm, w_query, w_key, w_value, w_out, mlp_norm, w_gate, w_up, w_down):
        layers, batch, seq, _, head = k_cache.shape
        d = hidden.shape[1]
        own = batch // (8 * CHUNKS)
        kc = k_cache.reshape(layers, batch, seq, head)
        vc = v_cache.reshape(layers, batch, seq, head)
        o, wo_first, *tables, qkv, k_out, v_out = first(hidden, attn_norm, w_query, w_key, w_value, w_out, positions, kc, vc)
        x = hidden.reshape(CHUNKS, 2, 4, own, d)
        x_out, *caches = body(positions, o, wo_first, x, mlp_norm, attn_norm, w_out, w_gate, w_up, w_down,
                              w_query, w_key, w_value, kc, vc, tables, qkv)
        x_out, k_out, v_out = write_cache(x_out.reshape(batch, d), *caches, k_out, v_out)
        return x_out, k_out.reshape(k_cache.shape), v_out.reshape(v_cache.shape)

    return jax.shard_map(local_step, mesh=mesh, in_specs=(row_spec, pos_spec, cache_spec, cache_spec, norm_spec, col_spec, col_spec, col_spec, split_rows, norm_spec, col_spec, col_spec, split_rows), out_specs=(row_spec, cache_spec, cache_spec), check_vma=False)
```

```python
import functools
import math

import jax
import jax.numpy as jnp
import numpy as np
from jax import lax
from jax.experimental import pallas as pl
from jax.experimental.pallas import tpu as pltpu
from jax.sharding import PartitionSpec as P

F32 = jnp.float32
BF16 = jnp.bfloat16
MESH = pl.DeviceIdType.MESH
VMEM_BYTES = 64 * 1024 * 1024 - 128 * 1024
BODY_BYTES = 36 * 1024 * 1024
FIRST_BYTES = 48 * 1024 * 1024
EPS = 1e-5


def in_hbm(*arrays):
    return [pltpu.with_memory_space_constraint(a, pltpu.HBM) for a in arrays]


def on_chip(*arrays):
    return [pltpu.with_memory_space_constraint(a, pltpu.VMEM) for a in arrays]


def rope_rows(head_dim):
    half_dim = head_dim // 2
    f32 = np.float32
    inv_freq = np.power(f32(500000.0), -np.arange(half_dim, dtype=f32) * f32(2.0 / head_dim))
    wavelen = f32(2.0 * math.pi) / inv_freq
    smooth = (f32(8192.0) / wavelen - f32(1.0)) / f32(3.0)
    blended = (f32(1.0) - smooth) * inv_freq / f32(8.0) + smooth * inv_freq
    scaled = np.where(wavelen < 2048.0, inv_freq, np.where(wavelen > 8192.0, inv_freq / f32(8.0), blended)).astype(f32)
    ones = np.ones(half_dim, f32)
    return np.stack([np.concatenate([scaled, scaled]), np.concatenate([-ones, ones])])


def normed(x, gain):
    xf = x.astype(F32)
    mean_sq = jnp.mean(xf * xf, axis=-1, keepdims=True)
    return (xf * lax.rsqrt(mean_sq + EPS) * gain).astype(BF16)


BLOCK = 32


def attend_block(qkv, cos, sin, posc, pos_at, k_at, v_at, k_put, v_put):
    head = cos.shape[1]
    seq = k_at(0).shape[0]
    heads = qkv.shape[1] // head - 2
    scale = head ** -0.5

    def rope(vec):
        vec = vec.astype(F32)
        return vec * cos + pltpu.roll(vec, head // 2, 1) * sin

    qs = [rope(qkv[:, h * head:(h + 1) * head]) for h in range(heads)]
    kn = rope(qkv[:, heads * head:(heads + 1) * head])
    vn = qkv[:, (heads + 1) * head:(heads + 2) * head].astype(F32)

    tiles = (seq // 16, 16, head)
    seq_ids = lax.broadcasted_iota(jnp.int32, tiles, 0) * 16 + lax.broadcasted_iota(jnp.int32, tiles, 1)
    seq_bf = seq_ids.astype(F32).astype(BF16)
    row_of = lax.broadcasted_iota(jnp.int32, (32, head), 0) % 8
    lane = lax.broadcasted_iota(jnp.int32, (32, seq), 1).astype(F32)

    def updated(cache, row, b):
        here = seq_bf == jnp.full((16, head), pos_at(b).astype(F32), F32).astype(BF16)[None]
        row = jnp.broadcast_to(row, (16, head)).astype(BF16)[None]
        return jnp.where(here, row, cache.reshape(tiles)).reshape(seq, head)

    all_scores = []
    for j in range(BLOCK // 8):
        pieces = [q[8 * j:8 * j + 8] for q in qs] + [jnp.zeros((8, head), F32)] * (4 - heads)
        qj = jnp.concatenate(pieces, axis=0).astype(BF16)
        scores = None
        for b8 in range(8):
            b = 8 * j + b8
            k_b = updated(k_at(b), kn[b:b + 1], b)
            k_put(b, k_b)
            s_b = lax.dot_general(qj, k_b, (((1,), (1,)), ((), ())), preferred_element_type=F32)
            scores = s_b if scores is None else jnp.where(row_of == b8, s_b, scores)
        all_scores.append(scores)
    probs = []
    for j in range(BLOCK // 8):
        limit = jnp.concatenate([posc[8 * j:8 * j + 8]] * 4, axis=0)
        scores = jnp.where(lane <= limit, all_scores[j] * scale, -jnp.inf)
        peak = jnp.max(scores, axis=1, keepdims=True)
        weight = jnp.exp(scores - peak)
        total = jnp.sum(weight, axis=1, keepdims=True)
        probs.append((weight * (1.0 / total)).astype(BF16))
    outs = []
    for j in range(BLOCK // 8):
        mixed = None
        for b8 in range(8):
            b = 8 * j + b8
            v_b = updated(v_at(b), vn[b:b + 1], b)
            v_put(b, v_b)
            o_b = jnp.dot(probs[j], v_b, preferred_element_type=F32)
            mixed = o_b if mixed is None else jnp.where(row_of == b8, o_b, mixed)
        outs.append(mixed)
    o = [jnp.concatenate([m[8 * h:8 * h + 8] for m in outs], axis=0).astype(BF16) for h in range(heads)]
    return o


def first_kernel(
    pos_hbm, x_hbm, g_hbm, wq_hbm, wk_hbm, wv_hbm, wo_hbm, pos2_hbm, rope_hbm, k_hbm, v_hbm,
    o_ref, wo_ref, cos_ref, sin_ref, posc_ref, ko_hbm, vo_hbm,
    h_ref, g_ref, wq, wk, wv, pos_s, pos_ref, rope_ref, qkv_ref, kbuf, vbuf, sem, in_sem, out_sem,
):
    rows = h_ref.shape[0]
    qd = wq.shape[1]
    kd = wk.shape[1]
    blocks = rows // BLOCK
    copies = [pltpu.make_async_copy(src, dst, sem.at[i]) for i, (src, dst) in enumerate(
        [(x_hbm, h_ref), (g_hbm, g_ref), (wq_hbm.at[0], wq), (wk_hbm.at[0], wk), (wv_hbm.at[0], wv)])]
    small = [pltpu.make_async_copy(src, dst, sem.at[i]) for i, (src, dst) in enumerate(
        [(pos_hbm, pos_s), (pos2_hbm, pos_ref), (rope_hbm, rope_ref)], 6)]
    for cp in copies[:2] + small + copies[2:]:
        cp.start()

    def reads(i):
        at = pl.ds(i * BLOCK, BLOCK)
        return (pltpu.make_async_copy(k_hbm.at[0, at], kbuf.at[at], in_sem.at[0, i]),
                pltpu.make_async_copy(v_hbm.at[0, at], vbuf.at[at], in_sem.at[1, i]))

    def writes(i):
        at = pl.ds(i * BLOCK, BLOCK)
        return (pltpu.make_async_copy(kbuf.at[at], ko_hbm.at[0, at], out_sem.at[0, i]),
                pltpu.make_async_copy(vbuf.at[at], vo_hbm.at[0, at], out_sem.at[1, i]))

    for cp in small:
        cp.wait()
    width = pos_ref.shape[1]
    diagonal = (lax.broadcasted_iota(jnp.int32, (width, width), 0) == lax.broadcasted_iota(jnp.int32, (width, width), 1))
    for i in range(rows // width):
        across = jnp.broadcast_to(pos_ref[i:i + 1, :].astype(F32), (width, width))
        down = jnp.sum(jnp.where(diagonal, across, 0.0), axis=1, keepdims=True)
        at = slice(i * width, (i + 1) * width)
        angles = down * rope_ref[0:1, :]
        posc_ref[at, :] = jnp.broadcast_to(down, (width, width))
        cos_ref[at, :] = jnp.cos(angles)
        sin_ref[at, :] = jnp.sin(angles) * rope_ref[1:2, :]

    copies[0].wait()
    copies[1].wait()
    for i in range(blocks):
        for cp in reads(i):
            cp.start()
    wo_copy = pltpu.make_async_copy(wo_hbm.at[0], wo_ref, sem.at[5])
    wo_copy.start()
    gain = g_ref[0:1, :].astype(F32)

    @pl.loop(0, rows // 16)
    def _(i):
        sl = pl.ds(pl.multiple_of(i * 16, 16), 16)
        h_ref[sl, :] = normed(h_ref[sl, :], gain)

    h = h_ref[...]
    copies[2].wait()
    qkv_ref[:, 0:qd] = jnp.dot(h, wq[...], preferred_element_type=F32).astype(BF16)
    copies[3].wait()
    copies[4].wait()
    qkv_ref[:, qd:qd + kd] = jnp.dot(h, wk[...], preferred_element_type=F32).astype(BF16)
    qkv_ref[:, qd + kd:] = jnp.dot(h, wv[...], preferred_element_type=F32).astype(BF16)

    @pl.loop(0, blocks)
    def _(i):
        base = pl.multiple_of(i * BLOCK, BLOCK)
        at = pl.ds(base, BLOCK)
        for cp in reads(i):
            cp.wait()

        def k_put(b, value):
            kbuf[base + b] = value

        def v_put(b, value):
            vbuf[base + b] = value

        o = attend_block(
            qkv_ref[at, :], cos_ref[at, :], sin_ref[at, :], posc_ref[at, :], lambda b: pos_s[base + b],
            lambda b: kbuf[base + b], lambda b: vbuf[base + b], k_put, v_put)
        for n, o_n in enumerate(o):
            o_ref[at, n * kd:(n + 1) * kd] = o_n
        for cp in writes(i):
            cp.start()

    for i in range(blocks):
        for cp in writes(i):
            cp.wait()
    wo_copy.wait()


def first(hidden, attn_norm, w_query, w_key, w_value, w_out, positions, k_cache, v_cache):
    rows, d = hidden.shape
    qd, kd = w_query.shape[2], w_key.shape[2]
    seq = k_cache.shape[2]
    blocks = rows // BLOCK
    vmem = pl.BlockSpec(memory_space=pltpu.VMEM)
    hbm = pl.BlockSpec(memory_space=pl.ANY)
    dma = pltpu.SemaphoreType.DMA
    table = pltpu.VMEM((rows, kd), F32)
    cache = jax.ShapeDtypeStruct(k_cache.shape, BF16)
    return pl.pallas_call(
        first_kernel,
        in_specs=[hbm] * 11,
        out_specs=[vmem] * 5 + [hbm, hbm],
        out_shape=[pltpu.VMEM((rows, qd), BF16), pltpu.VMEM(w_out.shape[1:], BF16), table, table, table, cache, cache],
        scratch_shapes=[
            pltpu.VMEM((rows, d), BF16), pltpu.VMEM(attn_norm.shape, BF16), pltpu.VMEM((d, qd), BF16),
            pltpu.VMEM((d, kd), BF16), pltpu.VMEM((d, kd), BF16),
            pltpu.SMEM((rows,), jnp.int32), pltpu.VMEM((rows // kd, kd), jnp.int32), pltpu.VMEM((2, kd), F32),
            pltpu.VMEM((rows, qd + 2 * kd), BF16),
            pltpu.VMEM((rows, seq, kd), BF16), pltpu.VMEM((rows, seq, kd), BF16),
            dma((9,)), dma((2, blocks)), dma((2, blocks)),
        ],
        compiler_params=pltpu.CompilerParams(vmem_limit_bytes=FIRST_BYTES),
        name="first",
    )(*in_hbm(positions, hidden, attn_norm, w_query, w_key, w_value, w_out, positions.reshape(rows // kd, kd),
              jnp.asarray(rope_rows(kd)), k_cache, v_cache))


def cache_kernel(layer, x_ref, k_ref, v_ref, k_prev, v_prev, x_hbm, ko_hbm, vo_hbm, out_sem, x_sem):
    batch = k_ref.shape[0]
    blocks = batch // BLOCK
    writes = []
    for i in range(blocks):
        at = pl.ds(i * BLOCK, BLOCK)
        writes.append(pltpu.make_async_copy(k_ref.at[at], ko_hbm.at[layer, at], out_sem.at[0, i]))
        writes.append(pltpu.make_async_copy(v_ref.at[at], vo_hbm.at[layer, at], out_sem.at[1, i]))
    writes.append(pltpu.make_async_copy(x_ref, x_hbm, x_sem.at[0]))
    for cp in writes:
        cp.start()
    for cp in writes:
        cp.wait()


def write_cache(layer, x, k_layer, v_layer, k_prev, v_prev):
    blocks = k_layer.shape[0] // BLOCK
    vmem = pl.BlockSpec(memory_space=pltpu.VMEM)
    hbm = pl.BlockSpec(memory_space=pl.ANY)
    dma = pltpu.SemaphoreType.DMA
    return pl.pallas_call(
        functools.partial(cache_kernel, layer),
        in_specs=[vmem, vmem, vmem, hbm, hbm],
        out_specs=[hbm] * 3,
        out_shape=[jax.ShapeDtypeStruct(a.shape, BF16) for a in (x, k_prev, v_prev)],
        input_output_aliases={3: 1, 4: 2},
        scratch_shapes=[dma((2, blocks)), dma((1,))],
        compiler_params=pltpu.CompilerParams(vmem_limit_bytes=2 * 1024 * 1024),
        name="write_cache",
    )(x, k_layer, v_layer, k_prev, v_prev)


CHUNKS = 4

ORDER = (
    "O03O00P03O01P00P01S03O02P02S00S01F03G03g03S02F00",
    "D03G00P13F01g00D00G01F02P10g01D01S13G02P11g02D02",
    "S10F13P12Q23S11A23B23O23F10P23S12Q20A20F11B20O20",
    "Q21A21P20B21O21S23F12P21Q22A22B22S20O22F23P22G23",
    "S21g23F20D23G20S22g20F21D20P33G21P30g21F22D21G22",
    "P31g22S33D22P32S30S31S32F30F31F33E30F32E33E31E32",
)


def body_kernel(
    o_first, wo_first, cos, sin, posc, pos_hbm, x_hbm, gm_hbm, ga_hbm, wo_hbm, wg_hbm, wu_hbm, wd_hbm, wq_hbm, wk_hbm, wv_hbm, k_hbm, v_hbm,
    x_out, kbuf, vbuf,
    wo, wg, wu, wd, wq, wk, wv, o_s, xres, part, hbuf, hst, abuf, qkv_s, d2d_in, rs_out, rs_in, acc,
    gm, ga, pos_s,
    w_sem, x_sem, kv_sem, t_sem, d2d_s, d2d_r, rs_s, rs_r, ag_s, ag_r, fw_s, fw_r,
):
    chunks, _, _, own, d = part.shape
    rows = 8 * own
    ff = wg.shape[1]
    head = kbuf.shape[2]
    me = lax.axis_index("tp")
    group = lax.axis_index("dp")
    core = me % 2
    chip = me // 2
    chips = [chip, chip + 1 - 2 * (chip % 2), (chip + 2) % 4, 3 - chip]
    partner = (group, chip * 2 + 1 - core)
    peers = [None] + [(group, chips[k] * 2 + core) for k in (1, 2, 3)]
    order = (3, 1, 2)

    loads = {}

    def load(name, src, dst, sem):
        loads[name] = pltpu.make_async_copy(src, dst, sem)
        loads[name].start()

    def need(*names):
        for name in names:
            if name in loads:
                loads.pop(name).wait()

    load("gm", gm_hbm, gm, t_sem.at[0])
    for q in range(chunks):
        load(("x", q), x_hbm.at[q, core, chip], xres.at[q], x_sem.at[q])
    load("wg", wg_hbm.at[0], wg, w_sem.at[1])
    load("wu", wu_hbm.at[0], wu, w_sem.at[2])
    load("wd", wd_hbm.at[0], wd, w_sem.at[3])
    load("ga", ga_hbm, ga, t_sem.at[1])
    load("pos", pos_hbm, pos_s, t_sem.at[2])
    load("wq", wq_hbm.at[1], wq, w_sem.at[4])
    load("wk", wk_hbm.at[1], wk, w_sem.at[5])
    load("wv", wv_hbm.at[1], wv, w_sem.at[6])
    load("wo", wo_hbm.at[1], wo, w_sem.at[0])

    def load_kv(i):
        at = pl.ds(i * BLOCK, BLOCK)
        load(("k", i), k_hbm.at[1, at], kbuf.at[at], kv_sem.at[0, i])
        load(("v", i), v_hbm.at[1, at], vbuf.at[at], kv_sem.at[1, i])

    barrier = pltpu.get_barrier_semaphore()
    for dev in [partner] + peers[1:]:
        pl.semaphore_signal(barrier, inc=1, device_id=dev, device_id_type=MESH)
    pl.semaphore_wait(barrier, 4)

    def remote(src, dst, s, r, dev):
        return pltpu.make_async_remote_copy(
            src_ref=src, dst_ref=dst, send_sem=s, recv_sem=r, device_id=dev, device_id_type=MESH)

    def d2d(q):
        return remote(part.at[q, 1 - core], d2d_in.at[q], d2d_s.at[q], d2d_r.at[q], partner)

    def rs(q, k):
        return remote(rs_out.at[q, k - 1], rs_in.at[q, k - 1], rs_s.at[q, k - 1], rs_r.at[q, k - 1], peers[k])

    def ag(q, k):
        ref = hbuf.at[q, core, chip]
        return remote(ref, ref, ag_s.at[q, k - 1], ag_r.at[q, k - 1], peers[k])

    def ag_in(q, k):
        ref = hbuf.at[q, core, chips[k]]
        return remote(ref, ref, ag_s.at[q, k - 1], ag_r.at[q, k - 1], peers[k])

    def fw(q, k):
        ref = hbuf.at[q, core, chips[k]]
        return remote(ref, ref, fw_s.at[q, k], fw_r.at[q, k], partner)

    def fw_in(q, k):
        ref = hbuf.at[q, 1 - core, chips[k]]
        return remote(ref, ref, fw_s.at[q, k], fw_r.at[q, k], partner)

    def put_part(q, cols, value):
        for p in range(2):
            for c in range(4):
                at = (p * 4 + c) * own
                part[q, p, c, :, cols] = value[at:at + own].astype(BF16)

    def pair_sums(q):
        d2d(q).wait_recv()
        for k in order:
            pair = part[q, core, chips[k]].astype(F32) + d2d_in[q, chips[k]].astype(F32)
            rs_out[q, k - 1] = pair.astype(BF16)
            rs(q, k).start()
        acc[q] = part[q, core, chip].astype(F32) + d2d_in[q, chip].astype(F32)
        d2d(q).wait_send()

    def totals(a, q):
        for k in (1, 2, 3):
            rs(q, k).wait_recv()
        need(("x", q))
        total = acc[q]
        for k in (1, 2, 3):
            total = total + rs_in[q, k - 1].astype(F32)
        x = (xres[q].astype(F32) + total.astype(BF16).astype(F32)).astype(BF16)
        if a == 3:
            hbuf[q, core, chip] = x
        else:
            xres[q] = x
            if a == 1:
                need("ga")
                gain = ga[1:2, :]
            else:
                need("gm")
                gain = gm[a // 2:a // 2 + 1, :]
            hbuf[q, core, chip] = normed(x, gain.astype(F32))
        for k in order:
            ag(q, k).start()
        fw(q, 0).start()
        for k in (1, 2, 3):
            rs(q, k).wait_send()

    def forward(q):
        for k in (1, 2, 3):
            ag_in(q, k).wait_recv()
            fw(q, k).start()

    def gathered(q):
        for k in range(4):
            fw_in(q, k).wait_recv()
        for k in (1, 2, 3):
            ag(q, k).wait_send()
        for k in range(4):
            fw(q, k).wait_send()

    def stage(q):
        gathered(q)
        hst[q] = hbuf[q].reshape(rows, d)

    def out_product(a, q):
        if a:
            need("wo")
        o, w = (o_s, wo) if a else (o_first, wo_first)

        @pl.loop(0, d // 1024)
        def _(n):
            cols = pl.ds(pl.multiple_of(n * 1024, 1024), 1024)
            put_part(q, cols, jnp.dot(o[q * rows:(q + 1) * rows, :], w[:, cols], preferred_element_type=F32))

        d2d(q).start()

    def gate_up(q, half):
        if half == 0:
            stage(q)
            need("wg", "wu")
        steps_n = ff // 512

        @pl.loop(half * steps_n, (half + 1) * steps_n)
        def _(n):
            cols = pl.ds(pl.multiple_of(n * 256, 256), 256)
            h = hst[q]
            g = jnp.dot(h, wg[:, cols], preferred_element_type=F32).astype(BF16).astype(F32)
            u = jnp.dot(h, wu[:, cols], preferred_element_type=F32).astype(BF16).astype(F32)
            abuf[q, :, cols] = (g * jax.nn.sigmoid(g) * u).astype(BF16)

    def down(q):
        need("wd")

        @pl.loop(0, d // 1024)
        def _(n):
            cols = pl.ds(pl.multiple_of(n * 1024, 1024), 1024)
            put_part(q, cols, jnp.dot(abuf[q], wd[:, cols], preferred_element_type=F32))

        d2d(q).start()

    def qkv(q):
        stage(q)
        need("wq", "wk", "wv")
        qd, kd = wq.shape[1], wk.shape[1]
        h = hst[q]
        qkv_s[q, :, 0:qd] = jnp.dot(h, wq[...], preferred_element_type=F32).astype(BF16)
        qkv_s[q, :, qd:qd + kd] = jnp.dot(h, wk[...], preferred_element_type=F32).astype(BF16)
        qkv_s[q, :, qd + kd:] = jnp.dot(h, wv[...], preferred_element_type=F32).astype(BF16)

    def attend(q, i):
        for j in range(rows // BLOCK // 2):
            need("pos")
            first = i * (rows // 2) + j * BLOCK
            block = (q * rows + first) // BLOCK
            need(("k", block), ("v", block))
            base = block * BLOCK
            at = slice(base, base + BLOCK)

            def k_put(b, value):
                kbuf[base + b] = value

            def v_put(b, value):
                vbuf[base + b] = value

            o = attend_block(
                qkv_s[q, first:first + BLOCK, :], cos[at, :], sin[at, :], posc[at, :], lambda b: pos_s[base + b],
                lambda b: kbuf[base + b], lambda b: vbuf[base + b], k_put, v_put)
            for h, o_h in enumerate(o):
                o_s[at, h * head:(h + 1) * head] = o_h

    def result(q):
        gathered(q)
        x_out[q] = hbuf[q]

    steps = [line[i:i + 3] for line in ORDER for i in range(0, len(line), 3)]
    last = {name: max(i for i, s in enumerate(steps) if s[0] == name and s[1] == "0") for name in "OgD"}
    for i, code in enumerate(steps):
        name, a, q = code[0], int(code[1]), int(code[2])
        if name == "O":
            out_product(a, q)
        elif name == "P":
            pair_sums(q)
        elif name == "S":
            totals(a, q)
        elif name == "F":
            forward(q)
        elif name in "Gg":
            gate_up(q, "Gg".index(name))
        elif name == "D":
            down(q)
        elif name == "Q":
            qkv(q)
        elif name in "AB":
            attend(q, "AB".index(name))
        else:
            result(q)
        if code == "D00":
            for j in range(kbuf.shape[0] // BLOCK):
                load_kv(j)
        if i == last["g"]:
            load("wg", wg_hbm.at[1], wg, w_sem.at[1])
            load("wu", wu_hbm.at[1], wu, w_sem.at[2])
        if i == last["D"]:
            load("wd", wd_hbm.at[1], wd, w_sem.at[3])


def body(positions, o, wo_first, x, mlp_norm, attn_norm, w_out, w_gate, w_up, w_down, w_query, w_key, w_value, k_cache, v_cache, cos2, sin2, posc):
    batch, qd = o.shape
    d = w_out.shape[2]
    ff = w_gate.shape[2]
    kd = w_key.shape[2]
    seq = k_cache.shape[2]
    own = batch // (8 * CHUNKS)
    rows = 8 * own
    vmem = pl.BlockSpec(memory_space=pltpu.VMEM)
    hbm = pl.BlockSpec(memory_space=pl.ANY)
    dma = pltpu.SemaphoreType.DMA
    cache = pltpu.VMEM((batch, seq, kd), BF16)
    return pl.pallas_call(
        body_kernel,
        in_specs=[vmem] * 5 + [hbm] * 13,
        out_specs=[vmem] * 3,
        out_shape=[pltpu.VMEM((CHUNKS, 2, 4, own, d), BF16), cache, cache],
        scratch_shapes=[
            pltpu.VMEM((qd, d), BF16), pltpu.VMEM((d, ff), BF16), pltpu.VMEM((d, ff), BF16), pltpu.VMEM((ff, d), BF16),
            pltpu.VMEM((d, qd), BF16), pltpu.VMEM((d, kd), BF16), pltpu.VMEM((d, kd), BF16),
            pltpu.VMEM((batch, qd), BF16),
            pltpu.VMEM((CHUNKS, own, d), BF16),
            pltpu.VMEM((CHUNKS, 2, 4, own, d), BF16),
            pltpu.VMEM((CHUNKS, 2, 4, own, d), BF16),
            pltpu.VMEM((CHUNKS, rows, d), BF16),
            pltpu.VMEM((CHUNKS, rows, ff), BF16),
            pltpu.VMEM((CHUNKS, rows, qd + 2 * kd), BF16),
            pltpu.VMEM((CHUNKS, 4, own, d), BF16),
            pltpu.VMEM((CHUNKS, 3, own, d), BF16),
            pltpu.VMEM((CHUNKS, 3, own, d), BF16),
            pltpu.VMEM((CHUNKS, own, d), F32),
            pltpu.VMEM(mlp_norm.shape, BF16), pltpu.VMEM(attn_norm.shape, BF16), pltpu.SMEM((batch,), jnp.int32),
            dma((7,)), dma((CHUNKS,)), dma((2, batch // BLOCK)), dma((3,)),
            dma((CHUNKS,)), dma((CHUNKS,)),
            dma((CHUNKS, 3)), dma((CHUNKS, 3)),
            dma((CHUNKS, 3)), dma((CHUNKS, 3)),
            dma((CHUNKS, 4)), dma((CHUNKS, 4)),
        ],
        compiler_params=pltpu.CompilerParams(vmem_limit_bytes=BODY_BYTES, collective_id=0, has_side_effects=True),
        name="body",
    )(*on_chip(o, wo_first, cos2, sin2, posc),
      *in_hbm(positions, x, mlp_norm, attn_norm, w_out, w_gate, w_up, w_down, w_query, w_key, w_value, k_cache, v_cache))


def solution(mesh):
    row_spec = P('dp', None)
    pos_spec = P('dp')
    cache_spec = P(None, 'dp', None, 'tp', None)
    norm_spec = P(None, None)
    col_spec = P(None, None, 'tp')
    split_rows = P(None, 'tp', None)

    def local_step(hidden, positions, k_cache, v_cache, attn_norm, w_query, w_key, w_value, w_out, mlp_norm, w_gate, w_up, w_down):
        layers, batch, seq, _, head = k_cache.shape
        d = hidden.shape[1]
        own = batch // (8 * CHUNKS)
        kc = k_cache.reshape(layers, batch, seq, head)
        vc = v_cache.reshape(layers, batch, seq, head)
        o, wo_first, cos2, sin2, posc, k_out, v_out = first(hidden, attn_norm, w_query, w_key, w_value, w_out, positions, kc, vc)
        x = hidden.reshape(CHUNKS, 2, 4, own, d)
        x_out, k_layer, v_layer = body(positions, o, wo_first, x, mlp_norm, attn_norm, w_out, w_gate, w_up, w_down,
                                     w_query, w_key, w_value, kc, vc, cos2, sin2, posc)
        x_out, k_out, v_out = write_cache(1, x_out.reshape(batch, d), k_layer, v_layer, k_out, v_out)
        return x_out, k_out.reshape(k_cache.shape), v_out.reshape(v_cache.shape)

    return jax.shard_map(local_step, mesh=mesh, in_specs=(row_spec, pos_spec, cache_spec, cache_spec, norm_spec, col_spec, col_spec, col_spec, split_rows, norm_spec, col_spec, col_spec, split_rows), out_specs=(row_spec, cache_spec, cache_spec), check_vma=False)
```
